8 devices in a mesh: ens: 1 (over z), col: 2 (over y), row: 4 (over x, core).
Axes of the slice: x: 2, y: 2, z: 1, core: 2. Of those that a mesh axis runs over, the one named last changes fastest.
Arguments:
- u_init: float32 [1024, 1024], P(('ens', 'row'), 'col')
- v_init: float32 [1024, 1024], P(('ens', 'row'), 'col')
- stencil_w: float32 [64, 3, 3], replicated
Outputs:
- output 1: float32 [1024, 1024], P(('ens', 'row'), 'col')
- output 2: float32 [1024, 1024], P(('ens', 'row'), 'col')
All inputs are finite; a program needn't handle non-finite values.
Results may differ from the reference program's by a relative error of at most 0.001.
Values are sent between devices in bfloat16 or wider.
A program may use at most 1 GiB of HBM per device.

```python
import jax
import jax.numpy as jnp
from jax import lax

GRID_ROWS = 1024
GRID_COLS = 1024
NUM_STEPS = 64
TIME_STEP = 0.5


def block_field(base_key, block_rows, block_cols):
    block_vals = jax.random.normal(base_key, (GRID_ROWS // block_rows, GRID_COLS // block_cols), jnp.float32)
    spread = jnp.broadcast_to(block_vals[:, None, :, None], (GRID_ROWS // block_rows, block_rows, GRID_COLS // block_cols, block_cols))
    return spread.reshape(GRID_ROWS, GRID_COLS)


def setup_inputs(seed: int = 0, part: int = 0) -> dict:
    part_key = jax.random.fold_in(jax.random.key(seed), part)
    key_ublock, key_unoise, key_vblock, key_vnoise = jax.random.split(part_key, 4)
    u_init = block_field(key_ublock, 8, 8) + 0.3 * jax.random.normal(key_unoise, (GRID_ROWS, GRID_COLS), jnp.float32)
    v_init = 0.5 * block_field(key_vblock, 8, 8) + 0.2 * jax.random.normal(key_vnoise, (GRID_ROWS, GRID_COLS), jnp.float32)
    key_pair, key_centre, key_total = jax.random.split(jax.random.key(seed + 1), 3)
    pair_weights = jax.random.uniform(key_pair, (NUM_STEPS, 4), jnp.float32, minval=0.07, maxval=0.13)
    centre = jax.random.uniform(key_centre, (NUM_STEPS,), jnp.float32, minval=0.2, maxval=0.35)
    weight_total = jax.random.uniform(key_total, (NUM_STEPS,), jnp.float32, minval=0.93, maxval=0.98)
    raw_weights = jnp.stack([
        pair_weights[:, 2], pair_weights[:, 0], pair_weights[:, 3],
        pair_weights[:, 1], centre, pair_weights[:, 1],
        pair_weights[:, 3], pair_weights[:, 0], pair_weights[:, 2]], axis=1)
    weight_scale = weight_total / jnp.sum(raw_weights, axis=1)
    stencil_w = (raw_weights * weight_scale[:, None]).reshape(NUM_STEPS, 3, 3)
    return {"u_init": u_init, "v_init": v_init, "stencil_w": stencil_w}


def stencil_sum(field_now, step_w):
    total_acc = step_w[0, 0] * jnp.roll(field_now, (1, 1), axis=(0, 1))
    for tap_index in range(1, 9):
        row_off, col_off = divmod(tap_index, 3)
        total_acc = total_acc + step_w[row_off, col_off] * jnp.roll(field_now, (1 - row_off, 1 - col_off), axis=(0, 1))
    return total_acc


def reference(u_init, v_init, stencil_w):
    def one_step(state_pair, step_w):
        u_now, v_now = state_pair
        v_next = v_now + (stencil_sum(u_now, step_w) - u_now)
        u_next = u_now + TIME_STEP * v_next
        return (u_next, v_next), None

    (u_final, v_final), _ = lax.scan(one_step, (u_init, v_init), stencil_w)
    return (u_final, v_final)
```

```python
import jax
import jax.numpy as jnp
from jax import lax
from jax.experimental import pallas as pl
from jax.experimental.pallas import tpu as pltpu
from jax.sharding import PartitionSpec as P

F32 = jnp.float32
MESH = pl.DeviceIdType.MESH
ROWS, COLS = 256, 512
G = 5
T = 16
SWEEPS = 4
TILES = 3
TILE = (ROWS + 2 * T) // TILES
NG = TILE // 8
OFF = 40
R = OFF + ROWS + OFF


def wave_kernel(u_hbm, v_hbm, w_ref, uo_hbm, vo_hbm, sa, sb, uraw, vraw, pbuf, hbuf, uout, vout, sbuf, rbuf,
                load_sem, raw_ssem, raw_rsem, pk_ssem, pk_rsem, dg_ssem, dg_rsem, ex_ssem, ex_rsem, out_sem):
    row = lax.axis_index("row")
    col = lax.axis_index("col")
    up = lax.rem(row + 3, 4)
    down = lax.rem(row + 1, 4)
    other = 1 - col

    loads = [
        pltpu.make_async_copy(u_hbm, uraw.at[pl.ds(T, ROWS)], load_sem.at[0]),
        pltpu.make_async_copy(v_hbm, vraw.at[pl.ds(T, ROWS)], load_sem.at[1]),
    ]
    for cp in loads:
        cp.start()

    barrier = pltpu.get_barrier_semaphore()
    for rr, cc in ((row, other), (up, col), (down, col), (up, other), (down, other)):
        pl.semaphore_signal(barrier, inc=1, device_id={"row": rr, "col": cc}, device_id_type=MESH)
    pl.semaphore_wait(barrier, 5)

    def raw_copy(f, side):
        src = (u_hbm, v_hbm)[f]
        dst = (uraw, vraw)[f]
        lo, at, to = ((0, T + ROWS, up), (ROWS - T, 0, down))[side]
        return pltpu.make_async_remote_copy(
            src_ref=src.at[pl.ds(lo, T)], dst_ref=dst.at[pl.ds(at, T)],
            send_sem=raw_ssem.at[f, side], recv_sem=raw_rsem.at[f, side],
            device_id={"row": to, "col": col}, device_id_type=MESH)

    raws = [raw_copy(f, side) for side in range(2) for f in range(2)]
    for cp in raws:
        cp.start()

    cuts = [0] + [TILE * (c + 1) - T for c in range(TILES - 1)] + [ROWS]

    def packed_copy(c):
        n = cuts[c + 1] - cuts[c]
        return pltpu.make_async_remote_copy(
            src_ref=pbuf.at[:, pl.ds(cuts[c], n)], dst_ref=hbuf.at[:, pl.ds(T + cuts[c], n)],
            send_sem=pk_ssem.at[c], recv_sem=pk_rsem.at[c],
            device_id={"row": row, "col": other}, device_id_type=MESH)

    def diag_copy(side):
        lo, at, to = ((0, T + ROWS, up), (ROWS - T, 0, down))[side]
        return pltpu.make_async_remote_copy(
            src_ref=pbuf.at[:, pl.ds(lo, T)], dst_ref=hbuf.at[:, pl.ds(at, T)],
            send_sem=dg_ssem.at[side], recv_sem=dg_rsem.at[side],
            device_id={"row": to, "col": other}, device_id_type=MESH)

    packs = [packed_copy(c) for c in range(TILES)]
    diags = [diag_copy(side) for side in range(2)]

    def zero(i, _):
        for g in range(G + 2):
            sa[g, pl.ds(pl.multiple_of(i * 8, 8), 8), :] = jnp.zeros((8, 128), F32)
            sb[g, pl.ds(pl.multiple_of(i * 8, 8), 8), :] = jnp.zeros((8, 128), F32)
        return 0

    lax.fori_loop(0, R // 8, zero, 0)
    for cp in loads:
        cp.wait()

    lane = lax.broadcasted_iota(jnp.int32, (8, 128), 1)

    def pack(i, _):
        r = pl.multiple_of(i * 8, 8)
        for f, ref in ((0, uraw), (1, vraw)):
            pbuf[f, pl.ds(r, 8), :] = jnp.where(lane < 64, ref[pl.ds(r + T, 8), 0:128], ref[pl.ds(r + T, 8), 384:512])
        return 0

    for c in range(TILES):
        lax.fori_loop(cuts[c] // 8, cuts[c + 1] // 8, pack, 0)
        if c == 0:
            diags[0].start()
        packs[c].start()
    diags[1].start()

    def place(g):
        c = lane * G + (g - 64)
        return lax.rem(c + 128, 128), lax.div(c + 128, 128)

    def lanes(x, idx):
        return jnp.take_along_axis(x, idx, axis=1, mode="promise_in_bounds")

    def put_main(i, _):
        r = pl.multiple_of(i * 8, 8)
        q = pl.multiple_of(i * 8 + (OFF - T), 8)
        us = [0.25 * uraw[pl.ds(r, 8), 128 * k:128 * k + 128] for k in range(4)]
        ps = [us[k] - 0.125 * vraw[pl.ds(r, 8), 128 * k:128 * k + 128] for k in range(4)]
        for g in range(G):
            idx, at = place(g)
            for dst, src in ((sa, us), (sb, ps)):
                x = lanes(src[0], idx)
                for k in range(1, 4):
                    x = jnp.where(at == k + 1, lanes(src[k], idx), x)
                dst[g + 1, pl.ds(q, 8), :] = x
        return 0

    def put_halo(i, _):
        r = pl.multiple_of(i * 8, 8)
        q = pl.multiple_of(i * 8 + (OFF - T), 8)
        hu = 0.25 * hbuf[0, pl.ds(r, 8), :]
        hp = hu - 0.125 * hbuf[1, pl.ds(r, 8), :]
        for g in range(G):
            idx, at = place(g)
            out = (at == 0) | (at == 5)
            x = jnp.where(out, lanes(hu, idx), sa[g + 1, pl.ds(q, 8), :])
            sa[g + 1, pl.ds(q, 8), :] = x
            if g == 0:
                sa[G + 1, pl.ds(q, 8), :] = pltpu.roll(x, 127, 1)
            if g == G - 1:
                sa[0, pl.ds(q, 8), :] = pltpu.roll(x, 1, 1)
            sb[g + 1, pl.ds(q, 8), :] = jnp.where(out, lanes(hp, idx), sb[g + 1, pl.ds(q, 8), :])
        return 0

    lax.fori_loop(T // 8, (T + ROWS) // 8, put_main, 0)

    def step(t, src, dst, start):
        wa, wb, wc, wd, we = [0.5 * w_ref[a, b, t] for a, b in ((0, 0), (0, 1), (0, 2), (1, 0), (1, 1))]
        wa, wb, wc, wd, we = [jnp.full((8, 128), x, F32) for x in (wa, wb, wc, wd, 1.5 + we)]
        sv = src.at[:, pl.ds(start - 1, TILE + 2)]
        dv = dst.at[:, pl.ds(start, TILE)]
        for i in range(NG):
            n = [sv[g, pl.ds(8 * i, 8), :] for g in range(G + 2)]
            m = [sv[g, pl.ds(8 * i + 1, 8), :] for g in range(G + 2)]
            s = [sv[g, pl.ds(8 * i + 2, 8), :] for g in range(G + 2)]
            for g in range(1, G + 1):
                x = (wa * (n[g - 1] + s[g + 1]) + wc * (n[g + 1] + s[g - 1])) + (wb * (n[g] + s[g]) + wd * (m[g - 1] + m[g + 1]))
                x = x + (we * m[g] - dv[g, pl.ds(8 * i, 8), :])
                dv[g, pl.ds(8 * i, 8), :] = x
                if g == 1:
                    dv[G + 1, pl.ds(8 * i, 8), :] = pltpu.roll(x, 127, 1)
                if g == G:
                    dv[0, pl.ds(8 * i, 8), :] = pltpu.roll(x, 1, 1)

    def exchange(e, side, to):
        return pltpu.make_async_remote_copy(
            src_ref=sbuf.at[e, side], dst_ref=rbuf.at[e, side],
            send_sem=ex_ssem.at[e, side], recv_sem=ex_rsem.at[e, side],
            device_id={"row": to, "col": col}, device_id_type=MESH)

    def get_plain(i, _):
        r = pl.multiple_of(i * 8, 8)
        q = pl.multiple_of(i * 8 + OFF, 8)
        us = [sa[g + 1, pl.ds(q, 8), :] for g in range(G)]
        vs = [8.0 * (us[g] - sb[g + 1, pl.ds(q, 8), :]) for g in range(G)]
        us = [4.0 * x for x in us]
        for h in range(4):
            p = lane + (128 * h + 64)
            idx, at = lax.div(p, G), lax.rem(p, G)
            for dst, src in ((uout, us), (vout, vs)):
                x = lanes(src[0], idx)
                for g in range(1, G):
                    x = jnp.where(at == g, lanes(src[g], idx), x)
                dst[pl.ds(r, 8), 128 * h:128 * h + 128] = x
        return 0

    ends = [ROWS] + [ROWS + T - TILE * (c + 1) + T for c in range(TILES - 1)] + [0]

    def out_copies(c):
        lo, n = ends[c + 1], ends[c] - ends[c + 1]
        return [pltpu.make_async_copy(src.at[pl.ds(lo, n)], dst.at[pl.ds(lo, n)], out_sem.at[f, c])
                for f, (src, dst) in enumerate(((uout, uo_hbm), (vout, vo_hbm)))]

    def tile(it, _):
        sweep, c = lax.div(it, TILES), lax.rem(it, TILES)
        odd = lax.rem(sweep, 2)
        base = jnp.where(odd == 0, OFF - T + TILE * c, OFF + ROWS + T - TILE * (c + 1))
        sign = 2 * odd - 1

        @pl.when(it == 0)
        def _():
            raws[2].wait_recv()
            raws[3].wait_recv()
            diags[1].wait_recv()
            packs[0].wait_recv()

        @pl.when(it == 1)
        def _():
            packs[1].wait_recv()

        @pl.when(it == 2)
        def _():
            raws[0].wait_recv()
            raws[1].wait_recv()
            diags[0].wait_recv()
            packs[2].wait_recv()

        @pl.when((it == 0) | (it == 2))
        def _():
            at = jnp.where(it == 0, 0, (T + ROWS) // 8)
            lax.fori_loop(at, at + T // 8, put_main, 0)

        @pl.when(sweep == 0)
        def _():
            lax.fori_loop(c * NG, c * NG + NG, put_halo, 0)

        prev = it - 1
        psweep, pc = lax.div(prev, TILES), lax.rem(prev, TILES)
        has_edge = (it > 0) & (pc != 1) & (psweep < SWEEPS - 1)
        pside = jnp.where(pc == 0, lax.rem(psweep, 2), 1 - lax.rem(psweep, 2))

        @pl.when(has_edge)
        def _():
            at = jnp.where(pside == 0, OFF, OFF + ROWS - T)
            for k in range(T // 8):
                q = pl.multiple_of(at + 8 * k, 8)
                for g in range(G):
                    sbuf[psweep, pside, 0, g, pl.ds(8 * k, 8), :] = sa[g + 1, pl.ds(q, 8), :]
                    sbuf[psweep, pside, 1, g, pl.ds(8 * k, 8), :] = sb[g + 1, pl.ds(q, 8), :]

        hside = jnp.where(c == 0, odd, 1 - odd)

        @pl.when((sweep > 0) & (c != 1))
        def _():
            exchange(sweep - 1, 1 - hside, down).wait_recv()
            at = jnp.where(hside == 0, OFF - T, OFF + ROWS)
            for k in range(T // 8):
                q = pl.multiple_of(at + 8 * k, 8)
                for g in range(G):
                    x = rbuf[sweep - 1, 1 - hside, 0, g, pl.ds(8 * k, 8), :]
                    sa[g + 1, pl.ds(q, 8), :] = x
                    if g == 0:
                        sa[G + 1, pl.ds(q, 8), :] = pltpu.roll(x, 127, 1)
                    if g == G - 1:
                        sa[0, pl.ds(q, 8), :] = pltpu.roll(x, 1, 1)
                    sb[g + 1, pl.ds(q, 8), :] = rbuf[sweep - 1, 1 - hside, 1, g, pl.ds(8 * k, 8), :]

        def pair(i, _):
            t = sweep * T + 2 * i
            step(t, sa, sb, base + sign * (2 * i + 1))
            step(t + 1, sb, sa, base + sign * (2 * i + 2))

            @pl.when((i == 0) & has_edge)
            def _():
                exchange(psweep, pside, jnp.where(pside == 0, up, down)).start()

            return 0

        lax.fori_loop(0, T // 2, pair, 0)

        @pl.when(sweep == SWEEPS - 1)
        def _():
            lo = jnp.where(c == TILES - 1, 0, ROWS + 2 * T - TILE * (c + 1))
            hi = jnp.where(c == 0, ROWS, ROWS + 2 * T - TILE * c)
            lax.fori_loop(lax.div(lo, 8), lax.div(hi, 8), get_plain, 0)
            for k in range(TILES):
                @pl.when(c == k)
                def _():
                    for cp in out_copies(k):
                        cp.start()

        return 0

    lax.fori_loop(0, SWEEPS * TILES, tile, 0)

    for cp in raws + packs + diags:
        cp.wait_send()
    for e in range(SWEEPS - 1):
        for side in range(2):
            exchange(e, side, up).wait_send()
    for k in range(TILES):
        for cp in out_copies(k):
            cp.wait()


def solution(mesh):
    def local_run(u_tile, v_tile, w):
        dma = pltpu.SemaphoreType.DMA
        return pl.pallas_call(
            wave_kernel,
            out_shape=[jax.ShapeDtypeStruct((ROWS, COLS), F32)] * 2,
            in_specs=[pl.BlockSpec(memory_space=pl.ANY)] * 2 + [pl.BlockSpec(memory_space=pltpu.SMEM)],
            out_specs=[pl.BlockSpec(memory_space=pl.ANY)] * 2,
            scratch_shapes=[
                pltpu.VMEM((G + 2, R, 128), F32), pltpu.VMEM((G + 2, R, 128), F32),
                pltpu.VMEM((ROWS + 2 * T, COLS), F32), pltpu.VMEM((ROWS + 2 * T, COLS), F32),
                pltpu.VMEM((2, ROWS, 128), F32), pltpu.VMEM((2, ROWS + 2 * T, 128), F32),
                pltpu.VMEM((ROWS, COLS), F32), pltpu.VMEM((ROWS, COLS), F32),
                pltpu.VMEM((SWEEPS - 1, 2, 2, G, T, 128), F32), pltpu.VMEM((SWEEPS - 1, 2, 2, G, T, 128), F32),
                dma((2,)), dma((2, 2)), dma((2, 2)), dma((TILES,)), dma((TILES,)), dma((2,)), dma((2,)),
                dma((SWEEPS - 1, 2)), dma((SWEEPS - 1, 2)), dma((2, TILES)),
            ],
            compiler_params=pltpu.CompilerParams(collective_id=0, has_side_effects=True),
        )(u_tile, v_tile, jnp.transpose(w, (1, 2, 0)))

    tile_spec = P(("ens", "row"), "col")
    return jax.shard_map(local_run, mesh=mesh, in_specs=(tile_spec, tile_spec, P()), out_specs=(tile_spec, tile_spec), check_vma=False)
```

```python
import jax
import jax.numpy as jnp
from jax import lax
from jax.experimental import pallas as pl
from jax.experimental.pallas import tpu as pltpu
from jax.sharding import PartitionSpec as P

F32 = jnp.float32
MESH = pl.DeviceIdType.MESH
ROWS, COLS = 256, 512
G = 5
T = 16
SWEEPS = 4
TILES = 3
TILE = (ROWS + 2 * T) // TILES
NG = TILE // 8
OFF = 40
R = OFF + ROWS + OFF


def wave_kernel(u_hbm, v_hbm, w_hbm, uo_hbm, vo_hbm, st, w_ref, maps, uraw, vraw, pbuf, hbuf, uout, vout, sbuf, rbuf,
                load_sem, raw_ssem, raw_rsem, pk_ssem, pk_rsem, dg_ssem, dg_rsem, ex_ssem, ex_rsem, out_sem):
    row = lax.axis_index("row")
    col = lax.axis_index("col")
    up = lax.rem(row + 3, 4)
    down = lax.rem(row + 1, 4)
    other = 1 - col

    loads = [
        pltpu.make_async_copy(u_hbm, uraw.at[pl.ds(T, ROWS)], load_sem.at[0]),
        pltpu.make_async_copy(v_hbm, vraw.at[pl.ds(T, ROWS)], load_sem.at[1]),
        pltpu.make_async_copy(w_hbm, w_ref, load_sem.at[2]),
    ]
    for cp in loads:
        cp.start()

    barrier = pltpu.get_barrier_semaphore()
    for rr, cc in ((row, other), (up, col), (down, col), (up, other), (down, other)):
        pl.semaphore_signal(barrier, inc=1, device_id={"row": rr, "col": cc}, device_id_type=MESH)
    pl.semaphore_wait(barrier, 5)

    def raw_copy(f, side):
        src = (u_hbm, v_hbm)[f]
        dst = (uraw, vraw)[f]
        lo, at, to = ((0, T + ROWS, up), (ROWS - T, 0, down))[side]
        return pltpu.make_async_remote_copy(
            src_ref=src.at[pl.ds(lo, T)], dst_ref=dst.at[pl.ds(at, T)],
            send_sem=raw_ssem.at[f, side], recv_sem=raw_rsem.at[f, side],
            device_id={"row": to, "col": col}, device_id_type=MESH)

    raws = [raw_copy(f, side) for side in range(2) for f in range(2)]
    for cp in raws[2:] + raws[:2]:
        cp.start()

    cuts = [0] + [TILE * (c + 1) - T for c in range(TILES - 1)] + [ROWS]

    def packed_copy(c):
        n = cuts[c + 1] - cuts[c]
        return pltpu.make_async_remote_copy(
            src_ref=pbuf.at[:, pl.ds(cuts[c], n)], dst_ref=hbuf.at[:, pl.ds(T + cuts[c], n)],
            send_sem=pk_ssem.at[c], recv_sem=pk_rsem.at[c],
            device_id={"row": row, "col": other}, device_id_type=MESH)

    def diag_copy(side):
        lo, at, to = ((0, T + ROWS, up), (ROWS - T, 0, down))[side]
        return pltpu.make_async_remote_copy(
            src_ref=pbuf.at[:, pl.ds(lo, T)], dst_ref=hbuf.at[:, pl.ds(at, T)],
            send_sem=dg_ssem.at[side], recv_sem=dg_rsem.at[side],
            device_id={"row": to, "col": other}, device_id_type=MESH)

    packs = [packed_copy(c) for c in range(TILES)]
    diags = [diag_copy(side) for side in range(2)]

    def zero(i, _):
        for f in range(2):
            for g in range(G + 2):
                st[f, g, pl.ds(pl.multiple_of(i * 8, 8), 8), :] = jnp.zeros((8, 128), F32)
        return 0

    lax.fori_loop(0, (OFF - T) // 8, zero, 0)
    lax.fori_loop((OFF + ROWS + T) // 8, R // 8, zero, 0)

    lane = lax.broadcasted_iota(jnp.int32, (8, 128), 1)
    maps[2 * G] = lax.rem(lane, G)
    for g in range(G):
        maps[g] = lax.rem(lane * G + (g + 64), 128)
        k = lax.rem(3 * (lane + (2 * G - g - 1)), G)
        maps[G + g] = lax.div(lax.rem(128 * k + lane + 64, 128 * G), G)

    for cp in loads:
        cp.wait()

    def pack(i, _):
        r = pl.multiple_of(i * 8, 8)
        for f, ref in ((0, uraw), (1, vraw)):
            pbuf[f, pl.ds(r, 8), :] = jnp.where(lane < 64, ref[pl.ds(r + T, 8), 0:128], ref[pl.ds(r + T, 8), 384:512])
        return 0

    lax.fori_loop((ROWS - T) // 8, ROWS // 8, pack, 0)
    lax.fori_loop(0, cuts[1] // 8, pack, 0)
    diags[1].start()
    packs[0].start()
    diags[0].start()
    lax.fori_loop(cuts[1] // 8, (ROWS - T) // 8, pack, 0)
    packs[1].start()
    packs[2].start()

    def lanes(x, idx):
        return jnp.take_along_axis(x, idx, axis=1, mode="promise_in_bounds")

    UN = 4

    def put(i, _):
        residue = maps[2 * G]
        rows = [(pl.multiple_of((i * UN + n) * 8, 8), pl.multiple_of((i * UN + n) * 8 + (OFF - T), 8)) for n in range(UN)]
        srcs = []
        for r, q in rows:
            us = [0.25 * uraw[pl.ds(r, 8), 128 * k:128 * k + 128] for k in range(4)] + [0.25 * hbuf[0, pl.ds(r, 8), :]]
            vs = [vraw[pl.ds(r, 8), 128 * k:128 * k + 128] for k in range(4)] + [hbuf[1, pl.ds(r, 8), :]]
            srcs.append((us, [u - 0.125 * v for u, v in zip(us, vs)]))
        for g in range(G):
            idx = maps[g]
            for (r, q), pair in zip(rows, srcs):
                for f in range(2):
                    x = pair[f][4]
                    for k in range(4):
                        x = jnp.where(residue == (g + 1 + 2 * k) % G, pair[f][k], x)
                    x = lanes(x, idx)
                    st[f, g + 1, pl.ds(q, 8), :] = x
                    if f == 0 and g == 0:
                        st[0, G + 1, pl.ds(q, 8), :] = pltpu.roll(x, 127, 1)
                    if f == 0 and g == G - 1:
                        st[0, 0, pl.ds(q, 8), :] = pltpu.roll(x, 1, 1)
        return 0

    def step(t, src, start):
        dst = 1 - src
        wa, wb, wc, wd, we = [0.5 * w_ref[a, b, t] for a, b in ((0, 0), (0, 1), (0, 2), (1, 0), (1, 1))]
        wa, wb, wc, wd, we = [jnp.full((8, 128), x, F32) for x in (wa, wb, wc, wd, 1.5 + we)]
        sv = st.at[:, :, pl.ds(start - 1, TILE + 2)]
        for i in range(NG):
            n = [sv[src, g, pl.ds(8 * i, 8), :] for g in range(G + 2)]
            m = [sv[src, g, pl.ds(8 * i + 1, 8), :] for g in range(G + 2)]
            s = [sv[src, g, pl.ds(8 * i + 2, 8), :] for g in range(G + 2)]
            for g in range(1, G + 1):
                x = (wa * (n[g - 1] + s[g + 1]) + wc * (n[g + 1] + s[g - 1])) + (wb * (n[g] + s[g]) + wd * (m[g - 1] + m[g + 1]))
                x = x + (we * m[g] - sv[dst, g, pl.ds(8 * i + 1, 8), :])
                sv[dst, g, pl.ds(8 * i + 1, 8), :] = x
                if g == 1:
                    sv[dst, G + 1, pl.ds(8 * i + 1, 8), :] = pltpu.roll(x, 127, 1)
                if g == G:
                    sv[dst, 0, pl.ds(8 * i + 1, 8), :] = pltpu.roll(x, 1, 1)

    def exchange(e, side, to):
        return pltpu.make_async_remote_copy(
            src_ref=sbuf.at[e, side], dst_ref=rbuf.at[e, side],
            send_sem=ex_ssem.at[e, side], recv_sem=ex_rsem.at[e, side],
            device_id={"row": to, "col": col}, device_id_type=MESH)

    def get_plain(i, _):
        residue = maps[2 * G]
        for f, out in ((0, uout), (1, vout)):
            zs = []
            for n in range(UN):
                q = pl.multiple_of((i * UN + n) * 8 + OFF, 8)
                for g in range(G):
                    x = st[0, g + 1, pl.ds(q, 8), :]
                    zs.append(4.0 * x if f == 0 else 8.0 * (x - st[1, g + 1, pl.ds(q, 8), :]))
            for g in range(G):
                idx = maps[G + g]
                for n in range(UN):
                    zs[n * G + g] = lanes(zs[n * G + g], idx)
            for n in range(UN):
                r = pl.multiple_of((i * UN + n) * 8, 8)
                for k in range(4):
                    x = zs[n * G]
                    for g in range(1, G):
                        x = jnp.where(residue == (g + 1 + 2 * k) % G, zs[n * G + g], x)
                    out[pl.ds(r, 8), 128 * k:128 * k + 128] = x
        return 0

    ends = [ROWS] + [ROWS + T - TILE * (c + 1) + T for c in range(TILES - 1)] + [0]

    def out_copies(c):
        lo, n = ends[c + 1], ends[c] - ends[c + 1]
        return [pltpu.make_async_copy(src.at[pl.ds(lo, n)], dst.at[pl.ds(lo, n)], out_sem.at[f, c])
                for f, (src, dst) in enumerate(((uout, uo_hbm), (vout, vo_hbm)))]

    def tile(it, _):
        sweep, c = lax.div(it, TILES), lax.rem(it, TILES)
        odd = lax.rem(sweep, 2)
        base = jnp.where(odd == 0, OFF - T + TILE * c, OFF + ROWS + T - TILE * (c + 1))
        sign = 2 * odd - 1

        @pl.when(it == 0)
        def _():
            raws[2].wait_recv()
            raws[3].wait_recv()
            diags[1].wait_recv()
            packs[0].wait_recv()

        @pl.when(it == 1)
        def _():
            packs[1].wait_recv()

        @pl.when(it == 2)
        def _():
            raws[0].wait_recv()
            raws[1].wait_recv()
            diags[0].wait_recv()
            packs[2].wait_recv()

        @pl.when(sweep == 0)
        def _():
            lax.fori_loop(c * (NG // UN), (c + 1) * (NG // UN), put, 0)

        prev = it - 1
        psweep, pc = lax.div(prev, TILES), lax.rem(prev, TILES)
        has_edge = (it > 0) & (pc != 1) & (psweep < SWEEPS - 1)
        pside = jnp.where(pc == 0, lax.rem(psweep, 2), 1 - lax.rem(psweep, 2))

        @pl.when(has_edge)
        def _():
            at = jnp.where(pside == 0, OFF, OFF + ROWS - T)
            for k in range(T // 8):
                q = pl.multiple_of(at + 8 * k, 8)
                for g in range(G):
                    sbuf[psweep, pside, 0, g, pl.ds(8 * k, 8), :] = st[0, g + 1, pl.ds(q, 8), :]
                    sbuf[psweep, pside, 1, g, pl.ds(8 * k, 8), :] = st[1, g + 1, pl.ds(q, 8), :]

        hside = jnp.where(c == 0, odd, 1 - odd)

        @pl.when((sweep > 0) & (c != 1))
        def _():
            exchange(sweep - 1, 1 - hside, down).wait_recv()
            at = jnp.where(hside == 0, OFF - T, OFF + ROWS)
            for k in range(T // 8):
                q = pl.multiple_of(at + 8 * k, 8)
                for g in range(G):
                    x = rbuf[sweep - 1, 1 - hside, 0, g, pl.ds(8 * k, 8), :]
                    st[0, g + 1, pl.ds(q, 8), :] = x
                    if g == 0:
                        st[0, G + 1, pl.ds(q, 8), :] = pltpu.roll(x, 127, 1)
                    if g == G - 1:
                        st[0, 0, pl.ds(q, 8), :] = pltpu.roll(x, 1, 1)
                    st[1, g + 1, pl.ds(q, 8), :] = rbuf[sweep - 1, 1 - hside, 1, g, pl.ds(8 * k, 8), :]

        def pair(i, _):
            t = sweep * T + 2 * i
            step(t, 0, base + sign * (2 * i + 1))
            step(t + 1, 1, base + sign * (2 * i + 2))

            @pl.when((i == 0) & has_edge)
            def _():
                exchange(psweep, pside, jnp.where(pside == 0, up, down)).start()

            return 0

        lax.fori_loop(0, T // 2, pair, 0)

        @pl.when(sweep == SWEEPS - 1)
        def _():
            lo = jnp.where(c == TILES - 1, 0, ROWS + 2 * T - TILE * (c + 1))
            hi = jnp.where(c == 0, ROWS, ROWS + 2 * T - TILE * c)
            lax.fori_loop(lax.div(lo, 8 * UN), lax.div(hi, 8 * UN), get_plain, 0)
            for k in range(TILES):
                @pl.when(c == k)
                def _():
                    for cp in out_copies(k):
                        cp.start()

        return 0

    lax.fori_loop(0, SWEEPS * TILES, tile, 0)

    for cp in raws + packs + diags:
        cp.wait_send()
    for e in range(SWEEPS - 1):
        for side in range(2):
            exchange(e, side, up).wait_send()
    for k in range(TILES):
        for cp in out_copies(k):
            cp.wait()


def solution(mesh):
    def local_run(u_tile, v_tile, w):
        dma = pltpu.SemaphoreType.DMA
        return pl.pallas_call(
            wave_kernel,
            out_shape=[jax.ShapeDtypeStruct((ROWS, COLS), F32)] * 2,
            in_specs=[pl.BlockSpec(memory_space=pl.ANY)] * 3,
            out_specs=[pl.BlockSpec(memory_space=pl.ANY)] * 2,
            scratch_shapes=[
                pltpu.VMEM((2, G + 2, R, 128), F32), pltpu.SMEM((3, 3, SWEEPS * T), F32), pltpu.VMEM((2 * G + 1, 8, 128), jnp.int32),
                pltpu.VMEM((ROWS + 2 * T, COLS), F32), pltpu.VMEM((ROWS + 2 * T, COLS), F32),
                pltpu.VMEM((2, ROWS, 128), F32), pltpu.VMEM((2, ROWS + 2 * T, 128), F32),
                pltpu.VMEM((ROWS, COLS), F32), pltpu.VMEM((ROWS, COLS), F32),
                pltpu.VMEM((SWEEPS - 1, 2, 2, G, T, 128), F32), pltpu.VMEM((SWEEPS - 1, 2, 2, G, T, 128), F32),
                dma((3,)), dma((2, 2)), dma((2, 2)), dma((TILES,)), dma((TILES,)), dma((2,)), dma((2,)),
                dma((SWEEPS - 1, 2)), dma((SWEEPS - 1, 2)), dma((2, TILES)),
            ],
            compiler_params=pltpu.CompilerParams(collective_id=0, has_side_effects=True),
        )(u_tile, v_tile, jnp.transpose(w, (1, 2, 0)))

    tile_spec = P(("ens", "row"), "col")
    return jax.shard_map(local_run, mesh=mesh, in_specs=(tile_spec, tile_spec, P()), out_specs=(tile_spec, tile_spec), check_vma=False)
```

```python
import jax
import jax.numpy as jnp
from jax import lax
from jax.experimental import pallas as pl
from jax.experimental.pallas import tpu as pltpu
from jax.sharding import PartitionSpec as P

F32 = jnp.float32
MESH = pl.DeviceIdType.MESH
ROWS, COLS = 256, 512
G = 5
T = 16
SWEEPS = 4
TILES = 3
TILE = (ROWS + 2 * T) // TILES
NG = TILE // 8
DROP = T // 8
OFF = 40
R = OFF + ROWS + OFF
VMEM_LIMIT = 55_300_000


def wave_kernel(u_hbm, v_hbm, w_hbm, now_ref, before_ref, st, w_ref, maps, uraw, vraw, pbuf, hbuf, sbuf, rbuf,
                load_sem, raw_ssem, raw_rsem, pk_ssem, pk_rsem, dg_ssem, dg_rsem, ex_ssem, ex_rsem):
    row = lax.axis_index("row")
    col = lax.axis_index("col")
    up = lax.rem(row + 3, 4)
    down = lax.rem(row + 1, 4)
    other = 1 - col

    pieces = ((0, 128), (384, 128), (128, 256))
    loads = [pltpu.make_async_copy(src.at[:, pl.ds(lo, n)], dst.at[pl.ds(T, ROWS), pl.ds(lo, n)], load_sem.at[f, k])
             for k, (lo, n) in enumerate(pieces) for f, (src, dst) in enumerate(((u_hbm, uraw), (v_hbm, vraw)))]
    loads.append(pltpu.make_async_copy(w_hbm, w_ref, load_sem.at[0, 3]))
    for cp in loads:
        cp.start()

    barrier = pltpu.get_barrier_semaphore()
    for rr, cc in ((row, other), (up, col), (down, col), (up, other), (down, other)):
        pl.semaphore_signal(barrier, inc=1, device_id={"row": rr, "col": cc}, device_id_type=MESH)
    def zero(i, _):
        for f in range(2):
            for g in range(G + 2):
                st[f, g, pl.ds(pl.multiple_of(i * 8, 8), 8), :] = jnp.zeros((8, 128), F32)
        return 0

    lax.fori_loop(0, (OFF - T) // 8, zero, 0)
    lax.fori_loop((OFF + ROWS + T) // 8, R // 8, zero, 0)

    lane = lax.broadcasted_iota(jnp.int32, (8, 128), 1)
    maps[2 * G] = lax.rem(lane, G)
    for g in range(G):
        maps[g] = lax.rem(lane * G + (g + 64), 128)
        k = lax.rem(3 * (lane + (2 * G - g - 1)), G)
        maps[G + g] = lax.div(lax.rem(128 * k + lane + 64, 128 * G), G)

    pl.semaphore_wait(barrier, 5)

    def raw_copy(f, side):
        src = (u_hbm, v_hbm)[f]
        dst = (uraw, vraw)[f]
        lo, at, to = ((0, T + ROWS, up), (ROWS - T, 0, down))[side]
        return pltpu.make_async_remote_copy(
            src_ref=src.at[pl.ds(lo, T)], dst_ref=dst.at[pl.ds(at, T)],
            send_sem=raw_ssem.at[f, side], recv_sem=raw_rsem.at[f, side],
            device_id={"row": to, "col": col}, device_id_type=MESH)

    raws = [raw_copy(f, side) for side in range(2) for f in range(2)]
    for cp in raws[2:] + raws[:2]:
        cp.start()

    cuts = [0] + [TILE * (c + 1) - T for c in range(TILES - 1)] + [ROWS]

    def packed_copy(c):
        n = cuts[c + 1] - cuts[c]
        return pltpu.make_async_remote_copy(
            src_ref=pbuf.at[:, pl.ds(cuts[c], n)], dst_ref=hbuf.at[:, pl.ds(T + cuts[c], n)],
            send_sem=pk_ssem.at[c], recv_sem=pk_rsem.at[c],
            device_id={"row": row, "col": other}, device_id_type=MESH)

    def diag_copy(side):
        lo, at, to = ((0, T + ROWS, up), (ROWS - T, 0, down))[side]
        return pltpu.make_async_remote_copy(
            src_ref=pbuf.at[:, pl.ds(lo, T)], dst_ref=hbuf.at[:, pl.ds(at, T)],
            send_sem=dg_ssem.at[side], recv_sem=dg_rsem.at[side],
            device_id={"row": to, "col": other}, device_id_type=MESH)

    packs = [packed_copy(c) for c in range(TILES)]
    diags = [diag_copy(side) for side in range(2)]

    for cp in loads[:4]:
        cp.wait()

    def pack(i, _):
        r = pl.multiple_of(i * 8, 8)
        for f, ref in ((0, uraw), (1, vraw)):
            pbuf[f, pl.ds(r, 8), :] = jnp.where(lane < 64, ref[pl.ds(r + T, 8), 0:128], ref[pl.ds(r + T, 8), 384:512])
        return 0

    lax.fori_loop((ROWS - T) // 8, ROWS // 8, pack, 0)
    lax.fori_loop(0, cuts[1] // 8, pack, 0)
    diags[1].start()
    packs[0].start()
    diags[0].start()
    lax.fori_loop(cuts[1] // 8, (ROWS - T) // 8, pack, 0)
    packs[1].start()
    packs[2].start()

    for cp in loads[4:]:
        cp.wait()

    def lanes(x, idx):
        return jnp.take_along_axis(x, idx, axis=1, mode="promise_in_bounds")

    UN = 4

    def put(i, _):
        residue = maps[2 * G]
        rows = [(pl.multiple_of((i * UN + n) * 8, 8), pl.multiple_of((i * UN + n) * 8 + (OFF - T), 8)) for n in range(UN)]
        srcs = []
        for r, q in rows:
            us = [0.25 * uraw[pl.ds(r, 8), 128 * k:128 * k + 128] for k in range(4)] + [0.25 * hbuf[0, pl.ds(r, 8), :]]
            vs = [vraw[pl.ds(r, 8), 128 * k:128 * k + 128] for k in range(4)] + [hbuf[1, pl.ds(r, 8), :]]
            srcs.append((us, [u - 0.125 * v for u, v in zip(us, vs)]))
        for g in range(G):
            idx = maps[g]
            for (r, q), pair in zip(rows, srcs):
                for f in range(2):
                    x = pair[f][4]
                    for k in range(4):
                        x = jnp.where(residue == (g + 1 + 2 * k) % G, pair[f][k], x)
                    x = lanes(x, idx)
                    st[f, g + 1, pl.ds(q, 8), :] = x
                    if f == 0 and g == 0:
                        st[0, G + 1, pl.ds(q, 8), :] = pltpu.roll(x, 127, 1)
                    if f == 0 and g == G - 1:
                        st[0, 0, pl.ds(q, 8), :] = pltpu.roll(x, 1, 1)
        return 0

    def step(t, src, start, ng):
        dst = 1 - src
        wa, wb, wc, wd, we = [0.5 * w_ref[a, b, t] for a, b in ((0, 0), (0, 1), (0, 2), (1, 0), (1, 1))]
        wa, wb, wc, wd, we = [jnp.full((8, 128), x, F32) for x in (wa, wb, wc, wd, 1.5 + we)]
        sv = st.at[:, :, pl.ds(start - 1, 8 * ng + 2)]
        for i in range(ng):
            n = [sv[src, g, pl.ds(8 * i, 8), :] for g in range(G + 2)]
            m = [sv[src, g, pl.ds(8 * i + 1, 8), :] for g in range(G + 2)]
            s = [sv[src, g, pl.ds(8 * i + 2, 8), :] for g in range(G + 2)]
            for g in range(1, G + 1):
                x = (wa * (n[g - 1] + s[g + 1]) + wc * (n[g + 1] + s[g - 1])) + (wb * (n[g] + s[g]) + wd * (m[g - 1] + m[g + 1]))
                x = x + (we * m[g] - sv[dst, g, pl.ds(8 * i + 1, 8), :])
                sv[dst, g, pl.ds(8 * i + 1, 8), :] = x
                if g == 1:
                    sv[dst, G + 1, pl.ds(8 * i + 1, 8), :] = pltpu.roll(x, 127, 1)
                if g == G:
                    sv[dst, 0, pl.ds(8 * i + 1, 8), :] = pltpu.roll(x, 1, 1)

    def exchange(e, side, to):
        return pltpu.make_async_remote_copy(
            src_ref=sbuf.at[e, side], dst_ref=rbuf.at[e, side],
            send_sem=ex_ssem.at[e, side], recv_sem=ex_rsem.at[e, side],
            device_id={"row": to, "col": col}, device_id_type=MESH)

    def get_plain(i, _):
        residue = maps[2 * G]
        for f, out in ((0, now_ref), (1, before_ref)):
            zs = []
            for n in range(UN):
                q = pl.multiple_of((i * UN + n) * 8 + OFF, 8)
                for g in range(G):
                    zs.append(st[f, g + 1, pl.ds(q, 8), :])
            for g in range(G):
                idx = maps[G + g]
                for n in range(UN):
                    zs[n * G + g] = lanes(zs[n * G + g], idx)
            for n in range(UN):
                r = pl.multiple_of((i * UN + n) * 8, 8)
                for k in range(4):
                    x = zs[n * G]
                    for g in range(1, G):
                        x = jnp.where(residue == (g + 1 + 2 * k) % G, zs[n * G + g], x)
                    out[pl.ds(r, 8), 128 * k:128 * k + 128] = x
        return 0

    def tile(it, _):
        sweep, c = lax.div(it, TILES), lax.rem(it, TILES)
        odd = lax.rem(sweep, 2)
        base = jnp.where(odd == 0, OFF - T + TILE * c, OFF + ROWS + T - TILE * (c + 1))
        sign = 2 * odd - 1

        @pl.when(it == 0)
        def _():
            raws[2].wait_recv()
            raws[3].wait_recv()
            diags[1].wait_recv()
            packs[0].wait_recv()

        @pl.when(it == 1)
        def _():
            packs[1].wait_recv()

        @pl.when(it == 2)
        def _():
            raws[0].wait_recv()
            raws[1].wait_recv()
            diags[0].wait_recv()
            packs[2].wait_recv()

        @pl.when(sweep == 0)
        def _():
            lax.fori_loop(c * (NG // UN), (c + 1) * (NG // UN), put, 0)

        prev = it - 1
        psweep, pc = lax.div(prev, TILES), lax.rem(prev, TILES)
        has_edge = (it > 0) & (pc != 1) & (psweep < SWEEPS - 1)
        pside = jnp.where(pc == 0, lax.rem(psweep, 2), 1 - lax.rem(psweep, 2))

        @pl.when(has_edge)
        def _():
            at = jnp.where(pside == 0, OFF, OFF + ROWS - T)
            for k in range(T // 8):
                q = pl.multiple_of(at + 8 * k, 8)
                for g in range(G):
                    sbuf[psweep, pside, 0, g, pl.ds(8 * k, 8), :] = st[0, g + 1, pl.ds(q, 8), :]
                    sbuf[psweep, pside, 1, g, pl.ds(8 * k, 8), :] = st[1, g + 1, pl.ds(q, 8), :]

        hside = jnp.where(c == 0, odd, 1 - odd)

        @pl.when((sweep > 0) & (c != 1))
        def _():
            exchange(sweep - 1, 1 - hside, down).wait_recv()
            at = jnp.where(hside == 0, OFF - T, OFF + ROWS)
            for k in range(T // 8):
                q = pl.multiple_of(at + 8 * k, 8)
                for g in range(G):
                    x = rbuf[sweep - 1, 1 - hside, 0, g, pl.ds(8 * k, 8), :]
                    st[0, g + 1, pl.ds(q, 8), :] = x
                    if g == 0:
                        st[0, G + 1, pl.ds(q, 8), :] = pltpu.roll(x, 127, 1)
                    if g == G - 1:
                        st[0, 0, pl.ds(q, 8), :] = pltpu.roll(x, 1, 1)
                    st[1, g + 1, pl.ds(q, 8), :] = rbuf[sweep - 1, 1 - hside, 1, g, pl.ds(8 * k, 8), :]

        def pair(i, _):
            t = sweep * T + 2 * i
            step(t, 0, base + sign * (2 * i + 1), NG)
            step(t + 1, 1, base + sign * (2 * i + 2), NG)

            @pl.when((i == 0) & has_edge)
            def _():
                exchange(psweep, pside, jnp.where(pside == 0, up, down)).start()

            return 0

        def short_pair(i, _):
            t = sweep * T + 2 * i
            low = base + (1 - odd) * 8 * DROP
            step(t, 0, low + sign * (2 * i + 1), NG - DROP)
            step(t + 1, 1, low + sign * (2 * i + 2), NG - DROP)
            return 0

        half = jnp.where(c == 0, T // 4, T // 2)
        lax.fori_loop(0, half, pair, 0)
        lax.fori_loop(half, T // 2, short_pair, 0)

        @pl.when(sweep == SWEEPS - 1)
        def _():
            lo = jnp.where(c == TILES - 1, 0, ROWS + 2 * T - TILE * (c + 1))
            hi = jnp.where(c == 0, ROWS, ROWS + 2 * T - TILE * c)
            lax.fori_loop(lax.div(lo, 8 * UN), lax.div(hi, 8 * UN), get_plain, 0)

        return 0

    lax.fori_loop(0, SWEEPS * TILES, tile, 0)

    for cp in raws + packs + diags:
        cp.wait_send()
    for e in range(SWEEPS - 1):
        for side in range(2):
            exchange(e, side, up).wait_send()


def solution(mesh):
    def local_run(u_tile, v_tile, w):
        dma = pltpu.SemaphoreType.DMA
        now, before = pl.pallas_call(
            wave_kernel,
            out_shape=[jax.ShapeDtypeStruct((ROWS, COLS), F32)] * 2,
            in_specs=[pl.BlockSpec(memory_space=pl.ANY)] * 3,
            out_specs=[pl.BlockSpec(memory_space=pltpu.VMEM)] * 2,
            scratch_shapes=[
                pltpu.VMEM((2, G + 2, R, 128), F32), pltpu.SMEM((3, 3, SWEEPS * T), F32), pltpu.VMEM((2 * G + 1, 8, 128), jnp.int32),
                pltpu.VMEM((ROWS + 2 * T, COLS), F32), pltpu.VMEM((ROWS + 2 * T, COLS), F32),
                pltpu.VMEM((2, ROWS, 128), F32), pltpu.VMEM((2, ROWS + 2 * T, 128), F32),
                pltpu.VMEM((SWEEPS - 1, 2, 2, G, T, 128), F32), pltpu.VMEM((SWEEPS - 1, 2, 2, G, T, 128), F32),
                dma((2, 4)), dma((2, 2)), dma((2, 2)), dma((TILES,)), dma((TILES,)), dma((2,)), dma((2,)),
                dma((SWEEPS - 1, 2)), dma((SWEEPS - 1, 2)),
            ],
            compiler_params=pltpu.CompilerParams(collective_id=0, has_side_effects=True, vmem_limit_bytes=VMEM_LIMIT),
        )(u_tile, v_tile, jnp.transpose(w, (1, 2, 0)))
        return 4.0 * now, 8.0 * (now - before)

    tile_spec = P(("ens", "row"), "col")
    return jax.shard_map(local_run, mesh=mesh, in_specs=(tile_spec, tile_spec, P()), out_specs=(tile_spec, tile_spec), check_vma=False)
```

```python
import jax
import jax.numpy as jnp
from jax import lax
from jax.experimental import pallas as pl
from jax.experimental.pallas import tpu as pltpu
from jax.sharding import PartitionSpec as P

F32 = jnp.float32
MESH = pl.DeviceIdType.MESH
ROWS, COLS = 256, 512
G = 5
T = 16
SWEEPS = 4
TILES = 3
TILE = (ROWS + 2 * T) // TILES
NG = TILE // 8
DROP = T // 8
RUN = 4
BLOCK = 2
OFF = 40
R = OFF + ROWS + OFF
VMEM_LIMIT = 55_300_000


def wave_kernel(u_hbm, v_hbm, w_hbm, now_ref, before_ref, st, w_ref, maps, uraw, vraw, pbuf, hbuf, sbuf, rbuf,
                load_sem, raw_ssem, raw_rsem, pk_ssem, pk_rsem, dg_ssem, dg_rsem, ex_ssem, ex_rsem):
    row = lax.axis_index("row")
    col = lax.axis_index("col")
    up = lax.rem(row + 3, 4)
    down = lax.rem(row + 1, 4)
    other = 1 - col

    pieces = ((0, 128), (384, 128), (128, 256))
    loads = [pltpu.make_async_copy(src.at[:, pl.ds(lo, n)], dst.at[pl.ds(T, ROWS), pl.ds(lo, n)], load_sem.at[f, k])
             for k, (lo, n) in enumerate(pieces) for f, (src, dst) in enumerate(((u_hbm, uraw), (v_hbm, vraw)))]
    loads.append(pltpu.make_async_copy(w_hbm, w_ref, load_sem.at[0, 3]))
    for cp in loads:
        cp.start()

    barrier = pltpu.get_barrier_semaphore()
    for rr, cc in ((row, other), (up, col), (down, col), (up, other), (down, other)):
        pl.semaphore_signal(barrier, inc=1, device_id={"row": rr, "col": cc}, device_id_type=MESH)
    def zero(i, _):
        for f in range(2):
            for g in range(G + 2):
                st[f, g, pl.ds(pl.multiple_of(i * 8, 8), 8), :] = jnp.zeros((8, 128), F32)
        return 0

    lax.fori_loop(0, (OFF - T) // 8, zero, 0)
    lax.fori_loop((OFF + ROWS + T) // 8, R // 8, zero, 0)

    lane = lax.broadcasted_iota(jnp.int32, (8, 128), 1)
    maps[2 * G] = lax.rem(lane, G)
    for g in range(G):
        maps[g] = lax.rem(lane * G + (g + 64), 128)
        k = lax.rem(3 * (lane + (2 * G - g - 1)), G)
        maps[G + g] = lax.div(lax.rem(128 * k + lane + 64, 128 * G), G)

    pl.semaphore_wait(barrier, 5)

    def raw_copy(f, side):
        src = (u_hbm, v_hbm)[f]
        dst = (uraw, vraw)[f]
        lo, at, to = ((0, T + ROWS, up), (ROWS - T, 0, down))[side]
        return pltpu.make_async_remote_copy(
            src_ref=src.at[pl.ds(lo, T)], dst_ref=dst.at[pl.ds(at, T)],
            send_sem=raw_ssem.at[f, side], recv_sem=raw_rsem.at[f, side],
            device_id={"row": to, "col": col}, device_id_type=MESH)

    raws = [raw_copy(f, side) for side in range(2) for f in range(2)]
    for cp in raws[2:] + raws[:2]:
        cp.start()

    cuts = [0] + [TILE * (c + 1) - T for c in range(TILES - 1)] + [ROWS]

    def packed_copy(c):
        n = cuts[c + 1] - cuts[c]
        return pltpu.make_async_remote_copy(
            src_ref=pbuf.at[:, pl.ds(cuts[c], n)], dst_ref=hbuf.at[:, pl.ds(T + cuts[c], n)],
            send_sem=pk_ssem.at[c], recv_sem=pk_rsem.at[c],
            device_id={"row": row, "col": other}, device_id_type=MESH)

    def diag_copy(side):
        lo, at, to = ((0, T + ROWS, up), (ROWS - T, 0, down))[side]
        return pltpu.make_async_remote_copy(
            src_ref=pbuf.at[:, pl.ds(lo, T)], dst_ref=hbuf.at[:, pl.ds(at, T)],
            send_sem=dg_ssem.at[side], recv_sem=dg_rsem.at[side],
            device_id={"row": to, "col": other}, device_id_type=MESH)

    packs = [packed_copy(c) for c in range(TILES)]
    diags = [diag_copy(side) for side in range(2)]

    for cp in loads[:4]:
        cp.wait()

    def pack(i, _):
        r = pl.multiple_of(i * 8, 8)
        for f, ref in ((0, uraw), (1, vraw)):
            pbuf[f, pl.ds(r, 8), :] = jnp.where(lane < 64, ref[pl.ds(r + T, 8), 0:128], ref[pl.ds(r + T, 8), 384:512])
        return 0

    lax.fori_loop((ROWS - T) // 8, ROWS // 8, pack, 0)
    lax.fori_loop(0, cuts[1] // 8, pack, 0)
    diags[1].start()
    packs[0].start()
    diags[0].start()
    lax.fori_loop(cuts[1] // 8, (ROWS - T) // 8, pack, 0)
    packs[1].start()
    packs[2].start()

    for cp in loads[4:]:
        cp.wait()

    def lanes(x, idx):
        return jnp.take_along_axis(x, idx, axis=1, mode="promise_in_bounds")

    UN = 4

    def put(i, _):
        residue = maps[2 * G]
        rows = [(pl.multiple_of((i * UN + n) * 8, 8), pl.multiple_of((i * UN + n) * 8 + (OFF - T), 8)) for n in range(UN)]
        srcs = []
        for r, q in rows:
            us = [0.25 * uraw[pl.ds(r, 8), 128 * k:128 * k + 128] for k in range(4)] + [0.25 * hbuf[0, pl.ds(r, 8), :]]
            vs = [vraw[pl.ds(r, 8), 128 * k:128 * k + 128] for k in range(4)] + [hbuf[1, pl.ds(r, 8), :]]
            srcs.append((us, [u - 0.125 * v for u, v in zip(us, vs)]))
        for g in range(G):
            idx = maps[g]
            for (r, q), pair in zip(rows, srcs):
                for f in range(2):
                    x = pair[f][4]
                    for k in range(4):
                        x = jnp.where(residue == (g + 1 + 2 * k) % G, pair[f][k], x)
                    x = lanes(x, idx)
                    st[f, g + 1, pl.ds(q, 8), :] = x
                    if f == 0 and g == 0:
                        st[0, G + 1, pl.ds(q, 8), :] = pltpu.roll(x, 127, 1)
                    if f == 0 and g == G - 1:
                        st[0, 0, pl.ds(q, 8), :] = pltpu.roll(x, 1, 1)
        return 0

    def run(t, start, ng, sign):
        low = min(0, sign * (RUN - 1))
        sv = st.at[:, :, pl.ds(start + (low - 1), 8 * ng + RUN + 1)]
        for k in range(RUN):
            src, dst, at = k % 2, 1 - k % 2, 1 + sign * k - low
            wa, wb, wc, wd, we = [0.5 * w_ref[a, b, t + k] for a, b in ((0, 0), (0, 1), (0, 2), (1, 0), (1, 1))]
            wa, wb, wc, wd, we = [jnp.full((G, 8 * BLOCK, 128), x, F32) for x in (wa, wb, wc, wd, 1.5 + we)]
            for i in range(0, ng, BLOCK):
                q = at + 8 * i
                n = sv[src, :, pl.ds(q - 1, 8 * BLOCK), :]
                m = sv[src, :, pl.ds(q, 8 * BLOCK), :]
                s = sv[src, :, pl.ds(q + 1, 8 * BLOCK), :]
                x = (wa * (n[0:G] + s[2:G + 2]) + wc * (n[2:G + 2] + s[0:G])) + (wb * (n[1:G + 1] + s[1:G + 1]) + wd * (m[0:G] + m[2:G + 2]))
                x = x + (we * m[1:G + 1] - sv[dst, 1:G + 1, pl.ds(q, 8 * BLOCK), :])
                sv[dst, 1:G + 1, pl.ds(q, 8 * BLOCK), :] = x
                sv[dst, G + 1, pl.ds(q, 8 * BLOCK), :] = pltpu.roll(x[0], 127, 1)
                sv[dst, 0, pl.ds(q, 8 * BLOCK), :] = pltpu.roll(x[G - 1], 1, 1)

    def exchange(e, side, to):
        return pltpu.make_async_remote_copy(
            src_ref=sbuf.at[e, side], dst_ref=rbuf.at[e, side],
            send_sem=ex_ssem.at[e, side], recv_sem=ex_rsem.at[e, side],
            device_id={"row": to, "col": col}, device_id_type=MESH)

    def get_plain(i, _):
        residue = maps[2 * G]
        for f, out in ((0, now_ref), (1, before_ref)):
            zs = []
            for n in range(UN):
                q = pl.multiple_of((i * UN + n) * 8 + OFF, 8)
                for g in range(G):
                    zs.append(st[f, g + 1, pl.ds(q, 8), :])
            for g in range(G):
                idx = maps[G + g]
                for n in range(UN):
                    zs[n * G + g] = lanes(zs[n * G + g], idx)
            for n in range(UN):
                r = pl.multiple_of((i * UN + n) * 8, 8)
                for k in range(4):
                    x = zs[n * G]
                    for g in range(1, G):
                        x = jnp.where(residue == (g + 1 + 2 * k) % G, zs[n * G + g], x)
                    out[pl.ds(r, 8), 128 * k:128 * k + 128] = x
        return 0

    def tile(it, _):
        sweep, c = lax.div(it, TILES), lax.rem(it, TILES)
        odd = lax.rem(sweep, 2)
        base = jnp.where(odd == 0, OFF - T + TILE * c, OFF + ROWS + T - TILE * (c + 1))

        @pl.when(it == 0)
        def _():
            raws[2].wait_recv()
            raws[3].wait_recv()
            diags[1].wait_recv()
            packs[0].wait_recv()

        @pl.when(it == 1)
        def _():
            packs[1].wait_recv()

        @pl.when(it == 2)
        def _():
            raws[0].wait_recv()
            raws[1].wait_recv()
            diags[0].wait_recv()
            packs[2].wait_recv()

        @pl.when(sweep == 0)
        def _():
            lax.fori_loop(c * (NG // UN), (c + 1) * (NG // UN), put, 0)

        prev = it - 1
        psweep, pc = lax.div(prev, TILES), lax.rem(prev, TILES)
        has_edge = (it > 0) & (pc != 1) & (psweep < SWEEPS - 1)
        pside = jnp.where(pc == 0, lax.rem(psweep, 2), 1 - lax.rem(psweep, 2))

        @pl.when(has_edge)
        def _():
            at = jnp.where(pside == 0, OFF, OFF + ROWS - T)
            for k in range(T // 8):
                q = pl.multiple_of(at + 8 * k, 8)
                for g in range(G):
                    sbuf[psweep, pside, 0, g, pl.ds(8 * k, 8), :] = st[0, g + 1, pl.ds(q, 8), :]
                    sbuf[psweep, pside, 1, g, pl.ds(8 * k, 8), :] = st[1, g + 1, pl.ds(q, 8), :]

        hside = jnp.where(c == 0, odd, 1 - odd)

        @pl.when((sweep > 0) & (c != 1))
        def _():
            exchange(sweep - 1, 1 - hside, down).wait_recv()
            at = jnp.where(hside == 0, OFF - T, OFF + ROWS)
            for k in range(T // 8):
                q = pl.multiple_of(at + 8 * k, 8)
                for g in range(G):
                    x = rbuf[sweep - 1, 1 - hside, 0, g, pl.ds(8 * k, 8), :]
                    st[0, g + 1, pl.ds(q, 8), :] = x
                    if g == 0:
                        st[0, G + 1, pl.ds(q, 8), :] = pltpu.roll(x, 127, 1)
                    if g == G - 1:
                        st[0, 0, pl.ds(q, 8), :] = pltpu.roll(x, 1, 1)
                    st[1, g + 1, pl.ds(q, 8), :] = rbuf[sweep - 1, 1 - hside, 1, g, pl.ds(8 * k, 8), :]

        half = jnp.where(c == 0, T // (2 * RUN), T // RUN)

        def steps(sign):
            def full(i, _):
                run(sweep * T + RUN * i, base + sign * (RUN * i + 1), NG, sign)

                @pl.when((i == 0) & has_edge)
                def _():
                    exchange(psweep, pside, jnp.where(pside == 0, up, down)).start()

                return 0

            def short(i, _):
                run(sweep * T + RUN * i, base + (8 * DROP if sign < 0 else 0) + sign * (RUN * i + 1), NG - DROP, sign)
                return 0

            lax.fori_loop(0, half, full, 0)
            lax.fori_loop(half, T // RUN, short, 0)

        @pl.when(odd == 0)
        def _():
            steps(-1)

        @pl.when(odd == 1)
        def _():
            steps(1)

        @pl.when(sweep == SWEEPS - 1)
        def _():
            lo = jnp.where(c == TILES - 1, 0, ROWS + 2 * T - TILE * (c + 1))
            hi = jnp.where(c == 0, ROWS, ROWS + 2 * T - TILE * c)
            lax.fori_loop(lax.div(lo, 8 * UN), lax.div(hi, 8 * UN), get_plain, 0)

        return 0

    lax.fori_loop(0, SWEEPS * TILES, tile, 0)

    for cp in raws + packs + diags:
        cp.wait_send()
    for e in range(SWEEPS - 1):
        for side in range(2):
            exchange(e, side, up).wait_send()


def solution(mesh):
    def local_run(u_tile, v_tile, w):
        dma = pltpu.SemaphoreType.DMA
        now, before = pl.pallas_call(
            wave_kernel,
            out_shape=[jax.ShapeDtypeStruct((ROWS, COLS), F32)] * 2,
            in_specs=[pl.BlockSpec(memory_space=pl.ANY)] * 3,
            out_specs=[pl.BlockSpec(memory_space=pltpu.VMEM)] * 2,
            scratch_shapes=[
                pltpu.VMEM((2, G + 2, R, 128), F32), pltpu.SMEM((3, 3, SWEEPS * T), F32), pltpu.VMEM((2 * G + 1, 8, 128), jnp.int32),
                pltpu.VMEM((ROWS + 2 * T, COLS), F32), pltpu.VMEM((ROWS + 2 * T, COLS), F32),
                pltpu.VMEM((2, ROWS, 128), F32), pltpu.VMEM((2, ROWS + 2 * T, 128), F32),
                pltpu.VMEM((SWEEPS - 1, 2, 2, G, T, 128), F32), pltpu.VMEM((SWEEPS - 1, 2, 2, G, T, 128), F32),
                dma((2, 4)), dma((2, 2)), dma((2, 2)), dma((TILES,)), dma((TILES,)), dma((2,)), dma((2,)),
                dma((SWEEPS - 1, 2)), dma((SWEEPS - 1, 2)),
            ],
            compiler_params=pltpu.CompilerParams(collective_id=0, has_side_effects=True, vmem_limit_bytes=VMEM_LIMIT),
        )(u_tile, v_tile, jnp.transpose(w, (1, 2, 0)))
        return 4.0 * now, 8.0 * (now - before)

    tile_spec = P(("ens", "row"), "col")
    return jax.shard_map(local_run, mesh=mesh, in_specs=(tile_spec, tile_spec, P()), out_specs=(tile_spec, tile_spec), check_vma=False)
```

```python
import jax
import jax.numpy as jnp
from jax import lax
from jax.experimental import pallas as pl
from jax.experimental.pallas import tpu as pltpu
from jax.sharding import PartitionSpec as P

F32 = jnp.float32
MESH = pl.DeviceIdType.MESH
ROWS, COLS = 256, 512
G = 5
T = 16
SWEEPS = 4
TILES = 3
TILE = (ROWS + 2 * T) // TILES
NG = TILE // 8
DROP = T // 8
RUN = 8
OFF = 32
R = 328
VMEM_LIMIT = 55_300_000


def wave_kernel(u_hbm, v_hbm, w_hbm, now_ref, before_ref, st, w_ref, maps, uraw, vraw, pbuf, hbuf, sbuf, rbuf,
                load_sem, raw_ssem, raw_rsem, pk_ssem, pk_rsem, dg_ssem, dg_rsem, ex_ssem, ex_rsem):
    row = lax.axis_index("row")
    col = lax.axis_index("col")
    up = lax.rem(row + 3, 4)
    down = lax.rem(row + 1, 4)
    other = 1 - col

    pieces = ((0, 128), (384, 128), (128, 256))
    loads = [pltpu.make_async_copy(src.at[:, pl.ds(lo, n)], dst.at[pl.ds(T, ROWS), pl.ds(lo, n)], load_sem.at[f, k])
             for k, (lo, n) in enumerate(pieces) for f, (src, dst) in enumerate(((u_hbm, uraw), (v_hbm, vraw)))]
    loads.append(pltpu.make_async_copy(w_hbm, w_ref, load_sem.at[0, 3]))
    for cp in loads:
        cp.start()

    barrier = pltpu.get_barrier_semaphore()
    for rr, cc in ((row, other), (up, col), (down, col), (up, other), (down, other)):
        pl.semaphore_signal(barrier, inc=1, device_id={"row": rr, "col": cc}, device_id_type=MESH)
    def zero(i, _):
        for f in range(2):
            for g in range(G + 2):
                st[f, g, pl.ds(pl.multiple_of(i * 8, 8), 8), :] = jnp.zeros((8, 128), F32)
        return 0

    lax.fori_loop(0, (OFF - T) // 8, zero, 0)
    lax.fori_loop((OFF + ROWS + T) // 8, R // 8, zero, 0)

    lane = lax.broadcasted_iota(jnp.int32, (8, 128), 1)
    maps[2 * G] = lax.rem(lane, G)
    for g in range(G):
        maps[g] = lax.rem(lane * G + (g + 64), 128)
        k = lax.rem(3 * (lane + (2 * G - g - 1)), G)
        maps[G + g] = lax.div(lax.rem(128 * k + lane + 64, 128 * G), G)

    pl.semaphore_wait(barrier, 5)

    def raw_copy(f, side):
        src = (u_hbm, v_hbm)[f]
        dst = (uraw, vraw)[f]
        lo, at, to = ((0, T + ROWS, up), (ROWS - T, 0, down))[side]
        return pltpu.make_async_remote_copy(
            src_ref=src.at[pl.ds(lo, T)], dst_ref=dst.at[pl.ds(at, T)],
            send_sem=raw_ssem.at[f, side], recv_sem=raw_rsem.at[f, side],
            device_id={"row": to, "col": col}, device_id_type=MESH)

    raws = [raw_copy(f, side) for side in range(2) for f in range(2)]
    for cp in raws[2:] + raws[:2]:
        cp.start()

    cuts = [0] + [TILE * (c + 1) - T for c in range(TILES - 1)] + [ROWS]

    def packed_copy(c):
        n = cuts[c + 1] - cuts[c]
        return pltpu.make_async_remote_copy(
            src_ref=pbuf.at[:, pl.ds(cuts[c], n)], dst_ref=hbuf.at[:, pl.ds(T + cuts[c], n)],
            send_sem=pk_ssem.at[c], recv_sem=pk_rsem.at[c],
            device_id={"row": row, "col": other}, device_id_type=MESH)

    def diag_copy(side):
        lo, at, to = ((0, T + ROWS, up), (ROWS - T, 0, down))[side]
        return pltpu.make_async_remote_copy(
            src_ref=pbuf.at[:, pl.ds(lo, T)], dst_ref=hbuf.at[:, pl.ds(at, T)],
            send_sem=dg_ssem.at[side], recv_sem=dg_rsem.at[side],
            device_id={"row": to, "col": other}, device_id_type=MESH)

    packs = [packed_copy(c) for c in range(TILES)]
    diags = [diag_copy(side) for side in range(2)]

    for cp in loads[:4]:
        cp.wait()

    def pack(i, _):
        r = pl.multiple_of(i * 8, 8)
        for f, ref in ((0, uraw), (1, vraw)):
            pbuf[f, pl.ds(r, 8), :] = jnp.where(lane < 64, ref[pl.ds(r + T, 8), 0:128], ref[pl.ds(r + T, 8), 384:512])
        return 0

    lax.fori_loop((ROWS - T) // 8, ROWS // 8, pack, 0)
    lax.fori_loop(0, cuts[1] // 8, pack, 0)
    diags[1].start()
    packs[0].start()
    diags[0].start()
    lax.fori_loop(cuts[1] // 8, (ROWS - T) // 8, pack, 0)
    packs[1].start()
    packs[2].start()

    for cp in loads[4:]:
        cp.wait()

    def lanes(x, idx):
        return jnp.take_along_axis(x, idx, axis=1, mode="promise_in_bounds")

    UN = 4

    def put(i, _):
        residue = maps[2 * G]
        rows = [(pl.multiple_of((i * UN + n) * 8, 8), pl.multiple_of((i * UN + n) * 8 + (OFF - T), 8)) for n in range(UN)]
        srcs = []
        for r, q in rows:
            us = [0.25 * uraw[pl.ds(r, 8), 128 * k:128 * k + 128] for k in range(4)] + [0.25 * hbuf[0, pl.ds(r, 8), :]]
            vs = [vraw[pl.ds(r, 8), 128 * k:128 * k + 128] for k in range(4)] + [hbuf[1, pl.ds(r, 8), :]]
            srcs.append((us, [u - 0.125 * v for u, v in zip(us, vs)]))
        for g in range(G):
            idx = maps[g]
            for (r, q), pair in zip(rows, srcs):
                for f in range(2):
                    x = pair[f][4]
                    for k in range(4):
                        x = jnp.where(residue == (g + 1 + 2 * k) % G, pair[f][k], x)
                    x = lanes(x, idx)
                    st[f, g + 1, pl.ds(q, 8), :] = x
                    if f == 0 and g == 0:
                        st[0, G + 1, pl.ds(q, 8), :] = pltpu.roll(x, 127, 1)
                    if f == 0 and g == G - 1:
                        st[0, 0, pl.ds(q, 8), :] = pltpu.roll(x, 1, 1)
        return 0

    def run(t, start, ng, sign):
        low = min(0, sign * (RUN - 1))
        rows = 32 if ng % 4 == 0 else 16
        sv = st.at[:, :, pl.ds(start + (low - 1), 8 * ng + RUN + 1)]
        for k in range(RUN):
            src, dst, at = k % 2, 1 - k % 2, 1 + sign * k - low
            wa, wb, wc, wd, we = [0.5 * w_ref[a, b, t + k] for a, b in ((0, 0), (0, 1), (0, 2), (1, 0), (1, 1))]
            wa, wb, wc, wd, we = [jnp.full((G, rows, 128), x, F32) for x in (wa, wb, wc, wd, 1.5 + we)]
            for q in range(at, at + 8 * ng, rows):
                n = sv[src, :, pl.ds(q - 1, rows), :]
                m = sv[src, :, pl.ds(q, rows), :]
                s = sv[src, :, pl.ds(q + 1, rows), :]
                x = (wa * (n[0:G] + s[2:G + 2]) + wc * (n[2:G + 2] + s[0:G])) + (wb * (n[1:G + 1] + s[1:G + 1]) + wd * (m[0:G] + m[2:G + 2]))
                x = x + (we * m[1:G + 1] - sv[dst, 1:G + 1, pl.ds(q, rows), :])
                sv[dst, 1:G + 1, pl.ds(q, rows), :] = x
                sv[dst, G + 1, pl.ds(q, rows), :] = pltpu.roll(x[0], 127, 1)
                sv[dst, 0, pl.ds(q, rows), :] = pltpu.roll(x[G - 1], 1, 1)

    def exchange(e, side, to, late):
        src = sbuf.at[e] if late else st.at[:, pl.ds(1, G), pl.ds(jnp.where(side == 0, OFF, OFF + ROWS - T), T)]
        return pltpu.make_async_remote_copy(
            src_ref=src, dst_ref=rbuf.at[e, side],
            send_sem=ex_ssem.at[e, side], recv_sem=ex_rsem.at[e, side],
            device_id={"row": to, "col": col}, device_id_type=MESH)

    def get_plain(i, _):
        residue = maps[2 * G]
        outs = [(f, n) for f in range(2) for n in range(2)]
        zs = {}
        for g in range(G):
            idx = maps[G + g]
            for f, n in outs:
                q = pl.multiple_of((i * 2 + n) * 8 + OFF, 8)
                zs[f, n, g] = lanes(st[f, g + 1, pl.ds(q, 8), :], idx)
        for f, n in outs:
            r = pl.multiple_of((i * 2 + n) * 8, 8)
            for k in range(4):
                x = zs[f, n, 0]
                for g in range(1, G):
                    x = jnp.where(residue == (g + 1 + 2 * k) % G, zs[f, n, g], x)
                (now_ref, before_ref)[f][pl.ds(r, 8), 128 * k:128 * k + 128] = x
        return 0

    def tile(it, _):
        sweep, c = lax.div(it, TILES), lax.rem(it, TILES)
        odd = lax.rem(sweep, 2)
        base = jnp.where(odd == 0, OFF - T + TILE * c, OFF + ROWS + T - TILE * (c + 1))

        @pl.when(it == 0)
        def _():
            raws[2].wait_recv()
            raws[3].wait_recv()
            diags[1].wait_recv()
            packs[0].wait_recv()

        @pl.when(it == 1)
        def _():
            packs[1].wait_recv()

        @pl.when(it == 2)
        def _():
            raws[0].wait_recv()
            raws[1].wait_recv()
            diags[0].wait_recv()
            packs[2].wait_recv()

        @pl.when(sweep == 0)
        def _():
            lax.fori_loop(c * (NG // UN), (c + 1) * (NG // UN), put, 0)

        first = odd
        last = 1 - odd
        to_first = jnp.where(odd == 0, up, down)
        to_last = jnp.where(odd == 0, down, up)

        def put_rows(side):
            at = jnp.where(side == 0, OFF - T, OFF + ROWS)
            for k in range(T // 8):
                q = pl.multiple_of(at + 8 * k, 8)
                for g in range(G):
                    x = rbuf[sweep - 1, 1 - side, 0, g, pl.ds(8 * k, 8), :]
                    st[0, g + 1, pl.ds(q, 8), :] = x
                    if g == 0:
                        st[0, G + 1, pl.ds(q, 8), :] = pltpu.roll(x, 127, 1)
                    if g == G - 1:
                        st[0, 0, pl.ds(q, 8), :] = pltpu.roll(x, 1, 1)
                    st[1, g + 1, pl.ds(q, 8), :] = rbuf[sweep - 1, 1 - side, 1, g, pl.ds(8 * k, 8), :]

        @pl.when((sweep > 0) & (c == 0))
        def _():
            at = jnp.where(first == 0, OFF, OFF + ROWS - T)
            for k in range(T // 8):
                q = pl.multiple_of(at + 8 * k, 8)
                for f in range(2):
                    for g in range(G):
                        sbuf[sweep - 1, f, g, pl.ds(8 * k, 8), :] = st[f, g + 1, pl.ds(q, 8), :]
            exchange(sweep - 1, 1 - first, up, True).wait_recv()
            put_rows(first)
            exchange(sweep - 1, first, to_first, True).start()

        @pl.when((sweep < SWEEPS - 1) & (c == 1))
        def _():
            exchange(sweep, first, to_first, False).start()

        @pl.when((sweep > 0) & (c == TILES - 1))
        def _():
            exchange(sweep - 1, last, up, False).wait_send()
            exchange(sweep - 1, 1 - last, up, True).wait_recv()
            put_rows(last)

        half = jnp.where(c == 0, T // (2 * RUN), T // RUN)

        def steps(sign):
            def full(i, _):
                run(sweep * T + RUN * i, base + sign * (RUN * i + 1), NG, sign)
                return 0

            def short(i, _):
                run(sweep * T + RUN * i, base + (8 * DROP if sign < 0 else 0) + sign * (RUN * i + 1), NG - DROP, sign)
                return 0

            lax.fori_loop(0, half, full, 0)
            lax.fori_loop(half, T // RUN, short, 0)

        @pl.when(odd == 0)
        def _():
            steps(-1)

        @pl.when(odd == 1)
        def _():
            steps(1)

        @pl.when(sweep == SWEEPS - 1)
        def _():
            lo = jnp.where(c == TILES - 1, 0, ROWS + 2 * T - TILE * (c + 1))
            hi = jnp.where(c == 0, ROWS, ROWS + 2 * T - TILE * c)
            lax.fori_loop(lax.div(lo, 16), lax.div(hi, 16), get_plain, 0)

        return 0

    lax.fori_loop(0, SWEEPS * TILES, tile, 0)

    for cp in raws + packs + diags:
        cp.wait_send()
    for e in range(SWEEPS - 1):
        exchange(e, (e + 1) % 2, up, True).wait_send()


def solution(mesh):
    def local_run(u_tile, v_tile, w):
        dma = pltpu.SemaphoreType.DMA
        now, before = pl.pallas_call(
            wave_kernel,
            out_shape=[jax.ShapeDtypeStruct((ROWS, COLS), F32)] * 2,
            in_specs=[pl.BlockSpec(memory_space=pl.ANY)] * 3,
            out_specs=[pl.BlockSpec(memory_space=pltpu.VMEM)] * 2,
            scratch_shapes=[
                pltpu.VMEM((2, G + 2, R, 128), F32), pltpu.SMEM((3, 3, SWEEPS * T), F32), pltpu.VMEM((2 * G + 1, 8, 128), jnp.int32),
                pltpu.VMEM((ROWS + 2 * T, COLS), F32), pltpu.VMEM((ROWS + 2 * T, COLS), F32),
                pltpu.VMEM((2, ROWS, 128), F32), pltpu.VMEM((2, ROWS + 2 * T, 128), F32),
                pltpu.VMEM((SWEEPS - 1, 2, G, T, 128), F32), pltpu.VMEM((SWEEPS - 1, 2, 2, G, T, 128), F32),
                dma((2, 4)), dma((2, 2)), dma((2, 2)), dma((TILES,)), dma((TILES,)), dma((2,)), dma((2,)),
                dma((SWEEPS - 1, 2)), dma((SWEEPS - 1, 2)),
            ],
            compiler_params=pltpu.CompilerParams(collective_id=0, has_side_effects=True, vmem_limit_bytes=VMEM_LIMIT),
        )(u_tile, v_tile, jnp.transpose(w, (1, 2, 0)))
        return 4.0 * now, 8.0 * (now - before)

    tile_spec = P(("ens", "row"), "col")
    return jax.shard_map(local_run, mesh=mesh, in_specs=(tile_spec, tile_spec, P()), out_specs=(tile_spec, tile_spec), check_vma=False)
```

```python
import jax
import jax.numpy as jnp
from jax import lax
from jax.experimental import pallas as pl
from jax.experimental.pallas import tpu as pltpu
from jax.sharding import PartitionSpec as P

F32 = jnp.float32
MESH = pl.DeviceIdType.MESH
ROWS, COLS = 256, 512
G = 5
T = 16
SWEEPS = 4
TILES = 3
TILE = (ROWS + 2 * T) // TILES
NG = TILE // 8
DROP = T // 8
RUN = 8
OFF = 32
R = 328
VMEM_LIMIT = 55_300_000


def wave_kernel(u_hbm, v_hbm, w_hbm, now_ref, before_ref, st, w_ref, maps, uraw, vraw, pbuf, hbuf, zbuf, sbuf, rbuf,
                load_sem, raw_ssem, raw_rsem, pk_ssem, pk_rsem, dg_ssem, dg_rsem, ex_ssem, ex_rsem):
    row = lax.axis_index("row")
    col = lax.axis_index("col")
    up = lax.rem(row + 3, 4)
    down = lax.rem(row + 1, 4)
    other = 1 - col

    pieces = ((0, 128), (384, 128), (128, 256))
    loads = [pltpu.make_async_copy(src.at[:, pl.ds(lo, n)], dst.at[pl.ds(T, ROWS), pl.ds(lo, n)], load_sem.at[f, k])
             for k, (lo, n) in enumerate(pieces) for f, (src, dst) in enumerate(((u_hbm, uraw), (v_hbm, vraw)))]
    loads.append(pltpu.make_async_copy(w_hbm, w_ref, load_sem.at[0, 3]))
    for cp in loads:
        cp.start()

    barrier = pltpu.get_barrier_semaphore()
    for rr, cc in ((row, other), (up, col), (down, col), (up, other), (down, other)):
        pl.semaphore_signal(barrier, inc=1, device_id={"row": rr, "col": cc}, device_id_type=MESH)
    def zero(i, _):
        for f in range(2):
            for g in range(G + 2):
                st[f, g, pl.ds(pl.multiple_of(i * 8, 8), 8), :] = jnp.zeros((8, 128), F32)
        return 0

    lax.fori_loop(0, (OFF - T) // 8, zero, 0)
    lax.fori_loop((OFF + ROWS + T) // 8, R // 8, zero, 0)

    lane = lax.broadcasted_iota(jnp.int32, (8, 128), 1)
    maps[2 * G] = lax.rem(lane, G)
    for g in range(G):
        maps[g] = lax.rem(lane * G + (g + 64), 128)
        k = lax.rem(3 * (lane + (2 * G - g - 1)), G)
        maps[G + g] = lax.div(lax.rem(128 * k + lane + 64, 128 * G), G)

    pl.semaphore_wait(barrier, 5)

    def raw_copy(f, side):
        src = (u_hbm, v_hbm)[f]
        dst = (uraw, vraw)[f]
        lo, at, to = ((0, T + ROWS, up), (ROWS - T, 0, down))[side]
        return pltpu.make_async_remote_copy(
            src_ref=src.at[pl.ds(lo, T)], dst_ref=dst.at[pl.ds(at, T)],
            send_sem=raw_ssem.at[f, side], recv_sem=raw_rsem.at[f, side],
            device_id={"row": to, "col": col}, device_id_type=MESH)

    raws = [raw_copy(f, side) for side in range(2) for f in range(2)]
    for cp in raws[2:] + raws[:2]:
        cp.start()

    cuts = [0] + [TILE * (c + 1) - T for c in range(TILES - 1)] + [ROWS]

    def packed_copy(c):
        n = cuts[c + 1] - cuts[c]
        return pltpu.make_async_remote_copy(
            src_ref=pbuf.at[:, pl.ds(cuts[c], n)], dst_ref=hbuf.at[:, pl.ds(T + cuts[c], n)],
            send_sem=pk_ssem.at[c], recv_sem=pk_rsem.at[c],
            device_id={"row": row, "col": other}, device_id_type=MESH)

    def diag_copy(side):
        lo, at, to = ((0, T + ROWS, up), (ROWS - T, 0, down))[side]
        return pltpu.make_async_remote_copy(
            src_ref=pbuf.at[:, pl.ds(lo, T)], dst_ref=hbuf.at[:, pl.ds(at, T)],
            send_sem=dg_ssem.at[side], recv_sem=dg_rsem.at[side],
            device_id={"row": to, "col": other}, device_id_type=MESH)

    packs = [packed_copy(c) for c in range(TILES)]
    diags = [diag_copy(side) for side in range(2)]

    for cp in loads[:4]:
        cp.wait()

    def pack(i, _):
        r = pl.multiple_of(i * 8, 8)
        for f, ref in ((0, uraw), (1, vraw)):
            pbuf[f, pl.ds(r, 8), :] = jnp.where(lane < 64, ref[pl.ds(r + T, 8), 0:128], ref[pl.ds(r + T, 8), 384:512])
        return 0

    lax.fori_loop((ROWS - T) // 8, ROWS // 8, pack, 0)
    lax.fori_loop(0, cuts[1] // 8, pack, 0)
    diags[1].start()
    packs[0].start()
    diags[0].start()
    lax.fori_loop(cuts[1] // 8, (ROWS - T) // 8, pack, 0)
    packs[1].start()
    packs[2].start()

    for cp in loads[4:]:
        cp.wait()

    def lanes(x, idx):
        return jnp.take_along_axis(x, idx, axis=1, mode="promise_in_bounds")

    def put(c):
        residue = maps[2 * G]
        for g in range(G):
            idx = maps[g]
            for n in range(NG):
                r = pl.multiple_of(c * TILE + 8 * n, 8)
                q = pl.multiple_of(c * TILE + (OFF - T + 8 * n), 8)
                u, v = hbuf[0, pl.ds(r, 8), :], hbuf[1, pl.ds(r, 8), :]
                for k in range(4):
                    mask = residue == (g + 1 + 2 * k) % G
                    u = jnp.where(mask, uraw[pl.ds(r, 8), 128 * k:128 * k + 128], u)
                    v = jnp.where(mask, vraw[pl.ds(r, 8), 128 * k:128 * k + 128], v)
                x = 0.25 * lanes(u, idx)
                st[0, g + 1, pl.ds(q, 8), :] = x
                st[1, g + 1, pl.ds(q, 8), :] = x - 0.125 * lanes(v, idx)
        for n in range(NG):
            q = pl.multiple_of(c * TILE + (OFF - T + 8 * n), 8)
            st[0, G + 1, pl.ds(q, 8), :] = pltpu.roll(st[0, 1, pl.ds(q, 8), :], 127, 1)
            st[0, 0, pl.ds(q, 8), :] = pltpu.roll(st[0, G, pl.ds(q, 8), :], 1, 1)

    def run(t, start, ng, sign):
        low = min(0, sign * (RUN - 1))
        rows = 16
        sv = st.at[:, :, pl.ds(start + (low - 1), 8 * ng + RUN + 1)]
        for k in range(RUN):
            src, dst, at = k % 2, 1 - k % 2, 1 + sign * k - low
            wa, wb, wc, wd, we = [0.5 * w_ref[a, b, t + k] for a, b in ((0, 0), (0, 1), (0, 2), (1, 0), (1, 1))]
            wa, wb, wc, wd, we = [jnp.full((G, rows, 128), x, F32) for x in (wa, wb, wc, wd, 1.5 + we)]
            for q in range(at, at + 8 * ng, rows):
                n = sv[src, :, pl.ds(q - 1, rows), :]
                m = sv[src, :, pl.ds(q, rows), :]
                s = sv[src, :, pl.ds(q + 1, rows), :]
                x = (wa * (n[0:G] + s[2:G + 2]) + wc * (n[2:G + 2] + s[0:G])) + (wb * (n[1:G + 1] + s[1:G + 1]) + wd * (m[0:G] + m[2:G + 2]))
                x = x + (we * m[1:G + 1] - sv[dst, 1:G + 1, pl.ds(q, rows), :])
                sv[dst, 1:G + 1, pl.ds(q, rows), :] = x
                sv[dst, G + 1, pl.ds(q, rows), :] = pltpu.roll(x[0], 127, 1)
                sv[dst, 0, pl.ds(q, rows), :] = pltpu.roll(x[G - 1], 1, 1)

    def exchange(e, side, to, late):
        src = sbuf.at[e] if late else st.at[:, pl.ds(1, G), pl.ds(jnp.where(side == 0, OFF, OFF + ROWS - T), T)]
        return pltpu.make_async_remote_copy(
            src_ref=src, dst_ref=rbuf.at[e, side],
            send_sem=ex_ssem.at[e, side], recv_sem=ex_rsem.at[e, side],
            device_id={"row": to, "col": col}, device_id_type=MESH)

    def get(lo):
        for g in range(G):
            idx = maps[G + g]
            for n in range(NG):
                q = pl.multiple_of(lo + (OFF + 8 * n), 8)
                for f in range(2):
                    zbuf[f, g, 8 * n:8 * n + 8, :] = lanes(st[f, g + 1, pl.ds(q, 8), :], idx)
        residue = maps[2 * G]
        for n in range(NG):
            r = pl.multiple_of(lo + 8 * n, 8)
            for f, out in ((0, now_ref), (1, before_ref)):
                for k in range(4):
                    x = zbuf[f, 0, 8 * n:8 * n + 8, :]
                    for g in range(1, G):
                        x = jnp.where(residue == (g + 1 + 2 * k) % G, zbuf[f, g, 8 * n:8 * n + 8, :], x)
                    out[pl.ds(r, 8), 128 * k:128 * k + 128] = x

    def tile(it, _):
        sweep, c = lax.div(it, TILES), lax.rem(it, TILES)
        odd = lax.rem(sweep, 2)
        base = jnp.where(odd == 0, OFF - T + TILE * c, OFF + ROWS + T - TILE * (c + 1))

        @pl.when(it == 0)
        def _():
            raws[2].wait_recv()
            raws[3].wait_recv()
            diags[1].wait_recv()
            packs[0].wait_recv()

        @pl.when(it == 1)
        def _():
            packs[1].wait_recv()

        @pl.when(it == 2)
        def _():
            raws[0].wait_recv()
            raws[1].wait_recv()
            diags[0].wait_recv()
            packs[2].wait_recv()

        @pl.when(sweep == 0)
        def _():
            put(c)

        first = odd
        last = 1 - odd
        to_first = jnp.where(odd == 0, up, down)
        to_last = jnp.where(odd == 0, down, up)

        def put_rows(side):
            at = jnp.where(side == 0, OFF - T, OFF + ROWS)
            for k in range(T // 8):
                q = pl.multiple_of(at + 8 * k, 8)
                for g in range(G):
                    x = rbuf[sweep - 1, 1 - side, 0, g, pl.ds(8 * k, 8), :]
                    st[0, g + 1, pl.ds(q, 8), :] = x
                    if g == 0:
                        st[0, G + 1, pl.ds(q, 8), :] = pltpu.roll(x, 127, 1)
                    if g == G - 1:
                        st[0, 0, pl.ds(q, 8), :] = pltpu.roll(x, 1, 1)
                    st[1, g + 1, pl.ds(q, 8), :] = rbuf[sweep - 1, 1 - side, 1, g, pl.ds(8 * k, 8), :]

        @pl.when((sweep > 0) & (c == 0))
        def _():
            at = jnp.where(first == 0, OFF, OFF + ROWS - T)
            for k in range(T // 8):
                q = pl.multiple_of(at + 8 * k, 8)
                for f in range(2):
                    for g in range(G):
                        sbuf[sweep - 1, f, g, pl.ds(8 * k, 8), :] = st[f, g + 1, pl.ds(q, 8), :]
            exchange(sweep - 1, 1 - first, up, True).wait_recv()
            put_rows(first)
            exchange(sweep - 1, first, to_first, True).start()

        @pl.when((sweep < SWEEPS - 1) & (c == 1))
        def _():
            exchange(sweep, first, to_first, False).start()

        @pl.when((sweep > 0) & (c == TILES - 1))
        def _():
            exchange(sweep - 1, last, up, False).wait_send()
            exchange(sweep - 1, 1 - last, up, True).wait_recv()
            put_rows(last)

        half = jnp.where(c == 0, T // (2 * RUN), T // RUN)

        def steps(sign):
            def full(i, _):
                run(sweep * T + RUN * i, base + sign * (RUN * i + 1), NG, sign)
                return 0

            def short(i, _):
                run(sweep * T + RUN * i, base + (8 * DROP if sign < 0 else 0) + sign * (RUN * i + 1), NG - DROP, sign)
                return 0

            lax.fori_loop(0, half, full, 0)
            lax.fori_loop(half, T // RUN, short, 0)

        @pl.when(odd == 0)
        def _():
            steps(-1)

        @pl.when(odd == 1)
        def _():
            steps(1)

        @pl.when(sweep == SWEEPS - 1)
        def _():
            get(pl.multiple_of(jnp.where(c == 0, ROWS - TILE, (TILES - 1 - c) * TILE), 8))

        return 0

    lax.fori_loop(0, SWEEPS * TILES, tile, 0)

    for cp in raws + packs + diags:
        cp.wait_send()
    for e in range(SWEEPS - 1):
        exchange(e, (e + 1) % 2, up, True).wait_send()


def solution(mesh):
    def local_run(u_tile, v_tile, w):
        dma = pltpu.SemaphoreType.DMA
        now, before = pl.pallas_call(
            wave_kernel,
            out_shape=[jax.ShapeDtypeStruct((ROWS, COLS), F32)] * 2,
            in_specs=[pl.BlockSpec(memory_space=pl.ANY)] * 3,
            out_specs=[pl.BlockSpec(memory_space=pltpu.VMEM)] * 2,
            scratch_shapes=[
                pltpu.VMEM((2, G + 2, R, 128), F32), pltpu.SMEM((3, 3, SWEEPS * T), F32), pltpu.VMEM((2 * G + 1, 8, 128), jnp.int32),
                pltpu.VMEM((ROWS + 2 * T, COLS), F32), pltpu.VMEM((ROWS + 2 * T, COLS), F32),
                pltpu.VMEM((2, ROWS, 128), F32), pltpu.VMEM((2, ROWS + 2 * T, 128), F32), pltpu.VMEM((2, G, TILE, 128), F32),
                pltpu.VMEM((SWEEPS - 1, 2, G, T, 128), F32), pltpu.VMEM((SWEEPS - 1, 2, 2, G, T, 128), F32),
                dma((2, 4)), dma((2, 2)), dma((2, 2)), dma((TILES,)), dma((TILES,)), dma((2,)), dma((2,)),
                dma((SWEEPS - 1, 2)), dma((SWEEPS - 1, 2)),
            ],
            compiler_params=pltpu.CompilerParams(collective_id=0, has_side_effects=True, vmem_limit_bytes=VMEM_LIMIT),
        )(u_tile, v_tile, pltpu.with_memory_space_constraint(jnp.transpose(w, (1, 2, 0)), pltpu.HBM))
        return 4.0 * now, 8.0 * (now - before)

    tile_spec = P(("ens", "row"), "col")
    return jax.shard_map(local_run, mesh=mesh, in_specs=(tile_spec, tile_spec, P()), out_specs=(tile_spec, tile_spec), check_vma=False)
```

```python
import jax
import jax.numpy as jnp
from jax import lax
from jax.experimental import pallas as pl
from jax.experimental.pallas import tpu as pltpu
from jax.sharding import PartitionSpec as P

F32 = jnp.float32
MESH = pl.DeviceIdType.MESH
ROWS, COLS = 256, 512
G = 5
T = 16
SWEEPS = 4
TILES = 3
TILE = (ROWS + 2 * T) // TILES
NG = TILE // 8
BLOCK = 4
OFF = 32
R = 328
VMEM_LIMIT = 55_300_000


def wave_kernel(u_hbm, v_hbm, w_hbm, now_ref, before_ref, st, w_ref, maps, uraw, vraw, pbuf, hbuf, zbuf, sbuf, rbuf,
                load_sem, raw_ssem, raw_rsem, pk_ssem, pk_rsem, dg_ssem, dg_rsem, ex_ssem, ex_rsem):
    row = lax.axis_index("row")
    col = lax.axis_index("col")
    up = lax.rem(row + 3, 4)
    down = lax.rem(row + 1, 4)
    other = 1 - col

    barrier = pltpu.get_barrier_semaphore()
    for rr, cc in ((row, other), (up, col), (down, col), (up, other), (down, other)):
        pl.semaphore_signal(barrier, inc=1, device_id={"row": rr, "col": cc}, device_id_type=MESH)

    cuts = [0] + [TILE * (c + 1) - T for c in range(TILES - 1)] + [ROWS]

    pieces = [(lo, n, at, 128) for lo, n in ((ROWS - T, T), (0, cuts[1]), (cuts[1], ROWS - T - cuts[1])) for at in (0, COLS - 128)]
    pieces.append((0, ROWS, 128, COLS - 256))
    loads = [pltpu.make_async_copy(src.at[pl.ds(lo, n), pl.ds(at, m)], dst.at[pl.ds(T + lo, n), pl.ds(at, m)], load_sem.at[f, k])
             for k, (lo, n, at, m) in enumerate(pieces) for f, (src, dst) in enumerate(((u_hbm, uraw), (v_hbm, vraw)))]
    loads.append(pltpu.make_async_copy(w_hbm, w_ref, load_sem.at[0, len(pieces)]))
    for cp in loads:
        cp.start()

    def zero(i, _):
        for f in range(2):
            for g in range(G + 2):
                st[f, g, pl.ds(pl.multiple_of(i * 8, 8), 8), :] = jnp.zeros((8, 128), F32)
        return 0

    lax.fori_loop(0, (OFF - T) // 8, zero, 0)
    lax.fori_loop((OFF + ROWS + T) // 8, R // 8, zero, 0)

    lane = lax.broadcasted_iota(jnp.int32, (8, 128), 1)
    maps[2 * G] = lax.rem(lane, G)
    for g in range(G):
        maps[g] = lax.rem(lane * G + (g + 64), 128)
        k = lax.rem(3 * (lane + (2 * G - g - 1)), G)
        maps[G + g] = lax.div(lax.rem(128 * k + lane + 64, 128 * G), G)

    pl.semaphore_wait(barrier, 5)

    def raw_copy(f, side):
        src = (u_hbm, v_hbm)[f]
        dst = (uraw, vraw)[f]
        lo, at, to = ((0, T + ROWS, up), (ROWS - T, 0, down))[side]
        return pltpu.make_async_remote_copy(
            src_ref=src.at[pl.ds(lo, T)], dst_ref=dst.at[pl.ds(at, T)],
            send_sem=raw_ssem.at[f, side], recv_sem=raw_rsem.at[f, side],
            device_id={"row": to, "col": col}, device_id_type=MESH)

    raws = [raw_copy(f, side) for side in range(2) for f in range(2)]
    for cp in raws[2:] + raws[:2]:
        cp.start()

    def packed_copy(c):
        n = cuts[c + 1] - cuts[c]
        return pltpu.make_async_remote_copy(
            src_ref=pbuf.at[:, pl.ds(cuts[c], n)], dst_ref=hbuf.at[:, pl.ds(T + cuts[c], n)],
            send_sem=pk_ssem.at[c], recv_sem=pk_rsem.at[c],
            device_id={"row": row, "col": other}, device_id_type=MESH)

    def diag_copy(side):
        lo, at, to = ((0, T + ROWS, up), (ROWS - T, 0, down))[side]
        return pltpu.make_async_remote_copy(
            src_ref=pbuf.at[:, pl.ds(lo, T)], dst_ref=hbuf.at[:, pl.ds(at, T)],
            send_sem=dg_ssem.at[side], recv_sem=dg_rsem.at[side],
            device_id={"row": to, "col": other}, device_id_type=MESH)

    packs = [packed_copy(c) for c in range(TILES)]
    diags = [diag_copy(side) for side in range(2)]

    for cp in loads[:8]:
        cp.wait()

    def pack(i, _):
        r = pl.multiple_of(i * 8, 8)
        for f, ref in ((0, uraw), (1, vraw)):
            pbuf[f, pl.ds(r, 8), :] = jnp.where(lane < 64, ref[pl.ds(r + T, 8), 0:128], ref[pl.ds(r + T, 8), 384:512])
        return 0

    lax.fori_loop((ROWS - T) // 8, ROWS // 8, pack, 0)
    lax.fori_loop(0, cuts[1] // 8, pack, 0)
    diags[1].start()
    packs[0].start()
    diags[0].start()
    for cp in loads[8:12]:
        cp.wait()
    lax.fori_loop(cuts[1] // 8, (ROWS - T) // 8, pack, 0)
    packs[1].start()
    packs[2].start()

    for cp in loads[12:]:
        cp.wait()

    def lanes(x, idx):
        return jnp.take_along_axis(x, idx, axis=1, mode="promise_in_bounds")

    def put(c):
        residue = maps[2 * G]
        for g in range(G):
            idx = maps[g]
            for n in range(NG):
                r = pl.multiple_of(c * TILE + 8 * n, 8)
                q = pl.multiple_of(c * TILE + (OFF - T + 8 * n), 8)
                u, v = hbuf[0, pl.ds(r, 8), :], hbuf[1, pl.ds(r, 8), :]
                for k in range(4):
                    mask = residue == (g + 1 + 2 * k) % G
                    u = jnp.where(mask, uraw[pl.ds(r, 8), 128 * k:128 * k + 128], u)
                    v = jnp.where(mask, vraw[pl.ds(r, 8), 128 * k:128 * k + 128], v)
                x = 0.25 * lanes(u, idx)
                st[0, g + 1, pl.ds(q, 8), :] = x
                st[1, g + 1, pl.ds(q, 8), :] = x - 0.125 * lanes(v, idx)
        for n in range(NG):
            q = pl.multiple_of(c * TILE + (OFF - T + 8 * n), 8)
            st[0, G + 1, pl.ds(q, 8), :] = pltpu.roll(st[0, 1, pl.ds(q, 8), :], 127, 1)
            st[0, 0, pl.ds(q, 8), :] = pltpu.roll(st[0, G, pl.ds(q, 8), :], 1, 1)

    def run(t, base, sign, first):
        drops = [2 * (k + 1) // 8 if first else 0 for k in range(T)]
        tops = [sign * (k + 1) + (8 * drops[k] if sign < 0 else 0) for k in range(T)]
        low = min(tops) - 1
        high = max(top + TILE - 8 * drop for top, drop in zip(tops, drops)) + 1
        sv = st.at[:, :, pl.ds(base + low, high - low)]
        for k in range(T):
            src, dst = k % 2, 1 - k % 2
            wa, wb, wc, wd, we = [0.5 * w_ref[a, b, t + k] for a, b in ((0, 0), (0, 1), (0, 2), (1, 0), (1, 1))]
            blocks = []
            at, left = tops[k] - low, NG - drops[k]
            while left:
                n = min(left, BLOCK if left > BLOCK + 1 or left == BLOCK else (left + 1) // 2)
                blocks.append((at, 8 * n))
                at, left = at + 8 * n, left - n
            for q, rows in blocks if sign < 0 else blocks[::-1]:
                ca, cb, cc, cd, ce = [jnp.full((G, rows, 128), x, F32) for x in (wa, wb, wc, wd, 1.5 + we)]
                n = sv[src, :, pl.ds(q - 1, rows), :]
                m = sv[src, :, pl.ds(q, rows), :]
                s = sv[src, :, pl.ds(q + 1, rows), :]
                x = (ca * (n[0:G] + s[2:G + 2]) + cc * (n[2:G + 2] + s[0:G])) + (cb * (n[1:G + 1] + s[1:G + 1]) + cd * (m[0:G] + m[2:G + 2]))
                x = x + (ce * m[1:G + 1] - sv[dst, 1:G + 1, pl.ds(q, rows), :])
                sv[dst, 1:G + 1, pl.ds(q, rows), :] = x
                sv[dst, G + 1, pl.ds(q, rows), :] = pltpu.roll(x[0], 127, 1)
                sv[dst, 0, pl.ds(q, rows), :] = pltpu.roll(x[G - 1], 1, 1)

    def exchange(e, side, to, late):
        src = sbuf.at[e] if late else st.at[:, pl.ds(1, G), pl.ds(jnp.where(side == 0, OFF, OFF + ROWS - T), T)]
        return pltpu.make_async_remote_copy(
            src_ref=src, dst_ref=rbuf.at[e, side],
            send_sem=ex_ssem.at[e, side], recv_sem=ex_rsem.at[e, side],
            device_id={"row": to, "col": col}, device_id_type=MESH)

    def get(lo):
        for g in range(G):
            idx = maps[G + g]
            for n in range(NG):
                q = pl.multiple_of(lo + (OFF + 8 * n), 8)
                for f in range(2):
                    zbuf[f, g, 8 * n:8 * n + 8, :] = lanes(st[f, g + 1, pl.ds(q, 8), :], idx)
        residue = maps[2 * G]
        for n in range(NG):
            r = pl.multiple_of(lo + 8 * n, 8)
            for f, out in ((0, now_ref), (1, before_ref)):
                for k in range(4):
                    x = zbuf[f, 0, 8 * n:8 * n + 8, :]
                    for g in range(1, G):
                        x = jnp.where(residue == (g + 1 + 2 * k) % G, zbuf[f, g, 8 * n:8 * n + 8, :], x)
                    out[pl.ds(r, 8), 128 * k:128 * k + 128] = x

    def tile(it, _):
        sweep, c = lax.div(it, TILES), lax.rem(it, TILES)
        odd = lax.rem(sweep, 2)
        base = jnp.where(odd == 0, OFF - T + TILE * c, OFF + ROWS + T - TILE * (c + 1))

        @pl.when(it == 0)
        def _():
            raws[2].wait_recv()
            raws[3].wait_recv()
            diags[1].wait_recv()
            packs[0].wait_recv()

        @pl.when(it == 1)
        def _():
            packs[1].wait_recv()

        @pl.when(it == 2)
        def _():
            raws[0].wait_recv()
            raws[1].wait_recv()
            diags[0].wait_recv()
            packs[2].wait_recv()

        @pl.when(sweep == 0)
        def _():
            put(c)

        first = odd
        last = 1 - odd
        to_first = jnp.where(odd == 0, up, down)
        to_last = jnp.where(odd == 0, down, up)

        def put_rows(side):
            at = jnp.where(side == 0, OFF - T, OFF + ROWS)
            for k in range(T // 8):
                q = pl.multiple_of(at + 8 * k, 8)
                for g in range(G):
                    x = rbuf[sweep - 1, 1 - side, 0, g, pl.ds(8 * k, 8), :]
                    st[0, g + 1, pl.ds(q, 8), :] = x
                    if g == 0:
                        st[0, G + 1, pl.ds(q, 8), :] = pltpu.roll(x, 127, 1)
                    if g == G - 1:
                        st[0, 0, pl.ds(q, 8), :] = pltpu.roll(x, 1, 1)
                    st[1, g + 1, pl.ds(q, 8), :] = rbuf[sweep - 1, 1 - side, 1, g, pl.ds(8 * k, 8), :]

        @pl.when((sweep > 0) & (c == 0))
        def _():
            at = jnp.where(first == 0, OFF, OFF + ROWS - T)
            for k in range(T // 8):
                q = pl.multiple_of(at + 8 * k, 8)
                for f in range(2):
                    for g in range(G):
                        sbuf[sweep - 1, f, g, pl.ds(8 * k, 8), :] = st[f, g + 1, pl.ds(q, 8), :]
            exchange(sweep - 1, 1 - first, up, True).wait_recv()
            put_rows(first)
            exchange(sweep - 1, first, to_first, True).start()

        @pl.when((sweep < SWEEPS - 1) & (c == 1))
        def _():
            exchange(sweep, first, to_first, False).start()

        @pl.when((sweep > 0) & (c == TILES - 1))
        def _():
            exchange(sweep - 1, last, up, False).wait_send()
            exchange(sweep - 1, 1 - last, up, True).wait_recv()
            put_rows(last)

        for sign in (-1, 1):
            for begins in (True, False):
                @pl.when((2 * odd - 1 == sign) & ((c == 0) == begins))
                def _():
                    run(sweep * T, base, sign, begins)

        @pl.when(sweep == SWEEPS - 1)
        def _():
            get(pl.multiple_of(jnp.where(c == 0, ROWS - TILE, (TILES - 1 - c) * TILE), 8))

        return 0

    lax.fori_loop(0, SWEEPS * TILES, tile, 0)

    for cp in raws + packs + diags:
        cp.wait_send()
    for e in range(SWEEPS - 1):
        exchange(e, (e + 1) % 2, up, True).wait_send()


def solution(mesh):
    def local_run(u_tile, v_tile, w):
        dma = pltpu.SemaphoreType.DMA
        now, before = pl.pallas_call(
            wave_kernel,
            out_shape=[jax.ShapeDtypeStruct((ROWS, COLS), F32)] * 2,
            in_specs=[pl.BlockSpec(memory_space=pl.ANY)] * 3,
            out_specs=[pl.BlockSpec(memory_space=pltpu.VMEM)] * 2,
            scratch_shapes=[
                pltpu.VMEM((2, G + 2, R, 128), F32), pltpu.SMEM((3, 3, SWEEPS * T), F32), pltpu.VMEM((2 * G + 1, 8, 128), jnp.int32),
                pltpu.VMEM((ROWS + 2 * T, COLS), F32), pltpu.VMEM((ROWS + 2 * T, COLS), F32),
                pltpu.VMEM((2, ROWS, 128), F32), pltpu.VMEM((2, ROWS + 2 * T, 128), F32), pltpu.VMEM((2, G, TILE, 128), F32),
                pltpu.VMEM((SWEEPS - 1, 2, G, T, 128), F32), pltpu.VMEM((SWEEPS - 1, 2, 2, G, T, 128), F32),
                dma((2, 8)), dma((2, 2)), dma((2, 2)), dma((TILES,)), dma((TILES,)), dma((2,)), dma((2,)),
                dma((SWEEPS - 1, 2)), dma((SWEEPS - 1, 2)),
            ],
            compiler_params=pltpu.CompilerParams(collective_id=0, has_side_effects=True, vmem_limit_bytes=VMEM_LIMIT),
        )(u_tile, v_tile, pltpu.with_memory_space_constraint(jnp.transpose(w, (1, 2, 0)), pltpu.HBM))
        return 4.0 * now, 8.0 * (now - before)

    tile_spec = P(("ens", "row"), "col")
    return jax.shard_map(local_run, mesh=mesh, in_specs=(tile_spec, tile_spec, P()), out_specs=(tile_spec, tile_spec), check_vma=False)
```

```python
import jax
import jax.numpy as jnp
from jax import lax
from jax.experimental import pallas as pl
from jax.experimental.pallas import tpu as pltpu
from jax.sharding import PartitionSpec as P

F32 = jnp.float32
MESH = pl.DeviceIdType.MESH
ROWS, COLS = 256, 512
G = 5
T = 16
SWEEPS = 4
TILES = 3
TILE = (ROWS + 2 * T) // TILES
NG = TILE // 8
BLOCK = 4
OFF = 32
R = 328
VMEM_LIMIT = 55_300_000


def wave_kernel(u_hbm, v_hbm, w_hbm, now_ref, before_ref, st, w_ref, maps, uraw, vraw, pbuf, hbuf, zbuf, sbuf, rbuf,
                load_sem, raw_ssem, raw_rsem, pk_ssem, pk_rsem, dg_rsem, ex_ssem, ex_rsem):
    row = lax.axis_index("row")
    col = lax.axis_index("col")
    up = lax.rem(row + 3, 4)
    down = lax.rem(row + 1, 4)
    other = 1 - col

    barrier = pltpu.get_barrier_semaphore()
    for rr, cc in ((row, other), (up, col), (down, col), (up, other), (down, other)):
        pl.semaphore_signal(barrier, inc=1, device_id={"row": rr, "col": cc}, device_id_type=MESH)

    cuts = [0] + [TILE * (c + 1) - T for c in range(TILES - 1)] + [ROWS]

    stages = [[(lo, n, at, 128) for lo, n in spans for at in (0, COLS - 128)]
              for spans in (((ROWS - T, T), (0, cuts[1])), ((cuts[1], ROWS - T - cuts[1]),))]
    stages.append([(0, ROWS, 128, COLS - 256)])
    for k, pieces in enumerate(stages):
        for lo, n, at, m in pieces:
            for src, dst in ((u_hbm, uraw), (v_hbm, vraw)):
                pltpu.make_async_copy(src.at[pl.ds(lo, n), pl.ds(at, m)], dst.at[pl.ds(T + lo, n), pl.ds(at, m)], load_sem.at[k]).start()
    weights = pltpu.make_async_copy(w_hbm, w_ref, load_sem.at[3])
    weights.start()

    def wait_bytes(ref, sem):
        pltpu.make_async_copy(ref, ref, sem).wait()

    def wait_stage(k):
        wait_bytes(uraw.at[pl.ds(0, sum(n * m for _, n, _, m in stages[k]) * 2 // COLS)], load_sem.at[k])

    def zero(i, _):
        for f in range(2):
            for g in range(G + 2):
                st[f, g, pl.ds(pl.multiple_of(i * 8, 8), 8), :] = jnp.zeros((8, 128), F32)
        return 0

    lax.fori_loop(0, (OFF - T) // 8, zero, 0)
    lax.fori_loop((OFF + ROWS + T) // 8, R // 8, zero, 0)

    lane = lax.broadcasted_iota(jnp.int32, (8, 128), 1)
    maps[2 * G] = lax.rem(lane, G)
    for g in range(G):
        maps[g] = lax.rem(lane * G + (g + 64), 128)
        k = lax.rem(3 * (lane + (2 * G - g - 1)), G)
        maps[G + g] = lax.div(lax.rem(128 * k + lane + 64, 128 * G), G)

    pl.semaphore_wait(barrier, 5)

    def raw_copy(f, side):
        src = (u_hbm, v_hbm)[f]
        dst = (uraw, vraw)[f]
        lo, at, to = ((0, T + ROWS, up), (ROWS - T, 0, down))[side]
        return pltpu.make_async_remote_copy(
            src_ref=src.at[pl.ds(lo, T)], dst_ref=dst.at[pl.ds(at, T)],
            send_sem=raw_ssem.at[0], recv_sem=raw_rsem.at[side],
            device_id={"row": to, "col": col}, device_id_type=MESH)

    raws = [raw_copy(f, side) for side in range(2) for f in range(2)]
    for cp in raws[2:] + raws[:2]:
        cp.start()

    def packed_copy(c):
        n = cuts[c + 1] - cuts[c]
        return pltpu.make_async_remote_copy(
            src_ref=pbuf.at[:, pl.ds(cuts[c], n)], dst_ref=hbuf.at[:, pl.ds(T + cuts[c], n)],
            send_sem=pk_ssem.at[0], recv_sem=pk_rsem.at[c],
            device_id={"row": row, "col": other}, device_id_type=MESH)

    def diag_copy(side):
        lo, at, to = ((0, T + ROWS, up), (ROWS - T, 0, down))[side]
        return pltpu.make_async_remote_copy(
            src_ref=pbuf.at[:, pl.ds(lo, T)], dst_ref=hbuf.at[:, pl.ds(at, T)],
            send_sem=pk_ssem.at[0], recv_sem=dg_rsem.at[side],
            device_id={"row": to, "col": other}, device_id_type=MESH)

    packs = [packed_copy(c) for c in range(TILES)]
    diags = [diag_copy(side) for side in range(2)]

    wait_stage(0)

    def pack(i, _):
        r = pl.multiple_of(i * 8, 8)
        for f, ref in ((0, uraw), (1, vraw)):
            pbuf[f, pl.ds(r, 8), :] = jnp.where(lane < 64, ref[pl.ds(r + T, 8), 0:128], ref[pl.ds(r + T, 8), 384:512])
        return 0

    lax.fori_loop((ROWS - T) // 8, ROWS // 8, pack, 0)
    lax.fori_loop(0, cuts[1] // 8, pack, 0)
    diags[1].start()
    packs[0].start()
    diags[0].start()
    wait_stage(1)
    lax.fori_loop(cuts[1] // 8, (ROWS - T) // 8, pack, 0)
    packs[1].start()
    packs[2].start()

    wait_stage(2)
    weights.wait()

    def lanes(x, idx):
        return jnp.take_along_axis(x, idx, axis=1, mode="promise_in_bounds")

    def put(c):
        residue = maps[2 * G]
        for g in range(G):
            idx = maps[g]
            for n in range(NG):
                r = pl.multiple_of(c * TILE + 8 * n, 8)
                q = pl.multiple_of(c * TILE + (OFF - T + 8 * n), 8)
                u, v = hbuf[0, pl.ds(r, 8), :], hbuf[1, pl.ds(r, 8), :]
                for k in range(4):
                    mask = residue == (g + 1 + 2 * k) % G
                    u = jnp.where(mask, uraw[pl.ds(r, 8), 128 * k:128 * k + 128], u)
                    v = jnp.where(mask, vraw[pl.ds(r, 8), 128 * k:128 * k + 128], v)
                x = 0.25 * lanes(u, idx)
                st[0, g + 1, pl.ds(q, 8), :] = x
                st[1, g + 1, pl.ds(q, 8), :] = x - 0.125 * lanes(v, idx)
        for n in range(NG):
            q = pl.multiple_of(c * TILE + (OFF - T + 8 * n), 8)
            st[0, G + 1, pl.ds(q, 8), :] = pltpu.roll(st[0, 1, pl.ds(q, 8), :], 127, 1)
            st[0, 0, pl.ds(q, 8), :] = pltpu.roll(st[0, G, pl.ds(q, 8), :], 1, 1)

    def run(t, base, sign, first):
        drops = [2 * (k + 1) // 8 if first else 0 for k in range(T)]
        tops = [sign * (k + 1) + (8 * drops[k] if sign < 0 else 0) for k in range(T)]
        low = min(tops) - 1
        high = max(top + TILE - 8 * drop for top, drop in zip(tops, drops)) + 1
        sv = st.at[:, :, pl.ds(base + low, high - low)]
        for k in range(T):
            src, dst = k % 2, 1 - k % 2
            wa, wb, wc, wd, we = [0.5 * w_ref[a, b, t + k] for a, b in ((0, 0), (0, 1), (0, 2), (1, 0), (1, 1))]
            blocks = []
            at, left = tops[k] - low, NG - drops[k]
            while left:
                n = min(left, BLOCK if left > BLOCK + 1 or left == BLOCK else (left + 1) // 2)
                blocks.append((at, 8 * n))
                at, left = at + 8 * n, left - n
            for q, rows in blocks if sign < 0 else blocks[::-1]:
                ca, cb, cc, cd, ce = [jnp.full((G, rows, 128), x, F32) for x in (wa, wb, wc, wd, 1.5 + we)]
                n = sv[src, :, pl.ds(q - 1, rows), :]
                m = sv[src, :, pl.ds(q, rows), :]
                s = sv[src, :, pl.ds(q + 1, rows), :]
                x = (ca * (n[0:G] + s[2:G + 2]) + cc * (n[2:G + 2] + s[0:G])) + (cb * (n[1:G + 1] + s[1:G + 1]) + cd * (m[0:G] + m[2:G + 2]))
                x = x + (ce * m[1:G + 1] - sv[dst, 1:G + 1, pl.ds(q, rows), :])
                sv[dst, 1:G + 1, pl.ds(q, rows), :] = x
                sv[dst, G + 1, pl.ds(q, rows), :] = pltpu.roll(x[0], 127, 1)
                sv[dst, 0, pl.ds(q, rows), :] = pltpu.roll(x[G - 1], 1, 1)

    def exchange(e, side, to, late):
        src = sbuf.at[e] if late else st.at[:, pl.ds(1, G), pl.ds(jnp.where(side == 0, OFF, OFF + ROWS - T), T)]
        return pltpu.make_async_remote_copy(
            src_ref=src, dst_ref=rbuf.at[e, side],
            send_sem=ex_ssem.at[int(late)], recv_sem=ex_rsem.at[e, side],
            device_id={"row": to, "col": col}, device_id_type=MESH)

    def get(lo):
        for g in range(G):
            idx = maps[G + g]
            for n in range(NG):
                q = pl.multiple_of(lo + (OFF + 8 * n), 8)
                for f in range(2):
                    zbuf[f, g, 8 * n:8 * n + 8, :] = lanes(st[f, g + 1, pl.ds(q, 8), :], idx)
        residue = maps[2 * G]
        for n in range(NG):
            r = pl.multiple_of(lo + 8 * n, 8)
            for f, out in ((0, now_ref), (1, before_ref)):
                for k in range(4):
                    x = zbuf[f, 0, 8 * n:8 * n + 8, :]
                    for g in range(1, G):
                        x = jnp.where(residue == (g + 1 + 2 * k) % G, zbuf[f, g, 8 * n:8 * n + 8, :], x)
                    out[pl.ds(r, 8), 128 * k:128 * k + 128] = x

    def tile(it, _):
        sweep, c = lax.div(it, TILES), lax.rem(it, TILES)
        odd = lax.rem(sweep, 2)
        base = jnp.where(odd == 0, OFF - T + TILE * c, OFF + ROWS + T - TILE * (c + 1))

        @pl.when(it == 0)
        def _():
            wait_bytes(uraw.at[pl.ds(0, 2 * T)], raw_rsem.at[1])
            wait_bytes(uraw.at[pl.ds(0, 4 * T)], raw_ssem.at[0])
            diags[1].wait_recv()
            packs[0].wait_recv()

        @pl.when(it == 1)
        def _():
            packs[1].wait_recv()

        @pl.when(it == 2)
        def _():
            wait_bytes(uraw.at[pl.ds(0, 2 * T)], raw_rsem.at[0])
            diags[0].wait_recv()
            packs[2].wait_recv()

        @pl.when(sweep == 0)
        def _():
            put(c)

        first = odd
        last = 1 - odd
        to_first = jnp.where(odd == 0, up, down)
        to_last = jnp.where(odd == 0, down, up)

        def put_rows(side):
            at = jnp.where(side == 0, OFF - T, OFF + ROWS)
            for k in range(T // 8):
                q = pl.multiple_of(at + 8 * k, 8)
                for g in range(G):
                    x = rbuf[sweep - 1, 1 - side, 0, g, pl.ds(8 * k, 8), :]
                    st[0, g + 1, pl.ds(q, 8), :] = x
                    if g == 0:
                        st[0, G + 1, pl.ds(q, 8), :] = pltpu.roll(x, 127, 1)
                    if g == G - 1:
                        st[0, 0, pl.ds(q, 8), :] = pltpu.roll(x, 1, 1)
                    st[1, g + 1, pl.ds(q, 8), :] = rbuf[sweep - 1, 1 - side, 1, g, pl.ds(8 * k, 8), :]

        @pl.when((sweep > 0) & (c == 0))
        def _():
            at = jnp.where(first == 0, OFF, OFF + ROWS - T)
            for k in range(T // 8):
                q = pl.multiple_of(at + 8 * k, 8)
                for f in range(2):
                    for g in range(G):
                        sbuf[sweep - 1, f, g, pl.ds(8 * k, 8), :] = st[f, g + 1, pl.ds(q, 8), :]
            exchange(sweep - 1, 1 - first, up, True).wait_recv()
            put_rows(first)
            exchange(sweep - 1, first, to_first, True).start()

        @pl.when((sweep > 0) & (c == 1))
        def _():
            exchange(sweep - 1, last, up, False).wait_send()

        @pl.when((sweep < SWEEPS - 1) & (c == 1))
        def _():
            exchange(sweep, first, to_first, False).start()

        @pl.when((sweep > 0) & (c == TILES - 1))
        def _():
            exchange(sweep - 1, 1 - last, up, True).wait_recv()
            put_rows(last)

        for sign in (-1, 1):
            for begins in (True, False):
                @pl.when((2 * odd - 1 == sign) & ((c == 0) == begins))
                def _():
                    run(sweep * T, base, sign, begins)

        @pl.when(sweep == SWEEPS - 1)
        def _():
            get(pl.multiple_of(jnp.where(c == 0, ROWS - TILE, (TILES - 1 - c) * TILE), 8))

        return 0

    lax.fori_loop(0, SWEEPS * TILES, tile, 0)

    wait_bytes(hbuf, pk_ssem.at[0])
    wait_bytes(sbuf, ex_ssem.at[1])


def solution(mesh):
    def local_run(u_tile, v_tile, w):
        dma = pltpu.SemaphoreType.DMA
        now, before = pl.pallas_call(
            wave_kernel,
            out_shape=[jax.ShapeDtypeStruct((ROWS, COLS), F32)] * 2,
            in_specs=[pl.BlockSpec(memory_space=pl.ANY)] * 3,
            out_specs=[pl.BlockSpec(memory_space=pltpu.VMEM)] * 2,
            scratch_shapes=[
                pltpu.VMEM((2, G + 2, R, 128), F32), pltpu.SMEM((3, 3, SWEEPS * T), F32), pltpu.VMEM((2 * G + 1, 8, 128), jnp.int32),
                pltpu.VMEM((ROWS + 2 * T, COLS), F32), pltpu.VMEM((ROWS + 2 * T, COLS), F32),
                pltpu.VMEM((2, ROWS, 128), F32), pltpu.VMEM((2, ROWS + 2 * T, 128), F32), pltpu.VMEM((2, G, TILE, 128), F32),
                pltpu.VMEM((SWEEPS - 1, 2, G, T, 128), F32), pltpu.VMEM((SWEEPS - 1, 2, 2, G, T, 128), F32),
                dma((4,)), dma((1,)), dma((2,)), dma((1,)), dma((TILES,)), dma((2,)), dma((2,)), dma((SWEEPS - 1, 2)),
            ],
            compiler_params=pltpu.CompilerParams(collective_id=0, has_side_effects=True, vmem_limit_bytes=VMEM_LIMIT),
        )(u_tile, v_tile, pltpu.with_memory_space_constraint(jnp.transpose(w, (1, 2, 0)), pltpu.HBM))
        return 4.0 * now, 8.0 * (now - before)

    tile_spec = P(("ens", "row"), "col")
    return jax.shard_map(local_run, mesh=mesh, in_specs=(tile_spec, tile_spec, P()), out_specs=(tile_spec, tile_spec), check_vma=False)
```

```python
import jax
import jax.numpy as jnp
from jax import lax
from jax.experimental import pallas as pl
from jax.experimental.pallas import tpu as pltpu
from jax.sharding import PartitionSpec as P

F32 = jnp.float32
MESH = pl.DeviceIdType.MESH
ROWS, COLS = 256, 512
G = 5
T = 16
SWEEPS = 4
TILES = 3
TILE = (ROWS + 2 * T) // TILES
NG = TILE // 8
BLOCK = 4
OFF = 32
R = 328
VMEM_LIMIT = 55_300_000


def wave_kernel(u_hbm, v_hbm, w_hbm, now_ref, before_ref, st, w_ref, maps, uraw, vraw, pbuf, hbuf, zbuf, sbuf, rbuf,
                load_sem, raw_ssem, raw_rsem, pk_ssem, pk_rsem, dg_rsem, ex_ssem, ex_rsem):
    row = lax.axis_index("row")
    col = lax.axis_index("col")
    up = lax.rem(row + 3, 4)
    down = lax.rem(row + 1, 4)
    other = 1 - col

    barrier = pltpu.get_barrier_semaphore()
    for rr, cc in ((row, other), (up, col), (down, col), (up, other), (down, other)):
        pl.semaphore_signal(barrier, inc=1, device_id={"row": rr, "col": cc}, device_id_type=MESH)

    cuts = [0] + [TILE * (c + 1) - T for c in range(TILES - 1)] + [ROWS]

    stages = [[(lo, n, at, 128) for lo, n in spans for at in (0, COLS - 128)]
              for spans in (((ROWS - T, T), (0, cuts[1])), ((cuts[1], ROWS - T - cuts[1]),))]
    stages.append([(0, ROWS, 128, COLS - 256)])
    for k, pieces in enumerate(stages):
        for lo, n, at, m in pieces:
            for src, dst in ((u_hbm, uraw), (v_hbm, vraw)):
                pltpu.make_async_copy(src.at[pl.ds(lo, n), pl.ds(at, m)], dst.at[pl.ds(T + lo, n), pl.ds(at, m)], load_sem.at[k]).start()
    weights = pltpu.make_async_copy(w_hbm, w_ref, load_sem.at[3])
    weights.start()

    def wait_bytes(ref, sem):
        pltpu.make_async_copy(ref, ref, sem).wait()

    def wait_stage(k):
        wait_bytes(uraw.at[pl.ds(0, sum(n * m for _, n, _, m in stages[k]) * 2 // COLS)], load_sem.at[k])

    def zero(i, _):
        for f in range(2):
            for g in range(G + 2):
                st[f, g, pl.ds(pl.multiple_of(i * 8, 8), 8), :] = jnp.zeros((8, 128), F32)
        return 0

    lax.fori_loop(0, (OFF - T) // 8, zero, 0)
    lax.fori_loop((OFF + ROWS + T) // 8, R // 8, zero, 0)

    lane = lax.broadcasted_iota(jnp.int32, (8, 128), 1)
    maps[2 * G] = lax.rem(lane, G)
    for g in range(G):
        maps[g] = lax.rem(lane * G + (g + 64), 128)
        k = lax.rem(3 * (lane + (2 * G - g - 1)), G)
        maps[G + g] = lax.div(lax.rem(128 * k + lane + 64, 128 * G), G)

    pl.semaphore_wait(barrier, 5)

    def raw_copy(f, side):
        src = (u_hbm, v_hbm)[f]
        dst = (uraw, vraw)[f]
        lo, at, to = ((0, T + ROWS, up), (ROWS - T, 0, down))[side]
        return pltpu.make_async_remote_copy(
            src_ref=src.at[pl.ds(lo, T)], dst_ref=dst.at[pl.ds(at, T)],
            send_sem=raw_ssem.at[0], recv_sem=raw_rsem.at[side],
            device_id={"row": to, "col": col}, device_id_type=MESH)

    raws = [raw_copy(f, side) for side in range(2) for f in range(2)]
    for cp in raws[2:] + raws[:2]:
        cp.start()

    def packed_copy(c):
        n = cuts[c + 1] - cuts[c]
        return pltpu.make_async_remote_copy(
            src_ref=pbuf.at[:, pl.ds(cuts[c], n)], dst_ref=hbuf.at[:, pl.ds(T + cuts[c], n)],
            send_sem=pk_ssem.at[0], recv_sem=pk_rsem.at[c],
            device_id={"row": row, "col": other}, device_id_type=MESH)

    def diag_copy(side):
        lo, at, to = ((0, T + ROWS, up), (ROWS - T, 0, down))[side]
        return pltpu.make_async_remote_copy(
            src_ref=pbuf.at[:, pl.ds(lo, T)], dst_ref=hbuf.at[:, pl.ds(at, T)],
            send_sem=pk_ssem.at[0], recv_sem=dg_rsem.at[side],
            device_id={"row": to, "col": other}, device_id_type=MESH)

    packs = [packed_copy(c) for c in range(TILES)]
    diags = [diag_copy(side) for side in range(2)]

    wait_stage(0)

    def pack(i, _):
        r = pl.multiple_of(i * 8, 8)
        for f, ref in ((0, uraw), (1, vraw)):
            pbuf[f, pl.ds(r, 8), :] = jnp.where(lane < 64, ref[pl.ds(r + T, 8), 0:128], ref[pl.ds(r + T, 8), 384:512])
        return 0

    lax.fori_loop((ROWS - T) // 8, ROWS // 8, pack, 0)
    lax.fori_loop(0, cuts[1] // 8, pack, 0)
    diags[1].start()
    packs[0].start()
    diags[0].start()
    wait_stage(1)
    lax.fori_loop(cuts[1] // 8, (ROWS - T) // 8, pack, 0)
    packs[1].start()
    packs[2].start()

    wait_stage(2)
    weights.wait()

    def lanes(x, idx):
        return jnp.take_along_axis(x, idx, axis=1, mode="promise_in_bounds")

    def put_main(c):
        residue = maps[2 * G]
        for g in range(G):
            idx = maps[g]
            masks = [residue == (g + 1 + 2 * k) % G for k in range(3)]
            for n in range(NG):
                r = pl.multiple_of(c * TILE + 8 * n, 8)
                q = pl.multiple_of(c * TILE + (OFF - T + 8 * n), 8)
                u, v = uraw[pl.ds(r, 8), 384:512], vraw[pl.ds(r, 8), 384:512]
                for k in range(3):
                    u = jnp.where(masks[k], uraw[pl.ds(r, 8), 128 * k:128 * k + 128], u)
                    v = jnp.where(masks[k], vraw[pl.ds(r, 8), 128 * k:128 * k + 128], v)
                x = 0.25 * lanes(u, idx)
                st[0, g + 1, pl.ds(q, 8), :] = x
                st[1, g + 1, pl.ds(q, 8), :] = x - 0.125 * lanes(v, idx)

    def put_halo(c):
        for g in range(G):
            idx = maps[g]
            column = lane * G + (g - 64)
            halo = (column < 0) | (column >= COLS)
            for n in range(NG):
                r = pl.multiple_of(c * TILE + 8 * n, 8)
                q = pl.multiple_of(c * TILE + (OFF - T + 8 * n), 8)
                h = 0.25 * lanes(hbuf[0, pl.ds(r, 8), :], idx)
                x = jnp.where(halo, h, st[0, g + 1, pl.ds(q, 8), :])
                st[0, g + 1, pl.ds(q, 8), :] = x
                st[1, g + 1, pl.ds(q, 8), :] = jnp.where(halo, h - 0.125 * lanes(hbuf[1, pl.ds(r, 8), :], idx), st[1, g + 1, pl.ds(q, 8), :])
                if g == 0:
                    st[0, G + 1, pl.ds(q, 8), :] = pltpu.roll(x, 127, 1)
                if g == G - 1:
                    st[0, 0, pl.ds(q, 8), :] = pltpu.roll(x, 1, 1)

    def put_tile(i, _):
        @pl.when(i == 1)
        def _():
            wait_bytes(uraw.at[pl.ds(0, 2 * T)], raw_rsem.at[1])
            wait_bytes(uraw.at[pl.ds(0, 2 * T)], raw_rsem.at[0])
            wait_bytes(uraw.at[pl.ds(0, 4 * T)], raw_ssem.at[0])

        put_main(lax.rem(i + 1, TILES))
        return 0

    lax.fori_loop(0, TILES, put_tile, 0)

    def run(t, base, sign, first):
        drops = [2 * (k + 1) // 8 if first else 0 for k in range(T)]
        tops = [sign * (k + 1) + (8 * drops[k] if sign < 0 else 0) for k in range(T)]
        low = min(tops) - 1
        high = max(top + TILE - 8 * drop for top, drop in zip(tops, drops)) + 1
        sv = st.at[:, :, pl.ds(base + low, high - low)]
        for k in range(T):
            src, dst = k % 2, 1 - k % 2
            wa, wb, wc, wd, we = [0.5 * w_ref[a, b, t + k] for a, b in ((0, 0), (0, 1), (0, 2), (1, 0), (1, 1))]
            blocks = []
            at, left = tops[k] - low, NG - drops[k]
            while left:
                n = min(left, BLOCK if left > BLOCK + 1 or left == BLOCK else (left + 1) // 2)
                blocks.append((at, 8 * n))
                at, left = at + 8 * n, left - n
            for q, rows in blocks if sign < 0 else blocks[::-1]:
                ca, cb, cc, cd, ce = [jnp.full((G, rows, 128), x, F32) for x in (wa, wb, wc, wd, 1.5 + we)]
                n = sv[src, :, pl.ds(q - 1, rows), :]
                m = sv[src, :, pl.ds(q, rows), :]
                s = sv[src, :, pl.ds(q + 1, rows), :]
                x = (ca * (n[0:G] + s[2:G + 2]) + cc * (n[2:G + 2] + s[0:G])) + (cb * (n[1:G + 1] + s[1:G + 1]) + cd * (m[0:G] + m[2:G + 2]))
                x = x + (ce * m[1:G + 1] - sv[dst, 1:G + 1, pl.ds(q, rows), :])
                sv[dst, 1:G + 1, pl.ds(q, rows), :] = x
                sv[dst, G + 1, pl.ds(q, rows), :] = pltpu.roll(x[0], 127, 1)
                sv[dst, 0, pl.ds(q, rows), :] = pltpu.roll(x[G - 1], 1, 1)

    def exchange(e, side, to, late):
        src = sbuf.at[e] if late else st.at[:, pl.ds(1, G), pl.ds(jnp.where(side == 0, OFF, OFF + ROWS - T), T)]
        return pltpu.make_async_remote_copy(
            src_ref=src, dst_ref=rbuf.at[e, side],
            send_sem=ex_ssem.at[int(late)], recv_sem=ex_rsem.at[e, side],
            device_id={"row": to, "col": col}, device_id_type=MESH)

    def get(lo):
        for g in range(G):
            idx = maps[G + g]
            for n in range(NG):
                q = pl.multiple_of(lo + (OFF + 8 * n), 8)
                for f in range(2):
                    zbuf[f, g, 8 * n:8 * n + 8, :] = lanes(st[f, g + 1, pl.ds(q, 8), :], idx)
        residue = maps[2 * G]
        for n in range(NG):
            r = pl.multiple_of(lo + 8 * n, 8)
            for f, out in ((0, now_ref), (1, before_ref)):
                for k in range(4):
                    x = zbuf[f, 0, 8 * n:8 * n + 8, :]
                    for g in range(1, G):
                        x = jnp.where(residue == (g + 1 + 2 * k) % G, zbuf[f, g, 8 * n:8 * n + 8, :], x)
                    out[pl.ds(r, 8), 128 * k:128 * k + 128] = x

    def tile(it, _):
        sweep, c = lax.div(it, TILES), lax.rem(it, TILES)
        odd = lax.rem(sweep, 2)
        base = jnp.where(odd == 0, OFF - T + TILE * c, OFF + ROWS + T - TILE * (c + 1))

        @pl.when(it == 0)
        def _():
            diags[1].wait_recv()
            packs[0].wait_recv()

        @pl.when(it == 1)
        def _():
            packs[1].wait_recv()

        @pl.when(it == 2)
        def _():
            diags[0].wait_recv()
            packs[2].wait_recv()

        @pl.when(sweep == 0)
        def _():
            put_halo(c)

        first = odd
        last = 1 - odd
        to_first = jnp.where(odd == 0, up, down)
        to_last = jnp.where(odd == 0, down, up)

        def put_rows(side):
            at = jnp.where(side == 0, OFF - T, OFF + ROWS)
            for k in range(T // 8):
                q = pl.multiple_of(at + 8 * k, 8)
                for g in range(G):
                    x = rbuf[sweep - 1, 1 - side, 0, g, pl.ds(8 * k, 8), :]
                    st[0, g + 1, pl.ds(q, 8), :] = x
                    if g == 0:
                        st[0, G + 1, pl.ds(q, 8), :] = pltpu.roll(x, 127, 1)
                    if g == G - 1:
                        st[0, 0, pl.ds(q, 8), :] = pltpu.roll(x, 1, 1)
                    st[1, g + 1, pl.ds(q, 8), :] = rbuf[sweep - 1, 1 - side, 1, g, pl.ds(8 * k, 8), :]

        @pl.when((sweep > 0) & (c == 0))
        def _():
            at = jnp.where(first == 0, OFF, OFF + ROWS - T)
            for k in range(T // 8):
                q = pl.multiple_of(at + 8 * k, 8)
                for f in range(2):
                    for g in range(G):
                        sbuf[sweep - 1, f, g, pl.ds(8 * k, 8), :] = st[f, g + 1, pl.ds(q, 8), :]
            exchange(sweep - 1, 1 - first, up, True).wait_recv()
            put_rows(first)
            exchange(sweep - 1, first, to_first, True).start()

        @pl.when((sweep > 0) & (c == 1))
        def _():
            exchange(sweep - 1, last, up, False).wait_send()

        @pl.when((sweep < SWEEPS - 1) & (c == 1))
        def _():
            exchange(sweep, first, to_first, False).start()

        @pl.when((sweep > 0) & (c == TILES - 1))
        def _():
            exchange(sweep - 1, 1 - last, up, True).wait_recv()
            put_rows(last)

        for sign in (-1, 1):
            for begins in (True, False):
                @pl.when((2 * odd - 1 == sign) & ((c == 0) == begins))
                def _():
                    run(sweep * T, base, sign, begins)

        @pl.when(sweep == SWEEPS - 1)
        def _():
            get(pl.multiple_of(jnp.where(c == 0, ROWS - TILE, (TILES - 1 - c) * TILE), 8))

        return 0

    lax.fori_loop(0, SWEEPS * TILES, tile, 0)

    wait_bytes(hbuf, pk_ssem.at[0])
    wait_bytes(sbuf, ex_ssem.at[1])


def solution(mesh):
    def local_run(u_tile, v_tile, w):
        dma = pltpu.SemaphoreType.DMA
        now, before = pl.pallas_call(
            wave_kernel,
            out_shape=[jax.ShapeDtypeStruct((ROWS, COLS), F32)] * 2,
            in_specs=[pl.BlockSpec(memory_space=pl.ANY)] * 3,
            out_specs=[pl.BlockSpec(memory_space=pltpu.VMEM)] * 2,
            scratch_shapes=[
                pltpu.VMEM((2, G + 2, R, 128), F32), pltpu.SMEM((3, 3, SWEEPS * T), F32), pltpu.VMEM((2 * G + 1, 8, 128), jnp.int32),
                pltpu.VMEM((ROWS + 2 * T, COLS), F32), pltpu.VMEM((ROWS + 2 * T, COLS), F32),
                pltpu.VMEM((2, ROWS, 128), F32), pltpu.VMEM((2, ROWS + 2 * T, 128), F32), pltpu.VMEM((2, G, TILE, 128), F32),
                pltpu.VMEM((SWEEPS - 1, 2, G, T, 128), F32), pltpu.VMEM((SWEEPS - 1, 2, 2, G, T, 128), F32),
                dma((4,)), dma((1,)), dma((2,)), dma((1,)), dma((TILES,)), dma((2,)), dma((2,)), dma((SWEEPS - 1, 2)),
            ],
            compiler_params=pltpu.CompilerParams(collective_id=0, has_side_effects=True, vmem_limit_bytes=VMEM_LIMIT),
        )(u_tile, v_tile, pltpu.with_memory_space_constraint(jnp.transpose(w, (1, 2, 0)), pltpu.HBM))
        return 4.0 * now, 8.0 * (now - before)

    tile_spec = P(("ens", "row"), "col")
    return jax.shard_map(local_run, mesh=mesh, in_specs=(tile_spec, tile_spec, P()), out_specs=(tile_spec, tile_spec), check_vma=False)
```

```python
import jax
import jax.numpy as jnp
from jax import lax
from jax.experimental import pallas as pl
from jax.experimental.pallas import tpu as pltpu
from jax.sharding import PartitionSpec as P

F32 = jnp.float32
MESH = pl.DeviceIdType.MESH
ROWS, COLS = 256, 512
G = 5
T = 16
SWEEPS = 4
TILES = 3
TILE = (ROWS + 2 * T) // TILES
NG = TILE // 8
BLOCK = 4
OFF = 32
R = 328
VMEM_LIMIT = 55_300_000


def wave_kernel(u_hbm, v_hbm, w_hbm, now_ref, before_ref, st, w_ref, maps, uraw, vraw, pbuf, hbuf, zbuf, sbuf, rbuf,
                load_sem, raw_ssem, raw_rsem, pk_ssem, pk_rsem, dg_rsem, ex_ssem, ex_rsem):
    row = lax.axis_index("row")
    col = lax.axis_index("col")
    up = lax.rem(row + 3, 4)
    down = lax.rem(row + 1, 4)
    other = 1 - col

    barrier = pltpu.get_barrier_semaphore()
    for rr, cc in ((row, other), (up, col), (down, col), (up, other), (down, other)):
        pl.semaphore_signal(barrier, inc=1, device_id={"row": rr, "col": cc}, device_id_type=MESH)

    cuts = [0] + [TILE * (c + 1) - T for c in range(TILES - 1)] + [ROWS]

    stages = [[(lo, n, at, 128) for lo, n in spans for at in (0, COLS - 128)]
              for spans in (((ROWS - T, T), (0, cuts[1])), ((cuts[1], ROWS - T - cuts[1]),))]
    stages.append([(0, ROWS, 128, COLS - 256)])
    for k, pieces in enumerate(stages):
        for lo, n, at, m in pieces:
            for src, dst in ((u_hbm, uraw), (v_hbm, vraw)):
                pltpu.make_async_copy(src.at[pl.ds(lo, n), pl.ds(at, m)], dst.at[pl.ds(T + lo, n), pl.ds(at, m)], load_sem.at[k]).start()
    weights = pltpu.make_async_copy(w_hbm, w_ref, load_sem.at[3])
    weights.start()

    def wait_bytes(ref, sem):
        pltpu.make_async_copy(ref, ref, sem).wait()

    def wait_stage(k):
        wait_bytes(uraw.at[pl.ds(0, sum(n * m for _, n, _, m in stages[k]) * 2 // COLS)], load_sem.at[k])

    def zero(i, _):
        for f in range(2):
            for g in range(G + 2):
                st[f, g, pl.ds(pl.multiple_of(i * 8, 8), 8), :] = jnp.zeros((8, 128), F32)
        return 0

    lax.fori_loop(0, (OFF - T) // 8, zero, 0)
    lax.fori_loop((OFF + ROWS + T) // 8, R // 8, zero, 0)

    lane = lax.broadcasted_iota(jnp.int32, (8, 128), 1)
    maps[2 * G] = lax.rem(lane, G)
    for g in range(G):
        maps[g] = lax.rem(lane * G + (g + 64), 128)
        k = lax.rem(3 * (lane + (2 * G - g - 1)), G)
        maps[G + g] = lax.div(lax.rem(128 * k + lane + 64, 128 * G), G)

    pl.semaphore_wait(barrier, 5)

    def raw_copy(f, side):
        src = (u_hbm, v_hbm)[f]
        dst = (uraw, vraw)[f]
        lo, at, to = ((0, T + ROWS, up), (ROWS - T, 0, down))[side]
        return pltpu.make_async_remote_copy(
            src_ref=src.at[pl.ds(lo, T)], dst_ref=dst.at[pl.ds(at, T)],
            send_sem=raw_ssem.at[0], recv_sem=raw_rsem.at[side],
            device_id={"row": to, "col": col}, device_id_type=MESH)

    raws = [raw_copy(f, side) for side in range(2) for f in range(2)]
    for cp in raws[2:] + raws[:2]:
        cp.start()

    def packed_copy(c):
        n = cuts[c + 1] - cuts[c]
        return pltpu.make_async_remote_copy(
            src_ref=pbuf.at[:, pl.ds(cuts[c], n)], dst_ref=hbuf.at[:, pl.ds(T + cuts[c], n)],
            send_sem=pk_ssem.at[0], recv_sem=pk_rsem.at[c],
            device_id={"row": row, "col": other}, device_id_type=MESH)

    def diag_copy(side):
        lo, at, to = ((0, T + ROWS, up), (ROWS - T, 0, down))[side]
        return pltpu.make_async_remote_copy(
            src_ref=pbuf.at[:, pl.ds(lo, T)], dst_ref=hbuf.at[:, pl.ds(at, T)],
            send_sem=pk_ssem.at[0], recv_sem=dg_rsem.at[side],
            device_id={"row": to, "col": other}, device_id_type=MESH)

    packs = [packed_copy(c) for c in range(TILES)]
    diags = [diag_copy(side) for side in range(2)]

    wait_stage(0)

    def pack(i, _):
        r = pl.multiple_of(i * 8, 8)
        for f, ref in ((0, uraw), (1, vraw)):
            pbuf[f, pl.ds(r, 8), :] = jnp.where(lane < 64, ref[pl.ds(r + T, 8), 0:128], ref[pl.ds(r + T, 8), 384:512])
        return 0

    lax.fori_loop((ROWS - T) // 8, ROWS // 8, pack, 0)
    lax.fori_loop(0, cuts[1] // 8, pack, 0)
    diags[1].start()
    packs[0].start()
    diags[0].start()
    wait_stage(1)
    lax.fori_loop(cuts[1] // 8, (ROWS - T) // 8, pack, 0)
    packs[1].start()
    packs[2].start()

    wait_stage(2)
    weights.wait()

    def lanes(x, idx):
        return jnp.take_along_axis(x, idx, axis=1, mode="promise_in_bounds")

    def put_main(c):
        residue = maps[2 * G]
        for g in range(G):
            idx = maps[g]
            masks = [residue == (g + 1 + 2 * k) % G for k in range(3)]
            for n in range(NG):
                r = pl.multiple_of(c * TILE + 8 * n, 8)
                q = pl.multiple_of(c * TILE + (OFF - T + 8 * n), 8)
                u, v = uraw[pl.ds(r, 8), 384:512], vraw[pl.ds(r, 8), 384:512]
                for k in range(3):
                    u = jnp.where(masks[k], uraw[pl.ds(r, 8), 128 * k:128 * k + 128], u)
                    v = jnp.where(masks[k], vraw[pl.ds(r, 8), 128 * k:128 * k + 128], v)
                x = 0.25 * lanes(u, idx)
                st[0, g + 1, pl.ds(q, 8), :] = x
                st[1, g + 1, pl.ds(q, 8), :] = x - 0.125 * lanes(v, idx)

    def put_halo(c):
        sv = st.at[:, :, pl.ds(pl.multiple_of(c * TILE + (OFF - T), 8), TILE)]
        hv = hbuf.at[:, pl.ds(pl.multiple_of(c * TILE, 8), TILE)]
        for g in range(G):
            idx = maps[g]
            column = lane * G + (g - 64)
            halo = (column < 0) | (column >= COLS)
            for n in range(NG):
                rows = pl.ds(8 * n, 8)
                h = 0.25 * lanes(hv[0, rows, :], idx)
                x = jnp.where(halo, h, sv[0, g + 1, rows, :])
                sv[0, g + 1, rows, :] = x
                sv[1, g + 1, rows, :] = jnp.where(halo, h - 0.125 * lanes(hv[1, rows, :], idx), sv[1, g + 1, rows, :])
                if g == 0:
                    sv[0, G + 1, rows, :] = pltpu.roll(x, 127, 1)
                if g == G - 1:
                    sv[0, 0, rows, :] = pltpu.roll(x, 1, 1)

    def put_tile(i, _):
        @pl.when(i == 1)
        def _():
            wait_bytes(uraw.at[pl.ds(0, 2 * T)], raw_rsem.at[1])
            wait_bytes(uraw.at[pl.ds(0, 2 * T)], raw_rsem.at[0])
            wait_bytes(uraw.at[pl.ds(0, 4 * T)], raw_ssem.at[0])

        put_main(lax.rem(i + 1, TILES))
        return 0

    lax.fori_loop(0, TILES, put_tile, 0)

    def run(t, base, sign, first):
        drops = [2 * (k + 1) // 8 if first else 0 for k in range(T)]
        tops = [sign * (k + 1) + (8 * drops[k] if sign < 0 else 0) for k in range(T)]
        low = min(tops) - 1
        high = max(top + TILE - 8 * drop for top, drop in zip(tops, drops)) + 1
        sv = st.at[:, :, pl.ds(base + low, high - low)]
        for k in range(T):
            src, dst = k % 2, 1 - k % 2
            wa, wb, wc, wd, we = [0.5 * w_ref[a, b, t + k] for a, b in ((0, 0), (0, 1), (0, 2), (1, 0), (1, 1))]
            blocks = []
            at, left = tops[k] - low, NG - drops[k]
            while left:
                n = min(left, BLOCK if left > BLOCK + 1 or left == BLOCK else (left + 1) // 2)
                blocks.append((at, 8 * n))
                at, left = at + 8 * n, left - n
            for q, rows in blocks if sign < 0 else blocks[::-1]:
                ca, cb, cc, cd, ce = [jnp.full((G, rows, 128), x, F32) for x in (wa, wb, wc, wd, 1.5 + we)]
                n = sv[src, :, pl.ds(q - 1, rows), :]
                m = sv[src, :, pl.ds(q, rows), :]
                s = sv[src, :, pl.ds(q + 1, rows), :]
                x = (ca * (n[0:G] + s[2:G + 2]) + cc * (n[2:G + 2] + s[0:G])) + (cb * (n[1:G + 1] + s[1:G + 1]) + cd * (m[0:G] + m[2:G + 2]))
                x = x + (ce * m[1:G + 1] - sv[dst, 1:G + 1, pl.ds(q, rows), :])
                sv[dst, 1:G + 1, pl.ds(q, rows), :] = x
                sv[dst, G + 1, pl.ds(q, rows), :] = pltpu.roll(x[0], 127, 1)
                sv[dst, 0, pl.ds(q, rows), :] = pltpu.roll(x[G - 1], 1, 1)

    def exchange(e, side, to, late):
        src = sbuf.at[e] if late else st.at[:, pl.ds(1, G), pl.ds(jnp.where(side == 0, OFF, OFF + ROWS - T), T)]
        return pltpu.make_async_remote_copy(
            src_ref=src, dst_ref=rbuf.at[e, side],
            send_sem=ex_ssem.at[int(late)], recv_sem=ex_rsem.at[e, side],
            device_id={"row": to, "col": col}, device_id_type=MESH)

    def get(lo):
        for g in range(G):
            idx = maps[G + g]
            for n in range(NG):
                q = pl.multiple_of(lo + (OFF + 8 * n), 8)
                for f in range(2):
                    zbuf[f, g, 8 * n:8 * n + 8, :] = lanes(st[f, g + 1, pl.ds(q, 8), :], idx)
        residue = maps[2 * G]
        for n in range(NG):
            r = pl.multiple_of(lo + 8 * n, 8)
            for f, out in ((0, now_ref), (1, before_ref)):
                for k in range(4):
                    x = zbuf[f, 0, 8 * n:8 * n + 8, :]
                    for g in range(1, G):
                        x = jnp.where(residue == (g + 1 + 2 * k) % G, zbuf[f, g, 8 * n:8 * n + 8, :], x)
                    out[pl.ds(r, 8), 128 * k:128 * k + 128] = x

    def tile(it, _):
        sweep, c = lax.div(it, TILES), lax.rem(it, TILES)
        odd = lax.rem(sweep, 2)
        base = jnp.where(odd == 0, OFF - T + TILE * c, OFF + ROWS + T - TILE * (c + 1))

        @pl.when(it == 0)
        def _():
            diags[1].wait_recv()
            packs[0].wait_recv()

        @pl.when(it == 1)
        def _():
            packs[1].wait_recv()

        @pl.when(it == 2)
        def _():
            diags[0].wait_recv()
            packs[2].wait_recv()

        @pl.when(sweep == 0)
        def _():
            put_halo(c)

        first = odd
        last = 1 - odd
        to_first = jnp.where(odd == 0, up, down)
        to_last = jnp.where(odd == 0, down, up)

        def put_rows(side):
            at = jnp.where(side == 0, OFF - T, OFF + ROWS)
            for k in range(T // 8):
                q = pl.multiple_of(at + 8 * k, 8)
                for g in range(G):
                    x = rbuf[sweep - 1, 1 - side, 0, g, pl.ds(8 * k, 8), :]
                    st[0, g + 1, pl.ds(q, 8), :] = x
                    if g == 0:
                        st[0, G + 1, pl.ds(q, 8), :] = pltpu.roll(x, 127, 1)
                    if g == G - 1:
                        st[0, 0, pl.ds(q, 8), :] = pltpu.roll(x, 1, 1)
                    st[1, g + 1, pl.ds(q, 8), :] = rbuf[sweep - 1, 1 - side, 1, g, pl.ds(8 * k, 8), :]

        @pl.when((sweep > 0) & (c == 0))
        def _():
            at = jnp.where(first == 0, OFF, OFF + ROWS - T)
            for k in range(T // 8):
                q = pl.multiple_of(at + 8 * k, 8)
                for f in range(2):
                    for g in range(G):
                        sbuf[sweep - 1, f, g, pl.ds(8 * k, 8), :] = st[f, g + 1, pl.ds(q, 8), :]
            exchange(sweep - 1, 1 - first, up, True).wait_recv()
            put_rows(first)
            exchange(sweep - 1, first, to_first, True).start()

        @pl.when((sweep > 0) & (c == 1))
        def _():
            exchange(sweep - 1, last, up, False).wait_send()

        @pl.when((sweep < SWEEPS - 1) & (c == 1))
        def _():
            exchange(sweep, first, to_first, False).start()

        @pl.when((sweep > 0) & (c == TILES - 1))
        def _():
            exchange(sweep - 1, 1 - last, up, True).wait_recv()
            put_rows(last)

        for sign in (-1, 1):
            for begins in (True, False):
                @pl.when((2 * odd - 1 == sign) & ((c == 0) == begins))
                def _():
                    run(sweep * T, base, sign, begins)

        @pl.when(sweep == SWEEPS - 1)
        def _():
            get(pl.multiple_of(jnp.where(c == 0, ROWS - TILE, (TILES - 1 - c) * TILE), 8))

        return 0

    lax.fori_loop(0, SWEEPS * TILES, tile, 0)

    wait_bytes(hbuf, pk_ssem.at[0])
    wait_bytes(sbuf, ex_ssem.at[1])


def solution(mesh):
    def local_run(u_tile, v_tile, w):
        dma = pltpu.SemaphoreType.DMA
        now, before = pl.pallas_call(
            wave_kernel,
            out_shape=[jax.ShapeDtypeStruct((ROWS, COLS), F32)] * 2,
            in_specs=[pl.BlockSpec(memory_space=pl.ANY)] * 3,
            out_specs=[pl.BlockSpec(memory_space=pltpu.VMEM)] * 2,
            scratch_shapes=[
                pltpu.VMEM((2, G + 2, R, 128), F32), pltpu.SMEM((3, 3, SWEEPS * T), F32), pltpu.VMEM((2 * G + 1, 8, 128), jnp.int32),
                pltpu.VMEM((ROWS + 2 * T, COLS), F32), pltpu.VMEM((ROWS + 2 * T, COLS), F32),
                pltpu.VMEM((2, ROWS, 128), F32), pltpu.VMEM((2, ROWS + 2 * T, 128), F32), pltpu.VMEM((2, G, TILE, 128), F32),
                pltpu.VMEM((SWEEPS - 1, 2, G, T, 128), F32), pltpu.VMEM((SWEEPS - 1, 2, 2, G, T, 128), F32),
                dma((4,)), dma((1,)), dma((2,)), dma((1,)), dma((TILES,)), dma((2,)), dma((2,)), dma((SWEEPS - 1, 2)),
            ],
            compiler_params=pltpu.CompilerParams(collective_id=0, has_side_effects=True, vmem_limit_bytes=VMEM_LIMIT),
        )(u_tile, v_tile, pltpu.with_memory_space_constraint(jnp.transpose(w, (1, 2, 0)), pltpu.HBM))
        return 4.0 * now, 8.0 * (now - before)

    tile_spec = P(("ens", "row"), "col")
    return jax.shard_map(local_run, mesh=mesh, in_specs=(tile_spec, tile_spec, P()), out_specs=(tile_spec, tile_spec), check_vma=False)
```

```python
import jax
import jax.numpy as jnp
from jax import lax
from jax.experimental import pallas as pl
from jax.experimental.pallas import tpu as pltpu
from jax.sharding import PartitionSpec as P

F32 = jnp.float32
MESH = pl.DeviceIdType.MESH
ROWS, COLS = 256, 512
G = 5
T = 16
SWEEPS = 4
TILES = 3
TILE = (ROWS + 2 * T) // TILES
NG = TILE // 8
BLOCK = 4
EARLY = 8
ORDER_STEPS = (1, 3, 5, 7, 9)
OFF = 32
R = 328
VMEM_LIMIT = 55_300_000


def wave_kernel(u_hbm, v_hbm, w_hbm, now_ref, before_ref, st, w_ref, maps, uraw, vraw, pbuf, hbuf, zbuf, sbuf, rbuf,
                load_sem, raw_ssem, raw_rsem, pk_ssem, pk_rsem, dg_rsem, ex_ssem, ex_rsem):
    row = lax.axis_index("row")
    col = lax.axis_index("col")
    up = lax.rem(row + 3, 4)
    down = lax.rem(row + 1, 4)
    other = 1 - col

    barrier = pltpu.get_barrier_semaphore()
    for rr, cc in ((row, other), (up, col), (down, col), (up, other), (down, other)):
        pl.semaphore_signal(barrier, inc=1, device_id={"row": rr, "col": cc}, device_id_type=MESH)

    cuts = [0] + [TILE * (c + 1) - T for c in range(TILES - 1)] + [ROWS]

    stages = [[(lo, n, at, 128) for lo, n in spans for at in (0, COLS - 128)]
              for spans in (((ROWS - T, T), (0, cuts[1])), ((cuts[1], ROWS - T - cuts[1]),))]
    stages.append([(0, ROWS, 128, COLS - 256)])
    for k, pieces in enumerate(stages):
        for lo, n, at, m in pieces:
            for src, dst in ((u_hbm, uraw), (v_hbm, vraw)):
                pltpu.make_async_copy(src.at[pl.ds(lo, n), pl.ds(at, m)], dst.at[pl.ds(T + lo, n), pl.ds(at, m)], load_sem.at[k]).start()
    weights = pltpu.make_async_copy(w_hbm, w_ref, load_sem.at[3])
    weights.start()

    def wait_bytes(ref, sem):
        pltpu.make_async_copy(ref, ref, sem).wait()

    def wait_stage(k):
        wait_bytes(uraw.at[pl.ds(0, sum(n * m for _, n, _, m in stages[k]) * 2 // COLS)], load_sem.at[k])

    def zero(i, _):
        for f in range(2):
            for g in range(G + 2):
                st[f, g, pl.ds(pl.multiple_of(i * 8, 8), 8), :] = jnp.zeros((8, 128), F32)
        return 0

    lax.fori_loop(0, (OFF - T) // 8, zero, 0)
    lax.fori_loop((OFF + ROWS + T) // 8, R // 8, zero, 0)

    lane = lax.broadcasted_iota(jnp.int32, (8, 128), 1)
    maps[2 * G] = lax.rem(lane, G)
    for g in range(G):
        maps[g] = lax.rem(lane * G + (g + 64), 128)
        k = lax.rem(3 * (lane + (2 * G - g - 1)), G)
        maps[G + g] = lax.div(lax.rem(128 * k + lane + 64, 128 * G), G)

    pl.semaphore_wait(barrier, 5)

    def raw_copy(f, side):
        src = (u_hbm, v_hbm)[f]
        dst = (uraw, vraw)[f]
        lo, at, to = ((0, T + ROWS, up), (ROWS - T, 0, down))[side]
        return pltpu.make_async_remote_copy(
            src_ref=src.at[pl.ds(lo, T)], dst_ref=dst.at[pl.ds(at, T)],
            send_sem=raw_ssem.at[0], recv_sem=raw_rsem.at[side],
            device_id={"row": to, "col": col}, device_id_type=MESH)

    raws = [raw_copy(f, side) for side in range(2) for f in range(2)]
    for cp in raws[2:] + raws[:2]:
        cp.start()

    def packed_copy(c):
        n = cuts[c + 1] - cuts[c]
        return pltpu.make_async_remote_copy(
            src_ref=pbuf.at[:, pl.ds(cuts[c], n)], dst_ref=hbuf.at[:, pl.ds(T + cuts[c], n)],
            send_sem=pk_ssem.at[0], recv_sem=pk_rsem.at[c],
            device_id={"row": row, "col": other}, device_id_type=MESH)

    def diag_copy(side):
        lo, at, to = ((0, T + ROWS, up), (ROWS - T, 0, down))[side]
        return pltpu.make_async_remote_copy(
            src_ref=pbuf.at[:, pl.ds(lo, T)], dst_ref=hbuf.at[:, pl.ds(at, T)],
            send_sem=pk_ssem.at[0], recv_sem=dg_rsem.at[side],
            device_id={"row": to, "col": other}, device_id_type=MESH)

    packs = [packed_copy(c) for c in range(TILES)]
    diags = [diag_copy(side) for side in range(2)]

    wait_stage(0)

    def pack(i, _):
        r = pl.multiple_of(i * 8, 8)
        for f, ref in ((0, uraw), (1, vraw)):
            pbuf[f, pl.ds(r, 8), :] = jnp.where(lane < 64, ref[pl.ds(r + T, 8), 0:128], ref[pl.ds(r + T, 8), 384:512])
        return 0

    lax.fori_loop((ROWS - T) // 8, ROWS // 8, pack, 0)
    lax.fori_loop(0, cuts[1] // 8, pack, 0)
    diags[1].start()
    packs[0].start()
    diags[0].start()
    wait_stage(1)
    lax.fori_loop(cuts[1] // 8, (ROWS - T) // 8, pack, 0)
    packs[1].start()
    packs[2].start()

    wait_stage(2)
    weights.wait()

    def lanes(x, idx):
        return jnp.take_along_axis(x, idx, axis=1, mode="promise_in_bounds")

    def put_main(c):
        residue = maps[2 * G]
        for g in range(G):
            idx = maps[g]
            masks = [residue == (g + 1 + 2 * k) % G for k in range(3)]
            for n in range(NG):
                r = pl.multiple_of(c * TILE + 8 * n, 8)
                q = pl.multiple_of(c * TILE + (OFF - T + 8 * n), 8)
                u, v = uraw[pl.ds(r, 8), 384:512], vraw[pl.ds(r, 8), 384:512]
                for k in range(3):
                    u = jnp.where(masks[k], uraw[pl.ds(r, 8), 128 * k:128 * k + 128], u)
                    v = jnp.where(masks[k], vraw[pl.ds(r, 8), 128 * k:128 * k + 128], v)
                x = 0.25 * lanes(u, idx)
                st[0, g + 1, pl.ds(q, 8), :] = x
                st[1, g + 1, pl.ds(q, 8), :] = x - 0.125 * lanes(v, idx)

    def put_halo(c):
        sv = st.at[:, :, pl.ds(pl.multiple_of(c * TILE + (OFF - T), 8), TILE)]
        hv = hbuf.at[:, pl.ds(pl.multiple_of(c * TILE, 8), TILE)]
        for g in range(G):
            idx = maps[g]
            column = lane * G + (g - 64)
            halo = (column < 0) | (column >= COLS)
            for n in range(NG):
                rows = pl.ds(8 * n, 8)
                h = 0.25 * lanes(hv[0, rows, :], idx)
                x = jnp.where(halo, h, sv[0, g + 1, rows, :])
                sv[0, g + 1, rows, :] = x
                sv[1, g + 1, rows, :] = jnp.where(halo, h - 0.125 * lanes(hv[1, rows, :], idx), sv[1, g + 1, rows, :])
                if g == 0:
                    sv[0, G + 1, rows, :] = pltpu.roll(x, 127, 1)
                if g == G - 1:
                    sv[0, 0, rows, :] = pltpu.roll(x, 1, 1)

    def put_tile(i, _):
        @pl.when(i == 1)
        def _():
            wait_bytes(uraw.at[pl.ds(0, 2 * T)], raw_rsem.at[1])
            wait_bytes(uraw.at[pl.ds(0, 2 * T)], raw_rsem.at[0])
            wait_bytes(uraw.at[pl.ds(0, 4 * T)], raw_ssem.at[0])

        put_main(lax.rem(i + 1, TILES))
        return 0

    lax.fori_loop(0, TILES, put_tile, 0)

    def merge(lo, groups):
        residue = maps[2 * G]
        for f, out in ((0, now_ref), (1, before_ref)):
            ov = out.at[pl.ds(lo, 8 * groups)]
            for n in range(groups):
                for k in range(4):
                    x = zbuf[f, 0, 8 * n:8 * n + 8, :]
                    for g in range(1, G):
                        x = jnp.where(residue == (g + 1 + 2 * k) % G, zbuf[f, g, 8 * n:8 * n + 8, :], x)
                    ov[8 * n:8 * n + 8, 128 * k:128 * k + 128] = x

    def get(lo, groups):
        for g in range(G):
            for n in range(groups):
                for f in range(2):
                    zbuf[f, g, 8 * n:8 * n + 8, :] = lanes(st[f, g + 1, pl.ds(lo + OFF + 8 * n, 8), :], maps[G + g])
        merge(lo, groups)

    def run(t, base, sign, first, lo=None):
        drops = [2 * (k + 1) // 8 if first else 0 for k in range(T)]
        tops = [sign * (k + 1) + (8 * drops[k] if sign < 0 else 0) for k in range(T)]
        low = min(tops) - 1
        high = max(top + TILE - 8 * drop for top, drop in zip(tops, drops)) + 1
        done = TILE + T
        if lo is not None:
            high = max(high, done + 8 * EARLY)
        sv = st.at[:, :, pl.ds(base + low, high - low)]
        for k in range(T):
            src, dst = k % 2, 1 - k % 2
            wa, wb, wc, wd, we = [0.5 * w_ref[a, b, t + k] for a, b in ((0, 0), (0, 1), (0, 2), (1, 0), (1, 1))]
            blocks = []
            at, left = tops[k] - low, NG - drops[k]
            while left:
                n = min(left, BLOCK if left > BLOCK + 1 or left == BLOCK else (left + 1) // 2)
                blocks.append((at, 8 * n))
                at, left = at + 8 * n, left - n
            for q, rows in blocks if sign < 0 else blocks[::-1]:
                ca, cb, cc, cd, ce = [jnp.full((G, rows, 128), x, F32) for x in (wa, wb, wc, wd, 1.5 + we)]
                n = sv[src, :, pl.ds(q - 1, rows), :]
                m = sv[src, :, pl.ds(q, rows), :]
                s = sv[src, :, pl.ds(q + 1, rows), :]
                x = (ca * (n[0:G] + s[2:G + 2]) + cc * (n[2:G + 2] + s[0:G])) + (cb * (n[1:G + 1] + s[1:G + 1]) + cd * (m[0:G] + m[2:G + 2]))
                x = x + (ce * m[1:G + 1] - sv[dst, 1:G + 1, pl.ds(q, rows), :])
                sv[dst, 1:G + 1, pl.ds(q, rows), :] = x
                sv[dst, G + 1, pl.ds(q, rows), :] = pltpu.roll(x[0], 127, 1)
                sv[dst, 0, pl.ds(q, rows), :] = pltpu.roll(x[G - 1], 1, 1)
            if lo is not None and k in ORDER_STEPS:
                g = ORDER_STEPS.index(k)
                for n in range(EARLY):
                    for f in range(2):
                        zbuf[f, g, 8 * n:8 * n + 8, :] = lanes(sv[f, g + 1, pl.ds(done - low + 8 * n, 8), :], maps[G + g])
        if lo is not None:
            merge(lo, EARLY)

    def exchange(e, side, to, late):
        src = sbuf.at[e] if late else st.at[:, pl.ds(1, G), pl.ds(jnp.where(side == 0, OFF, OFF + ROWS - T), T)]
        return pltpu.make_async_remote_copy(
            src_ref=src, dst_ref=rbuf.at[e, side],
            send_sem=ex_ssem.at[int(late)], recv_sem=ex_rsem.at[e, side],
            device_id={"row": to, "col": col}, device_id_type=MESH)

    def tile(it, _):
        sweep, c = lax.div(it, TILES), lax.rem(it, TILES)
        odd = lax.rem(sweep, 2)
        base = jnp.where(odd == 0, OFF - T + TILE * c, OFF + ROWS + T - TILE * (c + 1))

        @pl.when(it == 0)
        def _():
            diags[1].wait_recv()
            packs[0].wait_recv()

        @pl.when(it == 1)
        def _():
            packs[1].wait_recv()

        @pl.when(it == 2)
        def _():
            diags[0].wait_recv()
            packs[2].wait_recv()

        @pl.when(sweep == 0)
        def _():
            put_halo(c)

        first = odd
        last = 1 - odd
        to_first = jnp.where(odd == 0, up, down)
        to_last = jnp.where(odd == 0, down, up)

        def put_rows(side):
            at = jnp.where(side == 0, OFF - T, OFF + ROWS)
            for k in range(T // 8):
                q = pl.multiple_of(at + 8 * k, 8)
                for g in range(G):
                    x = rbuf[sweep - 1, 1 - side, 0, g, pl.ds(8 * k, 8), :]
                    st[0, g + 1, pl.ds(q, 8), :] = x
                    if g == 0:
                        st[0, G + 1, pl.ds(q, 8), :] = pltpu.roll(x, 127, 1)
                    if g == G - 1:
                        st[0, 0, pl.ds(q, 8), :] = pltpu.roll(x, 1, 1)
                    st[1, g + 1, pl.ds(q, 8), :] = rbuf[sweep - 1, 1 - side, 1, g, pl.ds(8 * k, 8), :]

        @pl.when((sweep > 0) & (c == 0))
        def _():
            at = jnp.where(first == 0, OFF, OFF + ROWS - T)
            for k in range(T // 8):
                q = pl.multiple_of(at + 8 * k, 8)
                for f in range(2):
                    for g in range(G):
                        sbuf[sweep - 1, f, g, pl.ds(8 * k, 8), :] = st[f, g + 1, pl.ds(q, 8), :]
            exchange(sweep - 1, 1 - first, up, True).wait_recv()
            put_rows(first)
            exchange(sweep - 1, first, to_first, True).start()

        @pl.when((sweep > 0) & (c == 1))
        def _():
            exchange(sweep - 1, last, up, False).wait_send()

        @pl.when((sweep < SWEEPS - 1) & (c == 1))
        def _():
            exchange(sweep, first, to_first, False).start()

        @pl.when((sweep > 0) & (c == TILES - 1))
        def _():
            exchange(sweep - 1, 1 - last, up, True).wait_recv()
            put_rows(last)

        for sign in (-1, 1):
            for begins in (True, False):
                @pl.when((2 * odd - 1 == sign) & ((c == 0) == begins) & ((sweep < SWEEPS - 1) | begins))
                def _():
                    run(sweep * T, base, sign, begins)

        @pl.when((sweep == SWEEPS - 1) & (c > 0))
        def _():
            run(sweep * T, base, 1, False, pl.multiple_of(ROWS + 2 * T - TILE * c, 8))

        return 0

    lax.fori_loop(0, SWEEPS * TILES, tile, 0)
    get(0, NG)
    get(ROWS + 2 * T - 2 * TILE + 8 * EARLY, NG - EARLY)

    wait_bytes(hbuf, pk_ssem.at[0])
    wait_bytes(sbuf, ex_ssem.at[1])


def solution(mesh):
    def local_run(u_tile, v_tile, w):
        dma = pltpu.SemaphoreType.DMA
        now, before = pl.pallas_call(
            wave_kernel,
            out_shape=[jax.ShapeDtypeStruct((ROWS, COLS), F32)] * 2,
            in_specs=[pl.BlockSpec(memory_space=pl.ANY)] * 3,
            out_specs=[pl.BlockSpec(memory_space=pltpu.VMEM)] * 2,
            scratch_shapes=[
                pltpu.VMEM((2, G + 2, R, 128), F32), pltpu.SMEM((3, 3, SWEEPS * T), F32), pltpu.VMEM((2 * G + 1, 8, 128), jnp.int32),
                pltpu.VMEM((ROWS + 2 * T, COLS), F32), pltpu.VMEM((ROWS + 2 * T, COLS), F32),
                pltpu.VMEM((2, ROWS, 128), F32), pltpu.VMEM((2, ROWS + 2 * T, 128), F32), pltpu.VMEM((2, G, TILE, 128), F32),
                pltpu.VMEM((SWEEPS - 1, 2, G, T, 128), F32), pltpu.VMEM((SWEEPS - 1, 2, 2, G, T, 128), F32),
                dma((4,)), dma((1,)), dma((2,)), dma((1,)), dma((TILES,)), dma((2,)), dma((2,)), dma((SWEEPS - 1, 2)),
            ],
            compiler_params=pltpu.CompilerParams(collective_id=0, has_side_effects=True, vmem_limit_bytes=VMEM_LIMIT),
        )(u_tile, v_tile, pltpu.with_memory_space_constraint(jnp.transpose(w, (1, 2, 0)), pltpu.HBM))
        return 4.0 * now, 8.0 * (now - before)

    tile_spec = P(("ens", "row"), "col")
    return jax.shard_map(local_run, mesh=mesh, in_specs=(tile_spec, tile_spec, P()), out_specs=(tile_spec, tile_spec), check_vma=False)
```

```python
import jax
import jax.numpy as jnp
from jax import lax
from jax.experimental import pallas as pl
from jax.experimental.pallas import tpu as pltpu
from jax.sharding import PartitionSpec as P

F32 = jnp.float32
MESH = pl.DeviceIdType.MESH
ROWS, COLS = 256, 512
G = 5
T = 16
SWEEPS = 4
TILES = 3
TILE = (ROWS + 2 * T) // TILES
NG = TILE // 8
BLOCK = 4
OFF = 32
R = 328
VMEM_LIMIT = 55_300_000


def wave_kernel(u_hbm, v_hbm, w_hbm, now_ref, before_ref, st, w_ref, maps, uraw, vraw, pbuf, hbuf, zbuf, sbuf, rbuf,
                load_sem, raw_ssem, raw_rsem, pk_ssem, pk_rsem, dg_rsem, ex_ssem, ex_rsem):
    row = lax.axis_index("row")
    col = lax.axis_index("col")
    up = lax.rem(row + 3, 4)
    down = lax.rem(row + 1, 4)
    other = 1 - col

    barrier = pltpu.get_barrier_semaphore()
    for rr, cc in ((row, other), (up, col), (down, col), (up, other), (down, other)):
        pl.semaphore_signal(barrier, inc=1, device_id={"row": rr, "col": cc}, device_id_type=MESH)

    cuts = [0, TILE // 2 - T] + [TILE * (c + 1) - T for c in range(TILES - 1)] + [ROWS]

    stages = [[(lo, n, at, 128) for lo, n in spans for at in (0, COLS - 128)]
              for spans in (((ROWS - T, T), (0, cuts[2])), ((cuts[2], ROWS - T - cuts[2]),))]
    stages.append([(0, ROWS, 128, COLS - 256)])

    def start_stage(k):
        for lo, n, at, m in stages[k]:
            for src, dst in ((u_hbm, uraw), (v_hbm, vraw)):
                pltpu.make_async_copy(src.at[pl.ds(lo, n), pl.ds(at, m)], dst.at[pl.ds(T + lo, n), pl.ds(at, m)], load_sem.at[k]).start()

    start_stage(0)
    start_stage(1)
    weights = pltpu.make_async_copy(w_hbm, w_ref, load_sem.at[3])
    weights.start()

    def wait_bytes(ref, sem):
        pltpu.make_async_copy(ref, ref, sem).wait()

    def wait_stage(k):
        wait_bytes(uraw.at[pl.ds(0, sum(n * m for _, n, _, m in stages[k]) * 2 // COLS)], load_sem.at[k])

    def zero(i, _):
        for f in range(2):
            for g in range(G + 2):
                st[f, g, pl.ds(pl.multiple_of(i * 8, 8), 8), :] = jnp.zeros((8, 128), F32)
        return 0

    lax.fori_loop(0, (OFF - T) // 8, zero, 0)
    lax.fori_loop((OFF + ROWS + T) // 8, R // 8, zero, 0)

    lane = lax.broadcasted_iota(jnp.int32, (8, 128), 1)
    maps[2 * G] = lax.rem(lane, G)
    for g in range(G):
        maps[g] = lax.rem(lane * G + (g + 64), 128)
        k = lax.rem(3 * (lane + (2 * G - g - 1)), G)
        maps[G + g] = lax.div(lax.rem(128 * k + lane + 64, 128 * G), G)

    pl.semaphore_wait(barrier, 5)

    def raw_copy(f, side):
        src = (u_hbm, v_hbm)[f]
        dst = (uraw, vraw)[f]
        lo, at, to = ((0, T + ROWS, up), (ROWS - T, 0, down))[side]
        return pltpu.make_async_remote_copy(
            src_ref=src.at[pl.ds(lo, T)], dst_ref=dst.at[pl.ds(at, T)],
            send_sem=raw_ssem.at[0], recv_sem=raw_rsem.at[side],
            device_id={"row": to, "col": col}, device_id_type=MESH)

    raws = [raw_copy(f, side) for side in range(2) for f in range(2)]
    for cp in raws[2:] + raws[:2]:
        cp.start()

    def packed_copy(c):
        n = cuts[c + 1] - cuts[c]
        return pltpu.make_async_remote_copy(
            src_ref=pbuf.at[:, pl.ds(cuts[c], n)], dst_ref=hbuf.at[:, pl.ds(T + cuts[c], n)],
            send_sem=pk_ssem.at[0], recv_sem=pk_rsem.at[c],
            device_id={"row": row, "col": other}, device_id_type=MESH)

    def diag_copy(side):
        lo, at, to = ((0, T + ROWS, up), (ROWS - T, 0, down))[side]
        return pltpu.make_async_remote_copy(
            src_ref=pbuf.at[:, pl.ds(lo, T)], dst_ref=hbuf.at[:, pl.ds(at, T)],
            send_sem=pk_ssem.at[0], recv_sem=dg_rsem.at[side],
            device_id={"row": to, "col": other}, device_id_type=MESH)

    packs = [packed_copy(c) for c in range(TILES + 1)]
    diags = [diag_copy(side) for side in range(2)]

    wait_stage(0)
    start_stage(2)

    def pack(i, _):
        r = pl.multiple_of(i * 8, 8)
        for f, ref in ((0, uraw), (1, vraw)):
            pbuf[f, pl.ds(r, 8), :] = jnp.where(lane < 64, ref[pl.ds(r + T, 8), 0:128], ref[pl.ds(r + T, 8), 384:512])
        return 0

    lax.fori_loop((ROWS - T) // 8, ROWS // 8, pack, 0)
    lax.fori_loop(0, cuts[2] // 8, pack, 0)
    diags[1].start()
    packs[0].start()
    packs[1].start()
    diags[0].start()
    wait_stage(1)
    lax.fori_loop(cuts[2] // 8, (ROWS - T) // 8, pack, 0)
    packs[2].start()
    packs[3].start()

    wait_stage(2)
    weights.wait()

    def lanes(x, idx):
        return jnp.take_along_axis(x, idx, axis=1, mode="promise_in_bounds")

    def put_main(c):
        residue = maps[2 * G]
        for g in range(G):
            idx = maps[g]
            masks = [residue == (g + 1 + 2 * k) % G for k in range(3)]
            for n in range(NG):
                r = pl.multiple_of(c * TILE + 8 * n, 8)
                q = pl.multiple_of(c * TILE + (OFF - T + 8 * n), 8)
                u, v = uraw[pl.ds(r, 8), 384:512], vraw[pl.ds(r, 8), 384:512]
                for k in range(3):
                    u = jnp.where(masks[k], uraw[pl.ds(r, 8), 128 * k:128 * k + 128], u)
                    v = jnp.where(masks[k], vraw[pl.ds(r, 8), 128 * k:128 * k + 128], v)
                x = 0.25 * lanes(u, idx)
                st[0, g + 1, pl.ds(q, 8), :] = x
                st[1, g + 1, pl.ds(q, 8), :] = x - 0.125 * lanes(v, idx)

    def put_halo(at, groups):
        sv = st.at[:, :, pl.ds(at + (OFF - T), 8 * groups)]
        hv = hbuf.at[:, pl.ds(at, 8 * groups)]
        for g in range(G):
            idx = maps[g]
            column = lane * G + (g - 64)
            halo = (column < 0) | (column >= COLS)
            for n in range(groups):
                rows = pl.ds(8 * n, 8)
                h = 0.25 * lanes(hv[0, rows, :], idx)
                x = jnp.where(halo, h, sv[0, g + 1, rows, :])
                sv[0, g + 1, rows, :] = x
                sv[1, g + 1, rows, :] = jnp.where(halo, h - 0.125 * lanes(hv[1, rows, :], idx), sv[1, g + 1, rows, :])
                if g == 0:
                    sv[0, G + 1, rows, :] = pltpu.roll(x, 127, 1)
                if g == G - 1:
                    sv[0, 0, rows, :] = pltpu.roll(x, 1, 1)

    def put_tile(i, _):
        @pl.when(i == 1)
        def _():
            wait_bytes(uraw.at[pl.ds(0, 2 * T)], raw_rsem.at[1])
            wait_bytes(uraw.at[pl.ds(0, 2 * T)], raw_rsem.at[0])
            wait_bytes(uraw.at[pl.ds(0, 4 * T)], raw_ssem.at[0])

        put_main(lax.rem(i + 1, TILES))
        return 0

    lax.fori_loop(0, TILES, put_tile, 0)

    def run(t, base, sign, first):
        drops = [2 * (k + 1) // 8 if first else 0 for k in range(T)]
        tops = [sign * (k + 1) + (8 * drops[k] if sign < 0 else 0) for k in range(T)]
        low = min(tops) - 1
        high = max(top + TILE - 8 * drop for top, drop in zip(tops, drops)) + 1
        sv = st.at[:, :, pl.ds(base + low, high - low)]
        for k in range(T):
            src, dst = k % 2, 1 - k % 2
            wa, wb, wc, wd, we = [0.5 * w_ref[a, b, t + k] for a, b in ((0, 0), (0, 1), (0, 2), (1, 0), (1, 1))]
            blocks = []
            at, left = tops[k] - low, NG - drops[k]
            while left:
                n = min(left, BLOCK if left > BLOCK + 1 or left == BLOCK else (left + 1) // 2)
                blocks.append((at, 8 * n))
                at, left = at + 8 * n, left - n
            for q, rows in blocks if sign < 0 else blocks[::-1]:
                ca, cb, cc, cd, ce = [jnp.full((G, rows, 128), x, F32) for x in (wa, wb, wc, wd, 1.5 + we)]
                n = sv[src, :, pl.ds(q - 1, rows), :]
                m = sv[src, :, pl.ds(q, rows), :]
                s = sv[src, :, pl.ds(q + 1, rows), :]
                x = (ca * (n[0:G] + s[2:G + 2]) + cc * (n[2:G + 2] + s[0:G])) + (cb * (n[1:G + 1] + s[1:G + 1]) + cd * (m[0:G] + m[2:G + 2]))
                x = x + (ce * m[1:G + 1] - sv[dst, 1:G + 1, pl.ds(q, rows), :])
                sv[dst, 1:G + 1, pl.ds(q, rows), :] = x
                sv[dst, G + 1, pl.ds(q, rows), :] = pltpu.roll(x[0], 127, 1)
                sv[dst, 0, pl.ds(q, rows), :] = pltpu.roll(x[G - 1], 1, 1)

    def exchange(e, side, to, late):
        src = sbuf.at[e] if late else st.at[:, pl.ds(1, G), pl.ds(jnp.where(side == 0, OFF, OFF + ROWS - T), T)]
        return pltpu.make_async_remote_copy(
            src_ref=src, dst_ref=rbuf.at[e, side],
            send_sem=ex_ssem.at[int(late)], recv_sem=ex_rsem.at[e, side],
            device_id={"row": to, "col": col}, device_id_type=MESH)

    def get(lo):
        for g in range(G):
            idx = maps[G + g]
            for n in range(NG):
                q = pl.multiple_of(lo + (OFF + 8 * n), 8)
                for f in range(2):
                    zbuf[f, g, 8 * n:8 * n + 8, :] = lanes(st[f, g + 1, pl.ds(q, 8), :], idx)
        residue = maps[2 * G]
        for n in range(NG):
            r = pl.multiple_of(lo + 8 * n, 8)
            for f, out in ((0, now_ref), (1, before_ref)):
                for k in range(4):
                    x = zbuf[f, 0, 8 * n:8 * n + 8, :]
                    for g in range(1, G):
                        x = jnp.where(residue == (g + 1 + 2 * k) % G, zbuf[f, g, 8 * n:8 * n + 8, :], x)
                    out[pl.ds(r, 8), 128 * k:128 * k + 128] = x

    def tile(it, _):
        sweep, c = lax.div(it, TILES), lax.rem(it, TILES)
        odd = lax.rem(sweep, 2)
        base = jnp.where(odd == 0, OFF - T + TILE * c, OFF + ROWS + T - TILE * (c + 1))

        @pl.when(it == 0)
        def _():
            diags[1].wait_recv()
            packs[0].wait_recv()
            put_halo(0, NG // 2)
            packs[1].wait_recv()
            put_halo(TILE // 2, NG // 2)

        @pl.when(it == 1)
        def _():
            packs[2].wait_recv()

        @pl.when(it == 2)
        def _():
            diags[0].wait_recv()
            packs[3].wait_recv()

        @pl.when((sweep == 0) & (c > 0))
        def _():
            put_halo(pl.multiple_of(c * TILE, 8), NG)

        first = odd
        last = 1 - odd
        to_first = jnp.where(odd == 0, up, down)
        to_last = jnp.where(odd == 0, down, up)

        def put_rows(side):
            at = jnp.where(side == 0, OFF - T, OFF + ROWS)
            for k in range(T // 8):
                q = pl.multiple_of(at + 8 * k, 8)
                for g in range(G):
                    x = rbuf[sweep - 1, 1 - side, 0, g, pl.ds(8 * k, 8), :]
                    st[0, g + 1, pl.ds(q, 8), :] = x
                    if g == 0:
                        st[0, G + 1, pl.ds(q, 8), :] = pltpu.roll(x, 127, 1)
                    if g == G - 1:
                        st[0, 0, pl.ds(q, 8), :] = pltpu.roll(x, 1, 1)
                    st[1, g + 1, pl.ds(q, 8), :] = rbuf[sweep - 1, 1 - side, 1, g, pl.ds(8 * k, 8), :]

        @pl.when((sweep > 0) & (c == 0))
        def _():
            at = jnp.where(first == 0, OFF, OFF + ROWS - T)
            for k in range(T // 8):
                q = pl.multiple_of(at + 8 * k, 8)
                for f in range(2):
                    for g in range(G):
                        sbuf[sweep - 1, f, g, pl.ds(8 * k, 8), :] = st[f, g + 1, pl.ds(q, 8), :]
            exchange(sweep - 1, 1 - first, up, True).wait_recv()
            put_rows(first)
            exchange(sweep - 1, first, to_first, True).start()

        @pl.when((sweep > 0) & (c == 1))
        def _():
            exchange(sweep - 1, last, up, False).wait_send()

        @pl.when((sweep < SWEEPS - 1) & (c == 1))
        def _():
            exchange(sweep, first, to_first, False).start()

        @pl.when((sweep > 0) & (c == TILES - 1))
        def _():
            exchange(sweep - 1, 1 - last, up, True).wait_recv()
            put_rows(last)

        for sign in (-1, 1):
            for begins in (True, False):
                @pl.when((2 * odd - 1 == sign) & ((c == 0) == begins))
                def _():
                    run(sweep * T, base, sign, begins)

        @pl.when(sweep == SWEEPS - 1)
        def _():
            get(pl.multiple_of(jnp.where(c == 0, ROWS - TILE, (TILES - 1 - c) * TILE), 8))

        return 0

    lax.fori_loop(0, SWEEPS * TILES, tile, 0)

    wait_bytes(hbuf, pk_ssem.at[0])
    wait_bytes(sbuf, ex_ssem.at[1])


def solution(mesh):
    def local_run(u_tile, v_tile, w):
        dma = pltpu.SemaphoreType.DMA
        now, before = pl.pallas_call(
            wave_kernel,
            out_shape=[jax.ShapeDtypeStruct((ROWS, COLS), F32)] * 2,
            in_specs=[pl.BlockSpec(memory_space=pl.ANY)] * 3,
            out_specs=[pl.BlockSpec(memory_space=pltpu.VMEM)] * 2,
            scratch_shapes=[
                pltpu.VMEM((2, G + 2, R, 128), F32), pltpu.SMEM((3, 3, SWEEPS * T), F32), pltpu.VMEM((2 * G + 1, 8, 128), jnp.int32),
                pltpu.VMEM((ROWS + 2 * T, COLS), F32), pltpu.VMEM((ROWS + 2 * T, COLS), F32),
                pltpu.VMEM((2, ROWS, 128), F32), pltpu.VMEM((2, ROWS + 2 * T, 128), F32), pltpu.VMEM((2, G, TILE, 128), F32),
                pltpu.VMEM((SWEEPS - 1, 2, G, T, 128), F32), pltpu.VMEM((SWEEPS - 1, 2, 2, G, T, 128), F32),
                dma((4,)), dma((1,)), dma((2,)), dma((1,)), dma((TILES + 1,)), dma((2,)), dma((2,)), dma((SWEEPS - 1, 2)),
            ],
            compiler_params=pltpu.CompilerParams(collective_id=0, has_side_effects=True, vmem_limit_bytes=VMEM_LIMIT),
        )(u_tile, v_tile, pltpu.with_memory_space_constraint(jnp.transpose(w, (1, 2, 0)), pltpu.HBM))
        return 4.0 * now, 8.0 * (now - before)

    tile_spec = P(("ens", "row"), "col")
    return jax.shard_map(local_run, mesh=mesh, in_specs=(tile_spec, tile_spec, P()), out_specs=(tile_spec, tile_spec), check_vma=False)
```

```python
import jax
import jax.numpy as jnp
from jax import lax
from jax.experimental import pallas as pl
from jax.experimental.pallas import tpu as pltpu
from jax.sharding import PartitionSpec as P

F32 = jnp.float32
MESH = pl.DeviceIdType.MESH
ROWS, COLS = 256, 512
G = 5
T = 16
SWEEPS = 4
TILES = 3
TILE = (ROWS + 2 * T) // TILES
NG = TILE // 8
BLOCK = 4
OFF = 32
R = 328
VMEM_LIMIT = 55_300_000


def wave_kernel(u_hbm, v_hbm, w_hbm, now_ref, before_ref, st, w_ref, maps, uraw, vraw, pbuf, hbuf, zbuf, sbuf, rbuf,
                load_sem, raw_ssem, raw_rsem, pk_ssem, pk_rsem, dg_rsem, ex_ssem, ex_rsem):
    row = lax.axis_index("row")
    col = lax.axis_index("col")
    up = lax.rem(row + 3, 4)
    down = lax.rem(row + 1, 4)
    other = 1 - col

    barrier = pltpu.get_barrier_semaphore()
    for rr, cc in ((row, other), (up, col), (down, col), (up, other), (down, other)):
        pl.semaphore_signal(barrier, inc=1, device_id={"row": rr, "col": cc}, device_id_type=MESH)

    cuts = [0, TILE // 2 - T] + [TILE * (c + 1) - T for c in range(TILES - 1)] + [ROWS]

    stages = [[(lo, n, at, 128) for lo, n in spans for at in (0, COLS - 128)]
              for spans in (((ROWS - T, T), (0, cuts[2])), ((cuts[2], ROWS - T - cuts[2]),))]
    stages.append([(0, ROWS, 128, COLS - 256)])

    def start_stage(k):
        for lo, n, at, m in stages[k]:
            for src, dst in ((u_hbm, uraw), (v_hbm, vraw)):
                pltpu.make_async_copy(src.at[pl.ds(lo, n), pl.ds(at, m)], dst.at[pl.ds(T + lo, n), pl.ds(at, m)], load_sem.at[k]).start()

    start_stage(0)
    start_stage(1)
    weights = pltpu.make_async_copy(w_hbm, w_ref, load_sem.at[3])
    weights.start()

    def wait_bytes(ref, sem):
        pltpu.make_async_copy(ref, ref, sem).wait()

    def wait_stage(k):
        wait_bytes(uraw.at[pl.ds(0, sum(n * m for _, n, _, m in stages[k]) * 2 // COLS)], load_sem.at[k])

    def zero(i, _):
        for f in range(2):
            for g in range(G + 2):
                st[f, g, pl.ds(pl.multiple_of(i * 8, 8), 8), :] = jnp.zeros((8, 128), F32)
        return 0

    lax.fori_loop(0, (OFF - T) // 8, zero, 0)
    lax.fori_loop((OFF + ROWS + T) // 8, R // 8, zero, 0)

    lane = lax.broadcasted_iota(jnp.int32, (8, 128), 1)
    maps[2 * G] = lax.rem(lane, G)
    for g in range(G):
        maps[g] = lax.rem(lane * G + (g + 64), 128)
        k = lax.rem(3 * (lane + (2 * G - g - 1)), G)
        maps[G + g] = lax.div(lax.rem(128 * k + lane + 64, 128 * G), G)

    pl.semaphore_wait(barrier, 5)

    def raw_copy(f, side):
        src = (u_hbm, v_hbm)[f]
        dst = (uraw, vraw)[f]
        lo, at, to = ((0, T + ROWS, up), (ROWS - T, 0, down))[side]
        return pltpu.make_async_remote_copy(
            src_ref=src.at[pl.ds(lo, T)], dst_ref=dst.at[pl.ds(at, T)],
            send_sem=raw_ssem.at[0], recv_sem=raw_rsem.at[side],
            device_id={"row": to, "col": col}, device_id_type=MESH)

    raws = [raw_copy(f, side) for side in range(2) for f in range(2)]
    for cp in raws[2:] + raws[:2]:
        cp.start()

    def packed_copy(c):
        n = cuts[c + 1] - cuts[c]
        return pltpu.make_async_remote_copy(
            src_ref=pbuf.at[:, pl.ds(cuts[c], n)], dst_ref=hbuf.at[:, pl.ds(T + cuts[c], n)],
            send_sem=pk_ssem.at[0], recv_sem=pk_rsem.at[c],
            device_id={"row": row, "col": other}, device_id_type=MESH)

    def diag_copy(side):
        lo, at, to = ((0, T + ROWS, up), (ROWS - T, 0, down))[side]
        return pltpu.make_async_remote_copy(
            src_ref=pbuf.at[:, pl.ds(lo, T)], dst_ref=hbuf.at[:, pl.ds(at, T)],
            send_sem=pk_ssem.at[0], recv_sem=dg_rsem.at[side],
            device_id={"row": to, "col": other}, device_id_type=MESH)

    packs = [packed_copy(c) for c in range(TILES + 1)]
    diags = [diag_copy(side) for side in range(2)]

    wait_stage(0)
    start_stage(2)

    def pack(i, _):
        r = pl.multiple_of(i * 8, 8)
        for f, ref in ((0, uraw), (1, vraw)):
            pbuf[f, pl.ds(r, 8), :] = jnp.where(lane < 64, ref[pl.ds(r + T, 8), 0:128], ref[pl.ds(r + T, 8), 384:512])
        return 0

    lax.fori_loop((ROWS - T) // 8, ROWS // 8, pack, 0)
    lax.fori_loop(0, cuts[2] // 8, pack, 0)
    diags[1].start()
    packs[0].start()
    packs[1].start()
    wait_stage(1)
    lax.fori_loop(cuts[2] // 8, (ROWS - T) // 8, pack, 0)
    packs[2].start()
    diags[0].start()
    packs[3].start()

    wait_stage(2)
    weights.wait()

    def lanes(x, idx):
        return jnp.take_along_axis(x, idx, axis=1, mode="promise_in_bounds")

    def put_main(c):
        residue = maps[2 * G]
        for g in range(G):
            idx = maps[g]
            masks = [residue == (g + 1 + 2 * k) % G for k in range(3)]
            for n in range(NG):
                r = pl.multiple_of(c * TILE + 8 * n, 8)
                q = pl.multiple_of(c * TILE + (OFF - T + 8 * n), 8)
                u, v = uraw[pl.ds(r, 8), 384:512], vraw[pl.ds(r, 8), 384:512]
                for k in range(3):
                    u = jnp.where(masks[k], uraw[pl.ds(r, 8), 128 * k:128 * k + 128], u)
                    v = jnp.where(masks[k], vraw[pl.ds(r, 8), 128 * k:128 * k + 128], v)
                x = 0.25 * lanes(u, idx)
                st[0, g + 1, pl.ds(q, 8), :] = x
                st[1, g + 1, pl.ds(q, 8), :] = x - 0.125 * lanes(v, idx)

    def put_halo(at, groups):
        sv = st.at[:, :, pl.ds(at + (OFF - T), 8 * groups)]
        hv = hbuf.at[:, pl.ds(at, 8 * groups)]
        for g in range(G):
            idx = maps[g]
            column = lane * G + (g - 64)
            halo = (column < 0) | (column >= COLS)
            for n in range(groups):
                rows = pl.ds(8 * n, 8)
                h = 0.25 * lanes(hv[0, rows, :], idx)
                x = jnp.where(halo, h, sv[0, g + 1, rows, :])
                sv[0, g + 1, rows, :] = x
                sv[1, g + 1, rows, :] = jnp.where(halo, h - 0.125 * lanes(hv[1, rows, :], idx), sv[1, g + 1, rows, :])
                if g == 0:
                    sv[0, G + 1, rows, :] = pltpu.roll(x, 127, 1)
                if g == G - 1:
                    sv[0, 0, rows, :] = pltpu.roll(x, 1, 1)

    def put_tile(i, _):
        @pl.when(i == 1)
        def _():
            wait_bytes(uraw.at[pl.ds(0, 2 * T)], raw_rsem.at[1])
            wait_bytes(uraw.at[pl.ds(0, 2 * T)], raw_rsem.at[0])
            wait_bytes(uraw.at[pl.ds(0, 4 * T)], raw_ssem.at[0])

        put_main(lax.rem(i + 1, TILES))
        return 0

    lax.fori_loop(0, TILES, put_tile, 0)

    def run(t, base, sign, first):
        drops = [2 * (k + 1) // 8 if first else 0 for k in range(T)]
        tops = [sign * (k + 1) + (8 * drops[k] if sign < 0 else 0) for k in range(T)]
        low = min(tops) - 1
        high = max(top + TILE - 8 * drop for top, drop in zip(tops, drops)) + 1
        sv = st.at[:, :, pl.ds(base + low, high - low)]
        for k in range(T):
            src, dst = k % 2, 1 - k % 2
            wa, wb, wc, wd, we = [0.5 * w_ref[a, b, t + k] for a, b in ((0, 0), (0, 1), (0, 2), (1, 0), (1, 1))]
            blocks = []
            at, left = tops[k] - low, NG - drops[k]
            while left:
                n = min(left, BLOCK if left > BLOCK + 1 or left == BLOCK else (left + 1) // 2)
                blocks.append((at, 8 * n))
                at, left = at + 8 * n, left - n
            for q, rows in blocks if sign < 0 else blocks[::-1]:
                ca, cb, cc, cd, ce = [jnp.full((G, rows, 128), x, F32) for x in (wa, wb, wc, wd, 1.5 + we)]
                n = sv[src, :, pl.ds(q - 1, rows), :]
                m = sv[src, :, pl.ds(q, rows), :]
                s = sv[src, :, pl.ds(q + 1, rows), :]
                x = (ca * (n[0:G] + s[2:G + 2]) + cc * (n[2:G + 2] + s[0:G])) + (cb * (n[1:G + 1] + s[1:G + 1]) + cd * (m[0:G] + m[2:G + 2]))
                x = x + (ce * m[1:G + 1] - sv[dst, 1:G + 1, pl.ds(q, rows), :])
                sv[dst, 1:G + 1, pl.ds(q, rows), :] = x
                sv[dst, G + 1, pl.ds(q, rows), :] = pltpu.roll(x[0], 127, 1)
                sv[dst, 0, pl.ds(q, rows), :] = pltpu.roll(x[G - 1], 1, 1)

    def exchange(e, side, to, late):
        src = sbuf.at[e] if late else st.at[:, pl.ds(1, G), pl.ds(jnp.where(side == 0, OFF, OFF + ROWS - T), T)]
        return pltpu.make_async_remote_copy(
            src_ref=src, dst_ref=rbuf.at[e, side],
            send_sem=ex_ssem.at[int(late)], recv_sem=ex_rsem.at[e, side],
            device_id={"row": to, "col": col}, device_id_type=MESH)

    def get(lo):
        for g in range(G):
            idx = maps[G + g]
            for n in range(NG):
                q = pl.multiple_of(lo + (OFF + 8 * n), 8)
                for f in range(2):
                    zbuf[f, g, 8 * n:8 * n + 8, :] = lanes(st[f, g + 1, pl.ds(q, 8), :], idx)
        residue = maps[2 * G]
        for n in range(NG):
            r = pl.multiple_of(lo + 8 * n, 8)
            for f, out in ((0, now_ref), (1, before_ref)):
                for k in range(4):
                    x = zbuf[f, 0, 8 * n:8 * n + 8, :]
                    for g in range(1, G):
                        x = jnp.where(residue == (g + 1 + 2 * k) % G, zbuf[f, g, 8 * n:8 * n + 8, :], x)
                    out[pl.ds(r, 8), 128 * k:128 * k + 128] = x

    def tile(it, _):
        sweep, c = lax.div(it, TILES), lax.rem(it, TILES)
        odd = lax.rem(sweep, 2)
        base = jnp.where(odd == 0, OFF - T + TILE * c, OFF + ROWS + T - TILE * (c + 1))

        @pl.when(it == 0)
        def _():
            diags[1].wait_recv()
            packs[0].wait_recv()
            put_halo(0, NG // 2)
            packs[1].wait_recv()
            put_halo(TILE // 2, NG // 2)

        @pl.when(it == 1)
        def _():
            packs[2].wait_recv()

        @pl.when(it == 2)
        def _():
            diags[0].wait_recv()
            packs[3].wait_recv()

        @pl.when((sweep == 0) & (c > 0))
        def _():
            put_halo(pl.multiple_of(c * TILE, 8), NG)

        first = odd
        last = 1 - odd
        to_first = jnp.where(odd == 0, up, down)
        to_last = jnp.where(odd == 0, down, up)

        def put_rows(side):
            at = jnp.where(side == 0, OFF - T, OFF + ROWS)
            for k in range(T // 8):
                q = pl.multiple_of(at + 8 * k, 8)
                for g in range(G):
                    x = rbuf[sweep - 1, 1 - side, 0, g, pl.ds(8 * k, 8), :]
                    st[0, g + 1, pl.ds(q, 8), :] = x
                    if g == 0:
                        st[0, G + 1, pl.ds(q, 8), :] = pltpu.roll(x, 127, 1)
                    if g == G - 1:
                        st[0, 0, pl.ds(q, 8), :] = pltpu.roll(x, 1, 1)
                    st[1, g + 1, pl.ds(q, 8), :] = rbuf[sweep - 1, 1 - side, 1, g, pl.ds(8 * k, 8), :]

        @pl.when((sweep > 0) & (c == 0))
        def _():
            at = jnp.where(first == 0, OFF, OFF + ROWS - T)
            for k in range(T // 8):
                q = pl.multiple_of(at + 8 * k, 8)
                for f in range(2):
                    for g in range(G):
                        sbuf[sweep - 1, f, g, pl.ds(8 * k, 8), :] = st[f, g + 1, pl.ds(q, 8), :]
            exchange(sweep - 1, 1 - first, up, True).wait_recv()
            put_rows(first)
            exchange(sweep - 1, first, to_first, True).start()

        @pl.when((sweep > 0) & (c == 1))
        def _():
            exchange(sweep - 1, last, up, False).wait_send()

        @pl.when((sweep < SWEEPS - 1) & (c == 1))
        def _():
            exchange(sweep, first, to_first, False).start()

        @pl.when((sweep > 0) & (c == TILES - 1))
        def _():
            exchange(sweep - 1, 1 - last, up, True).wait_recv()
            put_rows(last)

        for sign in (-1, 1):
            for begins in (True, False):
                @pl.when((2 * odd - 1 == sign) & ((c == 0) == begins))
                def _():
                    run(sweep * T, base, sign, begins)

        @pl.when(sweep == SWEEPS - 1)
        def _():
            get(pl.multiple_of(jnp.where(c == 0, ROWS - TILE, (TILES - 1 - c) * TILE), 8))

        return 0

    lax.fori_loop(0, SWEEPS * TILES, tile, 0)

    wait_bytes(hbuf, pk_ssem.at[0])
    wait_bytes(sbuf, ex_ssem.at[1])


def solution(mesh):
    def local_run(u_tile, v_tile, w):
        dma = pltpu.SemaphoreType.DMA
        now, before = pl.pallas_call(
            wave_kernel,
            out_shape=[jax.ShapeDtypeStruct((ROWS, COLS), F32)] * 2,
            in_specs=[pl.BlockSpec(memory_space=pl.ANY)] * 3,
            out_specs=[pl.BlockSpec(memory_space=pltpu.VMEM)] * 2,
            scratch_shapes=[
                pltpu.VMEM((2, G + 2, R, 128), F32), pltpu.SMEM((3, 3, SWEEPS * T), F32), pltpu.VMEM((2 * G + 1, 8, 128), jnp.int32),
                pltpu.VMEM((ROWS + 2 * T, COLS), F32), pltpu.VMEM((ROWS + 2 * T, COLS), F32),
                pltpu.VMEM((2, ROWS, 128), F32), pltpu.VMEM((2, ROWS + 2 * T, 128), F32), pltpu.VMEM((2, G, TILE, 128), F32),
                pltpu.VMEM((SWEEPS - 1, 2, G, T, 128), F32), pltpu.VMEM((SWEEPS - 1, 2, 2, G, T, 128), F32),
                dma((4,)), dma((1,)), dma((2,)), dma((1,)), dma((TILES + 1,)), dma((2,)), dma((2,)), dma((SWEEPS - 1, 2)),
            ],
            compiler_params=pltpu.CompilerParams(collective_id=0, has_side_effects=True, vmem_limit_bytes=VMEM_LIMIT),
        )(u_tile, v_tile, pltpu.with_memory_space_constraint(jnp.transpose(w, (1, 2, 0)), pltpu.HBM))
        return 4.0 * now, 8.0 * (now - before)

    tile_spec = P(("ens", "row"), "col")
    return jax.shard_map(local_run, mesh=mesh, in_specs=(tile_spec, tile_spec, P()), out_specs=(tile_spec, tile_spec), check_vma=False)
```

```python
import jax
import jax.numpy as jnp
from jax import lax
from jax.experimental import pallas as pl
from jax.experimental.pallas import tpu as pltpu
from jax.sharding import PartitionSpec as P

F32 = jnp.float32
MESH = pl.DeviceIdType.MESH
ROWS, COLS = 256, 512
G = 5
T = 16
SWEEPS = 4
TILES = 3
TILE = (ROWS + 2 * T) // TILES
NG = TILE // 8
BLOCK = 4
OFF = 32
R = 328
VMEM_LIMIT = 55_300_000


def wave_kernel(u_hbm, v_hbm, w_hbm, now_ref, before_ref, st, w_ref, maps, uraw, vraw, pbuf, hbuf, zbuf, sbuf, rbuf,
                load_sem, raw_rsem, pk_ssem, pk_rsem, dg_rsem, ex_rsem):
    row = lax.axis_index("row")
    col = lax.axis_index("col")
    up = lax.rem(row + 3, 4)
    down = lax.rem(row + 1, 4)
    other = 1 - col

    barrier = pltpu.get_barrier_semaphore()
    for rr, cc in ((up, other), (down, other), (row, other), (up, col), (down, col)):
        pl.semaphore_signal(barrier, inc=1, device_id={"row": rr, "col": cc}, device_id_type=MESH)

    cuts = [0] + [TILE * (c + 1) - T for c in range(TILES - 1)] + [ROWS]

    stages = [[(lo, n, at, 128) for lo, n in spans for at in (0, COLS - 128)]
              for spans in (((ROWS - T, T), (0, cuts[1])), ((cuts[1], ROWS - T - cuts[1]),))]
    stages.append([(0, ROWS, 128, COLS - 256)])
    for k, pieces in enumerate(stages):
        for lo, n, at, m in pieces:
            for src, dst in ((u_hbm, uraw), (v_hbm, vraw)):
                pltpu.make_async_copy(src.at[pl.ds(lo, n), pl.ds(at, m)], dst.at[pl.ds(T + lo, n), pl.ds(at, m)], load_sem.at[k]).start()
    weights = pltpu.make_async_copy(w_hbm, w_ref, load_sem.at[3])
    weights.start()

    def wait_bytes(ref, sem):
        pltpu.make_async_copy(ref, ref, sem).wait()

    def wait_stage(k):
        wait_bytes(uraw.at[pl.ds(0, sum(n * m for _, n, _, m in stages[k]) * 2 // COLS)], load_sem.at[k])

    def zero(i, _):
        for f in range(2):
            for g in range(G + 2):
                st[f, g, pl.ds(pl.multiple_of(i * 8, 8), 8), :] = jnp.zeros((8, 128), F32)
        return 0

    lax.fori_loop(0, (OFF - T) // 8, zero, 0)
    lax.fori_loop((OFF + ROWS + T) // 8, R // 8, zero, 0)

    lane = lax.broadcasted_iota(jnp.int32, (8, 128), 1)
    maps[2 * G] = lax.rem(lane, G)
    for g in range(G):
        maps[g] = lax.rem(lane * G + (g + 64), 128)
        k = lax.rem(3 * (lane + (2 * G - g - 1)), G)
        maps[G + g] = lax.div(lax.rem(128 * k + lane + 64, 128 * G), G)

    pl.semaphore_wait(barrier, 5)

    def raw_copy(f, side):
        src = (u_hbm, v_hbm)[f]
        dst = (uraw, vraw)[f]
        lo, at, to = ((0, T + ROWS, up), (ROWS - T, 0, down))[side]
        return pltpu.make_async_remote_copy(
            src_ref=src.at[pl.ds(lo, T)], dst_ref=dst.at[pl.ds(at, T)],
            send_sem=pk_ssem.at[0], recv_sem=raw_rsem.at[side],
            device_id={"row": to, "col": col}, device_id_type=MESH)

    raws = [raw_copy(f, side) for side in range(2) for f in range(2)]
    for cp in raws[2:] + raws[:2]:
        cp.start()

    def packed_copy(c):
        n = cuts[c + 1] - cuts[c]
        return pltpu.make_async_remote_copy(
            src_ref=pbuf.at[:, pl.ds(cuts[c], n)], dst_ref=hbuf.at[:, pl.ds(T + cuts[c], n)],
            send_sem=pk_ssem.at[0], recv_sem=pk_rsem.at[c],
            device_id={"row": row, "col": other}, device_id_type=MESH)

    def diag_copy(side):
        lo, at, to = ((0, T + ROWS, up), (ROWS - T, 0, down))[side]
        return pltpu.make_async_remote_copy(
            src_ref=pbuf.at[:, pl.ds(lo, T)], dst_ref=hbuf.at[:, pl.ds(at, T)],
            send_sem=pk_ssem.at[0], recv_sem=dg_rsem.at[side],
            device_id={"row": to, "col": other}, device_id_type=MESH)

    packs = [packed_copy(c) for c in range(TILES)]
    diags = [diag_copy(side) for side in range(2)]

    wait_stage(0)

    def pack(i, _):
        r = pl.multiple_of(i * 8, 8)
        for f, ref in ((0, uraw), (1, vraw)):
            pbuf[f, pl.ds(r, 8), :] = jnp.where(lane < 64, ref[pl.ds(r + T, 8), 0:128], ref[pl.ds(r + T, 8), 384:512])
        return 0

    lax.fori_loop((ROWS - T) // 8, ROWS // 8, pack, 0)
    lax.fori_loop(0, cuts[1] // 8, pack, 0)
    diags[1].start()
    packs[0].start()
    wait_stage(1)
    lax.fori_loop(cuts[1] // 8, (ROWS - T) // 8, pack, 0)
    packs[1].start()
    diags[0].start()
    packs[2].start()

    wait_stage(2)
    weights.wait()

    def lanes(x, idx):
        return jnp.take_along_axis(x, idx, axis=1, mode="promise_in_bounds")

    def put_main(c):
        residue = maps[2 * G]
        for g in range(G):
            idx = maps[g]
            masks = [residue == (g + 1 + 2 * k) % G for k in range(3)]
            for n in range(NG):
                r = pl.multiple_of(c * TILE + 8 * n, 8)
                q = pl.multiple_of(c * TILE + (OFF - T + 8 * n), 8)
                u, v = uraw[pl.ds(r, 8), 384:512], vraw[pl.ds(r, 8), 384:512]
                for k in range(3):
                    u = jnp.where(masks[k], uraw[pl.ds(r, 8), 128 * k:128 * k + 128], u)
                    v = jnp.where(masks[k], vraw[pl.ds(r, 8), 128 * k:128 * k + 128], v)
                x = 0.25 * lanes(u, idx)
                st[0, g + 1, pl.ds(q, 8), :] = x
                st[1, g + 1, pl.ds(q, 8), :] = x - 0.125 * lanes(v, idx)

    def put_halo(c):
        sv = st.at[:, :, pl.ds(pl.multiple_of(c * TILE + (OFF - T), 8), TILE)]
        hv = hbuf.at[:, pl.ds(pl.multiple_of(c * TILE, 8), TILE)]
        for g in range(G):
            idx = maps[g]
            column = lane * G + (g - 64)
            halo = (column < 0) | (column >= COLS)
            for n in range(NG):
                rows = pl.ds(8 * n, 8)
                h = 0.25 * lanes(hv[0, rows, :], idx)
                x = jnp.where(halo, h, sv[0, g + 1, rows, :])
                sv[0, g + 1, rows, :] = x
                sv[1, g + 1, rows, :] = jnp.where(halo, h - 0.125 * lanes(hv[1, rows, :], idx), sv[1, g + 1, rows, :])
                if g == 0:
                    sv[0, G + 1, rows, :] = pltpu.roll(x, 127, 1)
                if g == G - 1:
                    sv[0, 0, rows, :] = pltpu.roll(x, 1, 1)

    def put_tile(i, _):
        @pl.when(i == 1)
        def _():
            wait_bytes(uraw.at[pl.ds(0, 2 * T)], raw_rsem.at[1])
            wait_bytes(uraw.at[pl.ds(0, 2 * T)], raw_rsem.at[0])

        put_main(lax.rem(i + 1, TILES))
        return 0

    lax.fori_loop(0, TILES, put_tile, 0)

    def run(t, base, sign, first):
        drops = [2 * (k + 1) // 8 if first else 0 for k in range(T)]
        tops = [sign * (k + 1) + (8 * drops[k] if sign < 0 else 0) for k in range(T)]
        low = min(tops) - 1
        high = max(top + TILE - 8 * drop for top, drop in zip(tops, drops)) + 1
        sv = st.at[:, :, pl.ds(base + low, high - low)]
        for k in range(T):
            src, dst = k % 2, 1 - k % 2
            wa, wb, wc, wd, we = [0.5 * w_ref[a, b, t + k] for a, b in ((0, 0), (0, 1), (0, 2), (1, 0), (1, 1))]
            blocks = []
            at, left = tops[k] - low, NG - drops[k]
            while left:
                n = min(left, BLOCK if left > BLOCK + 1 or left == BLOCK else (left + 1) // 2)
                blocks.append((at, 8 * n))
                at, left = at + 8 * n, left - n
            for q, rows in blocks if sign < 0 else blocks[::-1]:
                ca, cb, cc, cd, ce = [jnp.full((G, rows, 128), x, F32) for x in (wa, wb, wc, wd, 1.5 + we)]
                n = sv[src, :, pl.ds(q - 1, rows), :]
                m = sv[src, :, pl.ds(q, rows), :]
                s = sv[src, :, pl.ds(q + 1, rows), :]
                x = (ca * (n[0:G] + s[2:G + 2]) + cc * (n[2:G + 2] + s[0:G])) + (cb * (n[1:G + 1] + s[1:G + 1]) + cd * (m[0:G] + m[2:G + 2]))
                x = x + (ce * m[1:G + 1] - sv[dst, 1:G + 1, pl.ds(q, rows), :])
                sv[dst, 1:G + 1, pl.ds(q, rows), :] = x
                sv[dst, G + 1, pl.ds(q, rows), :] = pltpu.roll(x[0], 127, 1)
                sv[dst, 0, pl.ds(q, rows), :] = pltpu.roll(x[G - 1], 1, 1)

    def exchange(e, side, to, late):
        src = sbuf.at[e] if late else st.at[:, pl.ds(1, G), pl.ds(jnp.where(side == 0, OFF, OFF + ROWS - T), T)]
        return pltpu.make_async_remote_copy(
            src_ref=src, dst_ref=rbuf.at[e, side],
            send_sem=load_sem.at[int(late)], recv_sem=ex_rsem.at[e, side],
            device_id={"row": to, "col": col}, device_id_type=MESH)

    def get(lo):
        for g in range(G):
            idx = maps[G + g]
            for n in range(NG):
                q = pl.multiple_of(lo + (OFF + 8 * n), 8)
                for f in range(2):
                    zbuf[f, g, 8 * n:8 * n + 8, :] = lanes(st[f, g + 1, pl.ds(q, 8), :], idx)
        residue = maps[2 * G]
        for n in range(NG):
            r = pl.multiple_of(lo + 8 * n, 8)
            for f, out in ((0, now_ref), (1, before_ref)):
                for k in range(4):
                    x = zbuf[f, 0, 8 * n:8 * n + 8, :]
                    for g in range(1, G):
                        x = jnp.where(residue == (g + 1 + 2 * k) % G, zbuf[f, g, 8 * n:8 * n + 8, :], x)
                    out[pl.ds(r, 8), 128 * k:128 * k + 128] = x

    def tile(it, _):
        sweep, c = lax.div(it, TILES), lax.rem(it, TILES)
        odd = lax.rem(sweep, 2)
        base = jnp.where(odd == 0, OFF - T + TILE * c, OFF + ROWS + T - TILE * (c + 1))

        @pl.when(it == 0)
        def _():
            diags[1].wait_recv()
            packs[0].wait_recv()

        @pl.when(it == 1)
        def _():
            packs[1].wait_recv()

        @pl.when(it == 2)
        def _():
            diags[0].wait_recv()
            packs[2].wait_recv()

        @pl.when(sweep == 0)
        def _():
            put_halo(c)

        first = odd
        last = 1 - odd
        to_first = jnp.where(odd == 0, up, down)
        to_last = jnp.where(odd == 0, down, up)

        def put_rows(side):
            at = jnp.where(side == 0, OFF - T, OFF + ROWS)
            for k in range(T // 8):
                q = pl.multiple_of(at + 8 * k, 8)
                for g in range(G):
                    x = rbuf[sweep - 1, 1 - side, 0, g, pl.ds(8 * k, 8), :]
                    st[0, g + 1, pl.ds(q, 8), :] = x
                    if g == 0:
                        st[0, G + 1, pl.ds(q, 8), :] = pltpu.roll(x, 127, 1)
                    if g == G - 1:
                        st[0, 0, pl.ds(q, 8), :] = pltpu.roll(x, 1, 1)
                    st[1, g + 1, pl.ds(q, 8), :] = rbuf[sweep - 1, 1 - side, 1, g, pl.ds(8 * k, 8), :]

        @pl.when((sweep > 0) & (c == 0))
        def _():
            at = jnp.where(first == 0, OFF, OFF + ROWS - T)
            for k in range(T // 8):
                q = pl.multiple_of(at + 8 * k, 8)
                for f in range(2):
                    for g in range(G):
                        sbuf[sweep - 1, f, g, pl.ds(8 * k, 8), :] = st[f, g + 1, pl.ds(q, 8), :]
            exchange(sweep - 1, 1 - first, up, True).wait_recv()
            put_rows(first)
            exchange(sweep - 1, first, to_first, True).start()

        @pl.when((sweep > 0) & (c == 1))
        def _():
            exchange(sweep - 1, last, up, False).wait_send()

        @pl.when((sweep < SWEEPS - 1) & (c == 1))
        def _():
            exchange(sweep, first, to_first, False).start()

        @pl.when((sweep > 0) & (c == TILES - 1))
        def _():
            exchange(sweep - 1, 1 - last, up, True).wait_recv()
            put_rows(last)

        for sign in (-1, 1):
            for begins in (True, False):
                @pl.when((2 * odd - 1 == sign) & ((c == 0) == begins))
                def _():
                    run(sweep * T, base, sign, begins)

        @pl.when(sweep == SWEEPS - 1)
        def _():
            get(pl.multiple_of(jnp.where(c == 0, ROWS - TILE, (TILES - 1 - c) * TILE), 8))

        return 0

    lax.fori_loop(0, SWEEPS * TILES, tile, 0)

    wait_bytes(uraw.at[pl.ds(0, 4 * T + 2 * (ROWS + 2 * T) * 128 // COLS)], pk_ssem.at[0])
    wait_bytes(sbuf, load_sem.at[1])


def solution(mesh):
    def local_run(u_tile, v_tile, w):
        dma = pltpu.SemaphoreType.DMA
        now, before = pl.pallas_call(
            wave_kernel,
            out_shape=[jax.ShapeDtypeStruct((ROWS, COLS), F32)] * 2,
            in_specs=[pl.BlockSpec(memory_space=pl.ANY)] * 3,
            out_specs=[pl.BlockSpec(memory_space=pltpu.VMEM)] * 2,
            scratch_shapes=[
                pltpu.VMEM((2, G + 2, R, 128), F32), pltpu.SMEM((3, 3, SWEEPS * T), F32), pltpu.VMEM((2 * G + 1, 8, 128), jnp.int32),
                pltpu.VMEM((ROWS + 2 * T, COLS), F32), pltpu.VMEM((ROWS + 2 * T, COLS), F32),
                pltpu.VMEM((2, ROWS, 128), F32), pltpu.VMEM((2, ROWS + 2 * T, 128), F32), pltpu.VMEM((2, G, TILE, 128), F32),
                pltpu.VMEM((SWEEPS - 1, 2, G, T, 128), F32), pltpu.VMEM((SWEEPS - 1, 2, 2, G, T, 128), F32),
                dma((4,)), dma((2,)), dma((1,)), dma((TILES,)), dma((2,)), dma((SWEEPS - 1, 2)),
            ],
            compiler_params=pltpu.CompilerParams(collective_id=0, has_side_effects=True, vmem_limit_bytes=VMEM_LIMIT),
        )(u_tile, v_tile, pltpu.with_memory_space_constraint(jnp.transpose(w, (1, 2, 0)), pltpu.HBM))
        return 4.0 * now, 8.0 * (now - before)

    tile_spec = P(("ens", "row"), "col")
    return jax.shard_map(local_run, mesh=mesh, in_specs=(tile_spec, tile_spec, P()), out_specs=(tile_spec, tile_spec), check_vma=False)
```

```python
import jax
import jax.numpy as jnp
from jax import lax
from jax.experimental import pallas as pl
from jax.experimental.pallas import tpu as pltpu
from jax.sharding import PartitionSpec as P

F32 = jnp.float32
MESH = pl.DeviceIdType.MESH
ROWS, COLS = 256, 512
G = 5
T = 16
SWEEPS = 4
TILES = 3
TILE = (ROWS + 2 * T) // TILES
NG = TILE // 8
BLOCK = 3
OFF = 32
R = 328
VMEM_LIMIT = 55_300_000


def wave_kernel(u_hbm, v_hbm, w_hbm, now_ref, before_ref, st, w_ref, maps, uraw, vraw, pbuf, hbuf, zbuf, sbuf, rbuf,
                load_sem, raw_rsem, pk_ssem, pk_rsem, dg_rsem, ex_rsem):
    row = lax.axis_index("row")
    col = lax.axis_index("col")
    up = lax.rem(row + 3, 4)
    down = lax.rem(row + 1, 4)
    other = 1 - col

    barrier = pltpu.get_barrier_semaphore()
    for rr, cc in ((up, other), (down, other), (row, other), (up, col), (down, col)):
        pl.semaphore_signal(barrier, inc=1, device_id={"row": rr, "col": cc}, device_id_type=MESH)

    cuts = [0] + [TILE * (c + 1) - T for c in range(TILES - 1)] + [ROWS]

    stages = [[(lo, n, at, 128) for lo, n in spans for at in (0, COLS - 128)]
              for spans in (((ROWS - T, T), (0, cuts[1])), ((cuts[1], ROWS - T - cuts[1]),))]
    stages.append([(0, ROWS, 128, COLS - 256)])
    for k, pieces in enumerate(stages):
        for lo, n, at, m in pieces:
            for src, dst in ((u_hbm, uraw), (v_hbm, vraw)):
                pltpu.make_async_copy(src.at[pl.ds(lo, n), pl.ds(at, m)], dst.at[pl.ds(T + lo, n), pl.ds(at, m)], load_sem.at[k]).start()
    weights = pltpu.make_async_copy(w_hbm, w_ref, load_sem.at[3])
    weights.start()

    def wait_bytes(ref, sem):
        pltpu.make_async_copy(ref, ref, sem).wait()

    def wait_stage(k):
        wait_bytes(uraw.at[pl.ds(0, sum(n * m for _, n, _, m in stages[k]) * 2 // COLS)], load_sem.at[k])

    def zero(i, _):
        for f in range(2):
            for g in range(G + 2):
                st[f, g, pl.ds(pl.multiple_of(i * 8, 8), 8), :] = jnp.zeros((8, 128), F32)
        return 0

    lax.fori_loop(0, (OFF - T) // 8, zero, 0)
    lax.fori_loop((OFF + ROWS + T) // 8, R // 8, zero, 0)

    lane = lax.broadcasted_iota(jnp.int32, (8, 128), 1)
    maps[2 * G] = lax.rem(lane, G)
    for g in range(G):
        maps[g] = lax.rem(lane * G + (g + 64), 128)
        k = lax.rem(3 * (lane + (2 * G - g - 1)), G)
        maps[G + g] = lax.div(lax.rem(128 * k + lane + 64, 128 * G), G)

    pl.semaphore_wait(barrier, 5)

    def raw_copy(f, side):
        src = (u_hbm, v_hbm)[f]
        dst = (uraw, vraw)[f]
        lo, at, to = ((0, T + ROWS, up), (ROWS - T, 0, down))[side]
        return pltpu.make_async_remote_copy(
            src_ref=src.at[pl.ds(lo, T)], dst_ref=dst.at[pl.ds(at, T)],
            send_sem=pk_ssem.at[0], recv_sem=raw_rsem.at[side],
            device_id={"row": to, "col": col}, device_id_type=MESH)

    raws = [raw_copy(f, side) for side in range(2) for f in range(2)]
    for cp in raws[2:] + raws[:2]:
        cp.start()

    def packed_copy(c):
        n = cuts[c + 1] - cuts[c]
        return pltpu.make_async_remote_copy(
            src_ref=pbuf.at[:, pl.ds(cuts[c], n)], dst_ref=hbuf.at[:, pl.ds(T + cuts[c], n)],
            send_sem=pk_ssem.at[0], recv_sem=pk_rsem.at[c],
            device_id={"row": row, "col": other}, device_id_type=MESH)

    def diag_copy(side):
        lo, at, to = ((0, T + ROWS, up), (ROWS - T, 0, down))[side]
        return pltpu.make_async_remote_copy(
            src_ref=pbuf.at[:, pl.ds(lo, T)], dst_ref=hbuf.at[:, pl.ds(at, T)],
            send_sem=pk_ssem.at[0], recv_sem=dg_rsem.at[side],
            device_id={"row": to, "col": other}, device_id_type=MESH)

    packs = [packed_copy(c) for c in range(TILES)]
    diags = [diag_copy(side) for side in range(2)]

    wait_stage(0)

    def pack(i, _):
        r = pl.multiple_of(i * 8, 8)
        for f, ref in ((0, uraw), (1, vraw)):
            pbuf[f, pl.ds(r, 8), :] = jnp.where(lane < 64, ref[pl.ds(r + T, 8), 0:128], ref[pl.ds(r + T, 8), 384:512])
        return 0

    lax.fori_loop((ROWS - T) // 8, ROWS // 8, pack, 0)
    lax.fori_loop(0, cuts[1] // 8, pack, 0)
    diags[1].start()
    packs[0].start()
    wait_stage(1)
    lax.fori_loop(cuts[1] // 8, (ROWS - T) // 8, pack, 0)
    packs[1].start()
    diags[0].start()
    packs[2].start()

    wait_stage(2)
    weights.wait()

    def lanes(x, idx):
        return jnp.take_along_axis(x, idx, axis=1, mode="promise_in_bounds")

    def put_main(c):
        residue = maps[2 * G]
        for g in range(G):
            idx = maps[g]
            masks = [residue == (g + 1 + 2 * k) % G for k in range(3)]
            for n in range(NG):
                r = pl.multiple_of(c * TILE + 8 * n, 8)
                q = pl.multiple_of(c * TILE + (OFF - T + 8 * n), 8)
                u, v = uraw[pl.ds(r, 8), 384:512], vraw[pl.ds(r, 8), 384:512]
                for k in range(3):
                    u = jnp.where(masks[k], uraw[pl.ds(r, 8), 128 * k:128 * k + 128], u)
                    v = jnp.where(masks[k], vraw[pl.ds(r, 8), 128 * k:128 * k + 128], v)
                x = 0.25 * lanes(u, idx)
                st[0, g + 1, pl.ds(q, 8), :] = x
                st[1, g + 1, pl.ds(q, 8), :] = x - 0.125 * lanes(v, idx)

    def put_halo(c):
        sv = st.at[:, :, pl.ds(pl.multiple_of(c * TILE + (OFF - T), 8), TILE)]
        hv = hbuf.at[:, pl.ds(pl.multiple_of(c * TILE, 8), TILE)]
        for g in range(G):
            idx = maps[g]
            column = lane * G + (g - 64)
            halo = (column < 0) | (column >= COLS)
            for n in range(NG):
                rows = pl.ds(8 * n, 8)
                h = 0.25 * lanes(hv[0, rows, :], idx)
                x = jnp.where(halo, h, sv[0, g + 1, rows, :])
                sv[0, g + 1, rows, :] = x
                sv[1, g + 1, rows, :] = jnp.where(halo, h - 0.125 * lanes(hv[1, rows, :], idx), sv[1, g + 1, rows, :])
                if g == 0:
                    sv[0, G + 1, rows, :] = pltpu.roll(x, 127, 1)
                if g == G - 1:
                    sv[0, 0, rows, :] = pltpu.roll(x, 1, 1)

    def put_tile(i, _):
        @pl.when(i == 1)
        def _():
            wait_bytes(uraw.at[pl.ds(0, 2 * T)], raw_rsem.at[1])
            wait_bytes(uraw.at[pl.ds(0, 2 * T)], raw_rsem.at[0])

        put_main(lax.rem(i + 1, TILES))
        return 0

    lax.fori_loop(0, TILES, put_tile, 0)

    def run(t, base, sign, first):
        drops = [2 * (k + 1) // 8 if first else 0 for k in range(T)]
        tops = [sign * (k + 1) + (8 * drops[k] if sign < 0 else 0) for k in range(T)]
        low = min(tops) - 1
        high = max(top + TILE - 8 * drop for top, drop in zip(tops, drops)) + 1
        sv = st.at[:, :, pl.ds(base + low, high - low)]
        for k in range(T):
            src, dst = k % 2, 1 - k % 2
            wa, wb, wc, wd, we = [0.5 * w_ref[a, b, t + k] for a, b in ((0, 0), (0, 1), (0, 2), (1, 0), (1, 1))]
            blocks = []
            at, left = tops[k] - low, NG - drops[k]
            while left:
                n = min(left, BLOCK if left > BLOCK + 1 or left == BLOCK else (left + 1) // 2)
                blocks.append((at, 8 * n))
                at, left = at + 8 * n, left - n
            for q, rows in blocks if sign < 0 else blocks[::-1]:
                ca, cb, cc, cd, ce = [jnp.full((G, rows, 128), x, F32) for x in (wa, wb, wc, wd, 1.5 + we)]
                n = sv[src, :, pl.ds(q - 1, rows), :]
                m = sv[src, :, pl.ds(q, rows), :]
                s = sv[src, :, pl.ds(q + 1, rows), :]
                x = (ca * (n[0:G] + s[2:G + 2]) + cc * (n[2:G + 2] + s[0:G])) + (cb * (n[1:G + 1] + s[1:G + 1]) + cd * (m[0:G] + m[2:G + 2]))
                x = x + (ce * m[1:G + 1] - sv[dst, 1:G + 1, pl.ds(q, rows), :])
                sv[dst, 1:G + 1, pl.ds(q, rows), :] = x
                sv[dst, G + 1, pl.ds(q, rows), :] = pltpu.roll(x[0], 127, 1)
                sv[dst, 0, pl.ds(q, rows), :] = pltpu.roll(x[G - 1], 1, 1)

    def exchange(e, side, to, late):
        src = sbuf.at[e] if late else st.at[:, pl.ds(1, G), pl.ds(jnp.where(side == 0, OFF, OFF + ROWS - T), T)]
        return pltpu.make_async_remote_copy(
            src_ref=src, dst_ref=rbuf.at[e, side],
            send_sem=load_sem.at[int(late)], recv_sem=ex_rsem.at[e, side],
            device_id={"row": to, "col": col}, device_id_type=MESH)

    def get(lo):
        for g in range(G):
            idx = maps[G + g]
            for n in range(NG):
                q = pl.multiple_of(lo + (OFF + 8 * n), 8)
                for f in range(2):
                    zbuf[f, g, 8 * n:8 * n + 8, :] = lanes(st[f, g + 1, pl.ds(q, 8), :], idx)
        residue = maps[2 * G]
        for n in range(NG):
            r = pl.multiple_of(lo + 8 * n, 8)
            for f, out in ((0, now_ref), (1, before_ref)):
                for k in range(4):
                    x = zbuf[f, 0, 8 * n:8 * n + 8, :]
                    for g in range(1, G):
                        x = jnp.where(residue == (g + 1 + 2 * k) % G, zbuf[f, g, 8 * n:8 * n + 8, :], x)
                    out[pl.ds(r, 8), 128 * k:128 * k + 128] = x

    def tile(it, _):
        sweep, c = lax.div(it, TILES), lax.rem(it, TILES)
        odd = lax.rem(sweep, 2)
        base = jnp.where(odd == 0, OFF - T + TILE * c, OFF + ROWS + T - TILE * (c + 1))

        @pl.when(it == 0)
        def _():
            diags[1].wait_recv()
            packs[0].wait_recv()

        @pl.when(it == 1)
        def _():
            packs[1].wait_recv()

        @pl.when(it == 2)
        def _():
            diags[0].wait_recv()
            packs[2].wait_recv()

        @pl.when(sweep == 0)
        def _():
            put_halo(c)

        first = odd
        last = 1 - odd
        to_first = jnp.where(odd == 0, up, down)
        to_last = jnp.where(odd == 0, down, up)

        def put_rows(side):
            at = jnp.where(side == 0, OFF - T, OFF + ROWS)
            for k in range(T // 8):
                q = pl.multiple_of(at + 8 * k, 8)
                for g in range(G):
                    x = rbuf[sweep - 1, 1 - side, 0, g, pl.ds(8 * k, 8), :]
                    st[0, g + 1, pl.ds(q, 8), :] = x
                    if g == 0:
                        st[0, G + 1, pl.ds(q, 8), :] = pltpu.roll(x, 127, 1)
                    if g == G - 1:
                        st[0, 0, pl.ds(q, 8), :] = pltpu.roll(x, 1, 1)
                    st[1, g + 1, pl.ds(q, 8), :] = rbuf[sweep - 1, 1 - side, 1, g, pl.ds(8 * k, 8), :]

        @pl.when((sweep > 0) & (c == 0))
        def _():
            at = jnp.where(first == 0, OFF, OFF + ROWS - T)
            for k in range(T // 8):
                q = pl.multiple_of(at + 8 * k, 8)
                for f in range(2):
                    for g in range(G):
                        sbuf[sweep - 1, f, g, pl.ds(8 * k, 8), :] = st[f, g + 1, pl.ds(q, 8), :]
            exchange(sweep - 1, 1 - first, up, True).wait_recv()
            put_rows(first)
            exchange(sweep - 1, first, to_first, True).start()

        @pl.when((sweep > 0) & (c == 1))
        def _():
            exchange(sweep - 1, last, up, False).wait_send()

        @pl.when((sweep < SWEEPS - 1) & (c == 1))
        def _():
            exchange(sweep, first, to_first, False).start()

        @pl.when((sweep > 0) & (c == TILES - 1))
        def _():
            exchange(sweep - 1, 1 - last, up, True).wait_recv()
            put_rows(last)

        for sign in (-1, 1):
            for begins in (True, False):
                @pl.when((2 * odd - 1 == sign) & ((c == 0) == begins))
                def _():
                    run(sweep * T, base, sign, begins)

        @pl.when(sweep == SWEEPS - 1)
        def _():
            get(pl.multiple_of(jnp.where(c == 0, ROWS - TILE, (TILES - 1 - c) * TILE), 8))

        return 0

    lax.fori_loop(0, SWEEPS * TILES, tile, 0)

    wait_bytes(uraw.at[pl.ds(0, 4 * T + 2 * (ROWS + 2 * T) * 128 // COLS)], pk_ssem.at[0])
    wait_bytes(sbuf, load_sem.at[1])


def solution(mesh):
    def local_run(u_tile, v_tile, w):
        dma = pltpu.SemaphoreType.DMA
        now, before = pl.pallas_call(
            wave_kernel,
            out_shape=[jax.ShapeDtypeStruct((ROWS, COLS), F32)] * 2,
            in_specs=[pl.BlockSpec(memory_space=pl.ANY)] * 3,
            out_specs=[pl.BlockSpec(memory_space=pltpu.VMEM)] * 2,
            scratch_shapes=[
                pltpu.VMEM((2, G + 2, R, 128), F32), pltpu.SMEM((3, 3, SWEEPS * T), F32), pltpu.VMEM((2 * G + 1, 8, 128), jnp.int32),
                pltpu.VMEM((ROWS + 2 * T, COLS), F32), pltpu.VMEM((ROWS + 2 * T, COLS), F32),
                pltpu.VMEM((2, ROWS, 128), F32), pltpu.VMEM((2, ROWS + 2 * T, 128), F32), pltpu.VMEM((2, G, TILE, 128), F32),
                pltpu.VMEM((SWEEPS - 1, 2, G, T, 128), F32), pltpu.VMEM((SWEEPS - 1, 2, 2, G, T, 128), F32),
                dma((4,)), dma((2,)), dma((1,)), dma((TILES,)), dma((2,)), dma((SWEEPS - 1, 2)),
            ],
            compiler_params=pltpu.CompilerParams(collective_id=0, has_side_effects=True, vmem_limit_bytes=VMEM_LIMIT),
        )(u_tile, v_tile, pltpu.with_memory_space_constraint(jnp.transpose(w, (1, 2, 0)), pltpu.HBM))
        return 4.0 * now, 8.0 * (now - before)

    tile_spec = P(("ens", "row"), "col")
    return jax.shard_map(local_run, mesh=mesh, in_specs=(tile_spec, tile_spec, P()), out_specs=(tile_spec, tile_spec), check_vma=False)
```
